32 devices in a mesh: model: 4 (over z), dp: 8 (over y, x, core).
Axes of the slice: x: 2, y: 2, z: 4, core: 2. Of those that a mesh axis runs over, the one named last changes fastest.
Arguments:
- weight: float32 [16, 768, 3072], P(None, 'dp', 'model')
- grad_parts: float32 [16, 6144, 3072], P(None, 'dp', 'model')
- row_stat: float32 [16, 768], P(None, 'dp')
- col_stat: float32 [16, 3072], P(None, 'model')
- norm_scale: float32 [16, 768], P(None, 'dp')
- norm_grads: float32 [16, 6144], P(None, 'dp')
- norm_stat: float32 [16, 768], P(None, 'dp')
- learn_rate: float32 [], replicated
Outputs:
- output 1: float32 [16, 768, 3072], P(None, 'dp', 'model')
- output 2: float32 [16, 768], P(None, 'dp')
- output 3: float32 [16, 3072], P(None, 'model')
- output 4: float32 [16, 768], P(None, 'dp')
- output 5: float32 [16, 768], P(None, 'dp')
All inputs are finite; a program needn't handle non-finite values.
Results may differ from the reference program's by a relative error of at most 0.001.
Values sent between devices are 32-bit elements.
A program may use at most 1 GiB of HBM per device.

```python
import jax
import jax.numpy as jnp
from jax import lax

NUM_LAYERS = 16
D_MODEL = 768
D_FF = 3072
DATA_REPLICAS = 8
STEP_COUNT = 4

DECAY_POWER = 0.8
EPS_FLOOR = 1e-30
SCALE_FLOOR = 1e-3
CLIP_LIMIT = 1.0


def unit_mean_square(values):
    return values * lax.rsqrt(jnp.mean(values * values, axis=-1, keepdims=True))


def setup_inputs(seed: int = 0) -> dict:
    keys = jax.random.split(jax.random.key(seed), 20)
    row_pos = jnp.linspace(-1.0, 1.0, D_MODEL)
    col_pos = jnp.linspace(-1.0, 1.0, D_FF)
    shape_rows = (NUM_LAYERS, D_MODEL)
    shape_cols = (NUM_LAYERS, D_FF)
    shape_layer = (NUM_LAYERS, 1)
    row_tilt = jax.random.uniform(keys[0], shape_layer, minval=0.6, maxval=1.0)
    col_tilt = jax.random.uniform(keys[1], shape_layer, minval=0.6, maxval=1.0)
    row_scale = unit_mean_square(jnp.exp(row_tilt * row_pos + 0.4 * jax.random.normal(keys[2], shape_rows)))
    col_scale = unit_mean_square(jnp.exp(-col_tilt * col_pos + 0.4 * jax.random.normal(keys[3], shape_cols)))
    rep_scale = jax.random.uniform(keys[4], (NUM_LAYERS, DATA_REPLICAS, 1, 1), minval=0.5, maxval=1.5)
    grad_noise = jax.random.normal(keys[5], (NUM_LAYERS, DATA_REPLICAS, D_MODEL, D_FF))
    grad_parts = grad_noise * rep_scale * (row_scale[:, None, :, None] * DATA_REPLICAS ** -0.5) * col_scale[:, None, None, :]
    grad_parts = grad_parts.reshape(NUM_LAYERS, DATA_REPLICAS * D_MODEL, D_FF)
    ratio_tilt = jax.random.uniform(keys[6], shape_layer, minval=0.8, maxval=1.2)
    row_stat = row_scale ** 2 * 0.4 * jnp.exp(ratio_tilt * row_pos + 0.3 * jax.random.normal(keys[7], shape_rows))
    col_stat = col_scale ** 2 * 0.4 * jnp.exp(-ratio_tilt * col_pos + 0.3 * jax.random.normal(keys[8], shape_cols))
    w_gain = jax.random.uniform(keys[9], (NUM_LAYERS, 1, 1), minval=0.5, maxval=2.0)
    w_row_tilt = jax.random.uniform(keys[10], shape_layer, minval=0.5, maxval=1.0)
    w_col_tilt = jax.random.uniform(keys[11], shape_layer, minval=0.5, maxval=1.0)
    weight = jax.random.normal(keys[12], (NUM_LAYERS, D_MODEL, D_FF)) * w_gain
    weight = weight * jnp.exp(w_row_tilt * row_pos)[:, :, None] * jnp.exp(w_col_tilt * col_pos)[:, None, :]
    gain_tilt = jax.random.uniform(keys[13], shape_layer, minval=0.6, maxval=1.0)
    norm_gain = unit_mean_square(jnp.exp(gain_tilt * row_pos + 0.4 * jax.random.normal(keys[14], shape_rows)))
    norm_rep = jax.random.uniform(keys[15], (NUM_LAYERS, DATA_REPLICAS, 1), minval=0.5, maxval=1.5)
    norm_grads = jax.random.normal(keys[16], (NUM_LAYERS, DATA_REPLICAS, D_MODEL)) * norm_rep * norm_gain[:, None, :] * DATA_REPLICAS ** -0.5
    norm_grads = norm_grads.reshape(NUM_LAYERS, DATA_REPLICAS * D_MODEL)
    norm_stat = norm_gain ** 2 * 0.4 * jnp.exp(ratio_tilt * row_pos + 0.3 * jax.random.normal(keys[17], shape_rows))
    norm_scale = jnp.exp(0.5 * gain_tilt * row_pos) * (1.0 + 0.2 * jax.random.normal(keys[18], shape_rows))
    learn_rate = jax.random.uniform(keys[19], (), minval=0.5, maxval=1.0)
    return {'weight': weight, 'grad_parts': grad_parts, 'row_stat': row_stat, 'col_stat': col_stat, 'norm_scale': norm_scale, 'norm_grads': norm_grads, 'norm_stat': norm_stat, 'learn_rate': learn_rate}


def reference(weight, grad_parts, row_stat, col_stat, norm_scale, norm_grads, norm_stat, learn_rate):
    decay_rate = 1.0 - STEP_COUNT ** -DECAY_POWER
    grad_sum = jnp.sum(grad_parts.reshape(NUM_LAYERS, DATA_REPLICAS, D_MODEL, D_FF), axis=1)
    grad_sq = grad_sum * grad_sum + EPS_FLOOR
    row_new = decay_rate * row_stat + (1.0 - decay_rate) * jnp.mean(grad_sq, axis=2)
    col_new = decay_rate * col_stat + (1.0 - decay_rate) * jnp.mean(grad_sq, axis=1)
    row_mean = jnp.mean(row_new, axis=1, keepdims=True)
    update = grad_sum * lax.rsqrt(row_new / row_mean)[:, :, None] * lax.rsqrt(col_new)[:, None, :]
    upd_rms = jnp.sqrt(jnp.mean(update * update, axis=(1, 2), keepdims=True))
    update = update / jnp.maximum(1.0, upd_rms / CLIP_LIMIT)
    weight_rms = jnp.sqrt(jnp.mean(weight * weight, axis=(1, 2), keepdims=True))
    weight_new = weight - learn_rate * jnp.maximum(SCALE_FLOOR, weight_rms) * update
    norm_grad = jnp.sum(norm_grads.reshape(NUM_LAYERS, DATA_REPLICAS, D_MODEL), axis=1)
    norm_stat_new = decay_rate * norm_stat + (1.0 - decay_rate) * (norm_grad * norm_grad + EPS_FLOOR)
    norm_update = norm_grad * lax.rsqrt(norm_stat_new)
    norm_rms = jnp.sqrt(jnp.mean(norm_update * norm_update, axis=1, keepdims=True))
    norm_update = norm_update / jnp.maximum(1.0, norm_rms / CLIP_LIMIT)
    scale_rms = jnp.sqrt(jnp.mean(norm_scale * norm_scale, axis=1, keepdims=True))
    norm_new = norm_scale - learn_rate * jnp.maximum(SCALE_FLOOR, scale_rms) * norm_update
    return (weight_new, row_new, col_new, norm_new, norm_stat_new)
```

```python
import functools

import jax
import jax.numpy as jnp
from jax import lax
from jax.experimental import pallas as pl
from jax.experimental.pallas import tpu as pltpu
from jax.sharding import PartitionSpec as P

STEP_COUNT = 4
DECAY_POWER = 0.8
EPS_FLOOR = 1e-30
SCALE_FLOOR = 1e-3
CLIP_LIMIT = 1.0
DECAY = 1.0 - STEP_COUNT ** -DECAY_POWER
MESH = pl.DeviceIdType.MESH
LANES = 128
AHEAD = 2


def step_kernel(w_hbm, g_hbm, r_hbm, c_hbm, n_hbm, ng_hbm, v_hbm, lr_ref,
                wo_hbm, ro_hbm, co_hbm, no_hbm, vo_hbm,
                own, peer, in1x, in1y, in2, w_buf,
                r_buf, c_buf, n_buf, ng_buf, v_buf, r_pad,
                r_all, c_all, s_all, t_all, h_all, h_out, k_all,
                load_sem, pair_send, pair_recv,
                x1_send, x1_recv, y1_send, y1_recv, x2_send, x2_recv, y2_send, y2_recv,
                r_send, r_recv, c_send, c_recv, s_send, s_recv, t_send, t_recv,
                w_in_sem, w_out_sem, small_sem, out_sem, h_send, h_recv, k_send, k_recv):
    layers, _, rows, cols = own.shape
    half = rows // 2
    zs, ds = r_all.shape[1], c_all.shape[1]
    rows_total, cols_total = rows * ds, cols * zs
    z = lax.axis_index('model')
    d = lax.axis_index('dp')
    core = d % 2
    dx = d + 2 - 4 * ((d // 2) % 2)
    dy = d + 4 - 8 * (d // 4)
    dxy = dx + dy - d
    dc = d + 1 - 2 * core
    blocks = (dx, dxy, dy, d)

    def remote(src, dst, send, recv, **where):
        return pltpu.make_async_remote_copy(src_ref=src, dst_ref=dst, send_sem=send, recv_sem=recv,
                                            device_id=where, device_id_type=MESH)

    def drain(ref, sem):
        pltpu.make_async_copy(ref, ref, sem).wait()

    def load_own(l):
        for k in range(4):
            pltpu.make_async_copy(g_hbm.at[l, blocks[k]], own.at[l, k], load_sem.at[l]).start()

    def send_pair(l):
        for k in range(4):
            remote(g_hbm.at[l, blocks[k] + dc - d], peer.at[l, k], pair_send.at[l], pair_recv.at[l], dp=dc).start()

    def x1(l):
        return remote(own.at[l, 0:2, 0:half], in1x.at[l], x1_send.at[l], x1_recv.at[l], dp=dx)

    def y1(l):
        return remote(own.at[l, 1:3, half:rows], in1y.at[l], y1_send.at[l], y1_recv.at[l], dp=dy)

    def y2(l):
        return remote(own.at[l, 2, 0:half], in2.at[l, 0], y2_send.at[l], y2_recv.at[l], dp=dy)

    def x2(l):
        return remote(own.at[l, 0, half:rows], in2.at[l, 1], x2_send.at[l], x2_recv.at[l], dp=dx)

    def spread_z(buf, l, send, recv):
        for j in range(1, zs):
            remote(buf.at[l, z], buf.at[l, z], send.at[l], recv.at[l], model=(z + j) % zs).start()

    def spread_d(buf, l, send, recv):
        for j in range(1, ds):
            remote(buf.at[l, d], buf.at[l, d], send.at[l], recv.at[l], dp=(d + j) % ds).start()

    def total(buf, l):
        acc = buf[l, 0]
        for j in range(1, buf.shape[1]):
            acc = acc + buf[l, j]
        return acc

    def column(row):
        return jnp.transpose(jnp.broadcast_to(row, (LANES, LANES)))[0:rows]

    def fold(values):
        acc = values[:, 0:LANES]
        for t in range(1, cols // LANES):
            acc = acc + values[:, t * LANES:(t + 1) * LANES]
        return acc

    small = ((r_hbm, r_buf), (c_hbm, c_buf), (n_hbm, n_buf), (ng_hbm, ng_buf), (v_hbm, v_buf))
    for i, (src, dst) in enumerate(small):
        pltpu.make_async_copy(src, dst, small_sem.at[i]).start()
    for l in range(AHEAD):
        load_own(l)

    barrier = pltpu.get_barrier_semaphore()
    for j in range(1, zs):
        pl.semaphore_signal(barrier, inc=1, device_id={'model': (z + j) % zs}, device_id_type=MESH)
    for j in range(1, ds):
        pl.semaphore_signal(barrier, inc=1, device_id={'dp': (d + j) % ds}, device_id_type=MESH)
    pl.semaphore_wait(barrier, zs + ds - 2)
    for l in range(AHEAD):
        send_pair(l)

    def norm_send():
        for i, (src, dst) in enumerate(small):
            pltpu.make_async_copy(src, dst, small_sem.at[i]).wait()
        r_pad[...] = jnp.zeros_like(r_pad)
        r_pad[:, 0:rows] = r_buf[...]
        h_out[...] = jnp.zeros_like(h_out)
        for k in range(ds):
            h_out[k, :, 0:rows] = ng_buf[:, k * rows:(k + 1) * rows]
        h_all[d] = h_out[d]
        for j in range(1, ds):
            other = (d + j) % ds
            remote(h_out.at[other], h_all.at[d], h_send, h_recv, dp=other).start()

    def norm_grad():
        acc = h_all[0]
        for k in range(1, ds):
            acc = acc + h_all[k]
        return acc[:, 0:rows]

    def layer_sums(values):
        padded = jnp.concatenate([values, jnp.zeros((layers, LANES - rows), jnp.float32)], axis=1)
        return jnp.sum(jnp.transpose(padded), axis=0, keepdims=True)

    def norm_stats():
        drain(h_all.at[0:ds - 1], h_recv)
        h = norm_grad()
        v_new = DECAY * v_buf[...] + (1.0 - DECAY) * (h * h + EPS_FLOOR)
        v_buf[...] = v_new
        zv = h * lax.rsqrt(v_new)
        nv = n_buf[...]
        k_all[d, :, 0:layers] = layer_sums(zv * zv)
        k_all[d, :, LANES:LANES + layers] = layer_sums(nv * nv)
        for j in range(1, ds):
            remote(k_all.at[d], k_all.at[d], k_send, k_recv, dp=(d + j) % ds).start()
        pltpu.make_async_copy(v_buf, vo_hbm, out_sem.at[0]).start()

    def norm_update():
        drain(k_all.at[0:ds - 1], k_recv)
        acc = k_all[0]
        for k in range(1, ds):
            acc = acc + k_all[k]
        z_sq, n_sq = acc[:, 0:layers], acc[:, LANES:LANES + layers]
        clip = jnp.maximum(1.0, jnp.sqrt(z_sq / rows_total) / CLIP_LIMIT)
        scale = lr_ref[0, 0] * jnp.maximum(SCALE_FLOOR, jnp.sqrt(n_sq / rows_total))
        clip = jnp.transpose(jnp.broadcast_to(clip, (LANES, layers)))[:, 0:rows]
        scale = jnp.transpose(jnp.broadcast_to(scale, (LANES, layers)))[:, 0:rows]
        zv = norm_grad() * lax.rsqrt(v_buf[...])
        n_buf[...] = n_buf[...] - scale * (zv / clip)

    def stage_combine(l):
        drain(own.at[l], load_sem.at[l])
        drain(peer.at[l], pair_recv.at[l])
        own[l] = own[l] + peer[l]
        x1(l).start()
        y1(l).start()

    def stage_forward(l):
        x1(l).wait_recv()
        own[l, 2, 0:half] = own[l, 2, 0:half] + in1x[l, 1]
        y1(l).wait_recv()
        own[l, 0, half:rows] = own[l, 0, half:rows] + in1y[l, 0]
        own[l, 3, 0:half] = own[l, 3, 0:half] + in1x[l, 0]
        y2(l).start()
        own[l, 3, half:rows] = own[l, 3, half:rows] + in1y[l, 1]
        x2(l).start()

    def stage_stats(l):
        y2(l).wait_recv()
        x2(l).wait_recv()
        g = own[l, 3] + in2[l].reshape(rows, cols)
        own[l, 3] = g
        q = g * g + EPS_FLOOR
        c_all[l, d] = jnp.sum(q, axis=0, keepdims=True)
        p = fold(q)
        p = jnp.concatenate([p, jnp.zeros((LANES - rows, LANES), jnp.float32)], axis=0)
        r_all[l, z] = jnp.sum(jnp.transpose(p), axis=0, keepdims=True)
        spread_d(c_all, l, c_send, c_recv)
        spread_z(r_all, l, r_send, r_recv)

    def stage_moments(l):
        drain(r_all.at[l, 0:zs - 1], r_recv.at[l])
        drain(c_all.at[l, 0:ds - 1], c_recv.at[l])
        drain(w_buf.at[l], w_in_sem.at[l])
        r_new = DECAY * r_pad[pl.ds(l, 1)] + (1.0 - DECAY) * (total(r_all, l) / cols_total)
        c_new = DECAY * c_buf[pl.ds(l, 1)] + (1.0 - DECAY) * (total(c_all, l) / rows_total)
        r_pad[pl.ds(l, 1)] = r_new
        r_buf[pl.ds(l, 1)] = r_new[:, 0:rows]
        c_buf[pl.ds(l, 1)] = c_new
        a = column(lax.rsqrt(r_new))
        b = lax.rsqrt(c_new)
        acc = jnp.zeros((1, LANES), jnp.float32)
        w_acc = jnp.zeros((1, LANES), jnp.float32)
        for t in range(cols // LANES):
            sl = slice(t * LANES, (t + 1) * LANES)
            u = own[l, 3, :, sl] * a * b[:, sl]
            acc = acc + jnp.sum(u * u, axis=0, keepdims=True)
            w = w_buf[l, :, sl]
            w_acc = w_acc + jnp.sum(w * w, axis=0, keepdims=True)
        s_all[l, z, :, 0:LANES] = acc
        s_all[l, z, :, LANES:2 * LANES] = w_acc
        spread_z(s_all, l, s_send, s_recv)

    def stage_gather(l):
        drain(s_all.at[l, 0:zs - 1], s_recv.at[l])
        t_all[l, d, :, 0:2 * LANES] = total(s_all, l)
        t_all[l, d, :, 2 * LANES:3 * LANES] = r_pad[pl.ds(l, 1)]
        spread_d(t_all, l, t_send, t_recv)

    def stage_update(l):
        drain(t_all.at[l, 0:ds - 1], t_recv.at[l])
        sums = total(t_all, l)
        count = rows_total * cols_total
        u_sum = jnp.sum(sums[:, 0:LANES], axis=1, keepdims=True)
        w_sum = jnp.sum(sums[:, LANES:2 * LANES], axis=1, keepdims=True)
        r_mean = jnp.sum(sums[:, 2 * LANES:3 * LANES], axis=1, keepdims=True) / rows_total
        u_rms = jnp.sqrt(u_sum / count * r_mean)
        clip = jnp.maximum(1.0, u_rms / CLIP_LIMIT)
        scale = lr_ref[0, 0] * jnp.maximum(SCALE_FLOOR, jnp.sqrt(w_sum / count))
        a = column(lax.rsqrt(r_pad[pl.ds(l, 1)] / r_mean))
        b = lax.rsqrt(c_buf[pl.ds(l, 1)]) / clip
        for t in range(cols // LANES):
            sl = slice(t * LANES, (t + 1) * LANES)
            u = own[l, 3, :, sl] * a * b[:, sl]
            w_buf[l, :, sl] = w_buf[l, :, sl] - scale * u

    def write(l):
        return pltpu.make_async_copy(w_buf.at[l], wo_hbm.at[l], w_out_sem.at[l])

    def body(i, carry):
        @pl.when(i + AHEAD < layers)
        def _():
            load_own(i + AHEAD)
            send_pair(i + AHEAD)

        @pl.when(i < layers)
        def _():
            pltpu.make_async_copy(w_hbm.at[i], w_buf.at[i], w_in_sem.at[i]).start()
            stage_combine(i)

        @pl.when((i >= 1) & (i < layers + 1))
        def _():
            stage_forward(i - 1)

        @pl.when(i == 1)
        def _():
            norm_send()

        @pl.when((i >= 2) & (i < layers + 2))
        def _():
            stage_stats(i - 2)

        @pl.when(i == 3)
        def _():
            norm_stats()

        @pl.when((i >= 3) & (i < layers + 3))
        def _():
            stage_moments(i - 3)

        @pl.when((i >= 4) & (i < layers + 4))
        def _():
            stage_gather(i - 4)

        @pl.when(i == 5)
        def _():
            norm_update()

        @pl.when((i >= 5) & (i < layers + 5))
        def _():
            stage_update(i - 5)

        @pl.when((i >= 6) & (i < layers + 6))
        def _():
            write(i - 6).start()

        @pl.when(i == layers + 3)
        def _():
            pltpu.make_async_copy(r_buf, ro_hbm, out_sem.at[1]).start()
            pltpu.make_async_copy(c_buf, co_hbm, out_sem.at[2]).start()
            pltpu.make_async_copy(n_buf, no_hbm, out_sem.at[3]).start()

        return carry

    lax.fori_loop(0, layers + 6, body, 0)

    def finish(l, carry):
        drain(peer.at[l], pair_send.at[l])
        x1(l).wait_send()
        y1(l).wait_send()
        x2(l).wait_send()
        y2(l).wait_send()
        drain(r_all.at[l, 0:zs - 1], r_send.at[l])
        drain(c_all.at[l, 0:ds - 1], c_send.at[l])
        drain(s_all.at[l, 0:zs - 1], s_send.at[l])
        drain(t_all.at[l, 0:ds - 1], t_send.at[l])
        write(l).wait()
        return carry

    lax.fori_loop(0, layers, finish, 0)
    drain(h_all.at[0:ds - 1], h_send)
    drain(k_all.at[0:ds - 1], k_send)
    for i, (src, dst) in enumerate(((v_buf, vo_hbm), (r_buf, ro_hbm), (c_buf, co_hbm), (n_buf, no_hbm))):
        pltpu.make_async_copy(src, dst, out_sem.at[i]).wait()


def solution(mesh):
    ds = mesh.shape['dp']
    zs = mesh.shape['model']

    def local_step(weight, grad_parts, row_stat, col_stat, norm_scale, norm_grads, norm_stat, learn_rate):
        layers, rows, cols = weight.shape
        half = rows // 2
        f32 = jnp.float32
        grads = grad_parts.reshape(layers, ds, rows, cols)
        any_spec = pl.BlockSpec(memory_space=pltpu.MemorySpace.HBM)
        dma = pltpu.SemaphoreType.DMA
        per_layer = [dma((layers,))] * 21
        return pl.pallas_call(
            step_kernel,
            out_shape=[jax.ShapeDtypeStruct(a.shape, f32) for a in (weight, row_stat, col_stat, norm_scale, norm_stat)],
            in_specs=[any_spec] * 7 + [pl.BlockSpec(memory_space=pltpu.SMEM)],
            out_specs=[any_spec] * 5,
            scratch_shapes=[
                pltpu.VMEM((layers, 4, rows, cols), f32),
                pltpu.VMEM((layers, 4, rows, cols), f32),
                pltpu.VMEM((layers, 2, half, cols), f32),
                pltpu.VMEM((layers, 2, half, cols), f32),
                pltpu.VMEM((layers, 2, half, cols), f32),
                pltpu.VMEM((layers, rows, cols), f32),
                pltpu.VMEM(row_stat.shape, f32),
                pltpu.VMEM(col_stat.shape, f32),
                pltpu.VMEM(norm_scale.shape, f32),
                pltpu.VMEM(norm_grads.shape, f32),
                pltpu.VMEM(norm_stat.shape, f32),
                pltpu.VMEM((layers, LANES), f32),
                pltpu.VMEM((layers, zs, 1, LANES), f32),
                pltpu.VMEM((layers, ds, 1, cols), f32),
                pltpu.VMEM((layers, zs, 1, 2 * LANES), f32),
                pltpu.VMEM((layers, ds, 1, 3 * LANES), f32),
                pltpu.VMEM((ds, layers, LANES), f32),
                pltpu.VMEM((ds, layers, LANES), f32),
                pltpu.VMEM((ds, 1, 2 * LANES), f32),
                *per_layer[:19],
                dma((layers,)), dma((layers,)), dma((5,)), dma((4,)),
                dma, dma, dma, dma,
            ],
            compiler_params=pltpu.CompilerParams(collective_id=0, has_side_effects=True, vmem_limit_bytes=67043328),
            name='adafactor_step',
        )(weight, grads, row_stat, col_stat, norm_scale, norm_grads, norm_stat, learn_rate.reshape(1, 1))

    mat_spec = P(None, 'dp', 'model')
    row_spec = P(None, 'dp')
    col_spec = P(None, 'model')
    return jax.shard_map(local_step, mesh=mesh, in_specs=(mat_spec, mat_spec, row_spec, col_spec, row_spec, row_spec, row_spec, P()), out_specs=(mat_spec, row_spec, col_spec, row_spec, row_spec), check_vma=False)
```

```python
import functools

import jax
import jax.numpy as jnp
from jax import lax
from jax.experimental import pallas as pl
from jax.experimental.pallas import tpu as pltpu
from jax.sharding import PartitionSpec as P

STEP_COUNT = 4
DECAY_POWER = 0.8
EPS_FLOOR = 1e-30
SCALE_FLOOR = 1e-3
CLIP_LIMIT = 1.0
DECAY = 1.0 - STEP_COUNT ** -DECAY_POWER
MESH = pl.DeviceIdType.MESH
LANES = 128
AHEAD = 2


def step_kernel(w_hbm, g_hbm, r_hbm, c_hbm, n_hbm, ng_hbm, v_hbm, lr_ref,
                w_buf, r_buf, c_buf, n_buf, v_buf,
                own, peer, in1x, in1y, in2, ng_buf, r_pad,
                r_all, c_all, s_all, t_all, h_all, h_out, k_all,
                load_sem, pair_send, pair_recv,
                x1_send, x1_recv, y1_send, y1_recv, x2_send, x2_recv, y2_send, y2_recv,
                r_send, r_recv, c_send, c_recv, s_send, s_recv, t_send, t_recv,
                w_in_sem, small_sem, h_send, h_recv, k_send, k_recv):
    layers, _, rows, cols = own.shape
    half = rows // 2
    zs, ds = r_all.shape[1], c_all.shape[1]
    rows_total, cols_total = rows * ds, cols * zs
    z = lax.axis_index('model')
    d = lax.axis_index('dp')
    core = d % 2
    dx = d + 2 - 4 * ((d // 2) % 2)
    dy = d + 4 - 8 * (d // 4)
    dxy = dx + dy - d
    dc = d + 1 - 2 * core
    blocks = (dx, dxy, dy, d)

    def remote(src, dst, send, recv, **where):
        return pltpu.make_async_remote_copy(src_ref=src, dst_ref=dst, send_sem=send, recv_sem=recv,
                                            device_id=where, device_id_type=MESH)

    def drain(ref, sem):
        pltpu.make_async_copy(ref, ref, sem).wait()

    def load_own(l):
        for k in range(4):
            pltpu.make_async_copy(g_hbm.at[l, blocks[k]], own.at[l, k], load_sem.at[l]).start()

    def send_pair(l):
        for k in range(4):
            remote(g_hbm.at[l, blocks[k] + dc - d], peer.at[l, k], pair_send.at[l], pair_recv.at[l], dp=dc).start()

    def x1(l):
        return remote(own.at[l, 0:2, 0:half], in1x.at[l], x1_send.at[l], x1_recv.at[l], dp=dx)

    def y1(l):
        return remote(own.at[l, 1:3, half:rows], in1y.at[l], y1_send.at[l], y1_recv.at[l], dp=dy)

    def y2(l):
        return remote(own.at[l, 2, 0:half], in2.at[l, 0], y2_send.at[l], y2_recv.at[l], dp=dy)

    def x2(l):
        return remote(own.at[l, 0, half:rows], in2.at[l, 1], x2_send.at[l], x2_recv.at[l], dp=dx)

    def spread_z(buf, l, send, recv):
        for j in range(1, zs):
            remote(buf.at[l, z], buf.at[l, z], send.at[l], recv.at[l], model=(z + j) % zs).start()

    def spread_d(buf, l, send, recv):
        for j in range(1, ds):
            remote(buf.at[l, d], buf.at[l, d], send.at[l], recv.at[l], dp=(d + j) % ds).start()

    def total(buf, l):
        acc = buf[l, 0]
        for j in range(1, buf.shape[1]):
            acc = acc + buf[l, j]
        return acc

    def column(row):
        return jnp.transpose(jnp.broadcast_to(row, (LANES, LANES)))[0:rows]

    def fold(values):
        acc = values[:, 0:LANES]
        for t in range(1, cols // LANES):
            acc = acc + values[:, t * LANES:(t + 1) * LANES]
        return acc

    small = ((r_hbm, r_buf), (c_hbm, c_buf), (n_hbm, n_buf), (ng_hbm, ng_buf), (v_hbm, v_buf))
    for i, (src, dst) in enumerate(small):
        pltpu.make_async_copy(src, dst, small_sem.at[i]).start()
    for l in range(AHEAD):
        load_own(l)

    barrier = pltpu.get_barrier_semaphore()
    for j in range(1, zs):
        pl.semaphore_signal(barrier, inc=1, device_id={'model': (z + j) % zs}, device_id_type=MESH)
    for j in range(1, ds):
        pl.semaphore_signal(barrier, inc=1, device_id={'dp': (d + j) % ds}, device_id_type=MESH)
    pl.semaphore_wait(barrier, zs + ds - 2)
    for l in range(AHEAD):
        send_pair(l)

    def norm_send():
        for i, (src, dst) in enumerate(small):
            pltpu.make_async_copy(src, dst, small_sem.at[i]).wait()
        r_pad[...] = jnp.zeros_like(r_pad)
        r_pad[:, 0:rows] = r_buf[...]
        h_out[...] = jnp.zeros_like(h_out)
        for k in range(ds):
            h_out[k, :, 0:rows] = ng_buf[:, k * rows:(k + 1) * rows]
        h_all[d] = h_out[d]
        for j in range(1, ds):
            other = (d + j) % ds
            remote(h_out.at[other], h_all.at[d], h_send, h_recv, dp=other).start()

    def norm_grad():
        acc = h_all[0]
        for k in range(1, ds):
            acc = acc + h_all[k]
        return acc[:, 0:rows]

    def layer_sums(values):
        padded = jnp.concatenate([values, jnp.zeros((layers, LANES - rows), jnp.float32)], axis=1)
        return jnp.sum(jnp.transpose(padded), axis=0, keepdims=True)

    def norm_stats():
        drain(h_all.at[0:ds - 1], h_recv)
        h = norm_grad()
        v_new = DECAY * v_buf[...] + (1.0 - DECAY) * (h * h + EPS_FLOOR)
        v_buf[...] = v_new
        zv = h * lax.rsqrt(v_new)
        nv = n_buf[...]
        k_all[d, :, 0:layers] = layer_sums(zv * zv)
        k_all[d, :, LANES:LANES + layers] = layer_sums(nv * nv)
        for j in range(1, ds):
            remote(k_all.at[d], k_all.at[d], k_send, k_recv, dp=(d + j) % ds).start()

    def norm_update():
        drain(k_all.at[0:ds - 1], k_recv)
        acc = k_all[0]
        for k in range(1, ds):
            acc = acc + k_all[k]
        z_sq, n_sq = acc[:, 0:layers], acc[:, LANES:LANES + layers]
        clip = jnp.maximum(1.0, jnp.sqrt(z_sq / rows_total) / CLIP_LIMIT)
        scale = lr_ref[0, 0] * jnp.maximum(SCALE_FLOOR, jnp.sqrt(n_sq / rows_total))
        clip = jnp.transpose(jnp.broadcast_to(clip, (LANES, layers)))[:, 0:rows]
        scale = jnp.transpose(jnp.broadcast_to(scale, (LANES, layers)))[:, 0:rows]
        zv = norm_grad() * lax.rsqrt(v_buf[...])
        n_buf[...] = n_buf[...] - scale * (zv / clip)

    def stage_combine(l):
        drain(own.at[l], load_sem.at[l])
        drain(peer.at[l], pair_recv.at[l])
        own[l] = own[l] + peer[l]
        x1(l).start()
        y1(l).start()

    def stage_forward(l):
        x1(l).wait_recv()
        own[l, 2, 0:half] = own[l, 2, 0:half] + in1x[l, 1]
        y1(l).wait_recv()
        own[l, 0, half:rows] = own[l, 0, half:rows] + in1y[l, 0]
        own[l, 3, 0:half] = own[l, 3, 0:half] + in1x[l, 0]
        y2(l).start()
        own[l, 3, half:rows] = own[l, 3, half:rows] + in1y[l, 1]
        x2(l).start()

    def stage_stats(l):
        y2(l).wait_recv()
        x2(l).wait_recv()
        g = own[l, 3] + in2[l].reshape(rows, cols)
        own[l, 3] = g
        q = g * g + EPS_FLOOR
        c_all[l, d] = jnp.sum(q, axis=0, keepdims=True)
        p = fold(q)
        p = jnp.concatenate([p, jnp.zeros((LANES - rows, LANES), jnp.float32)], axis=0)
        r_all[l, z] = jnp.sum(jnp.transpose(p), axis=0, keepdims=True)
        spread_d(c_all, l, c_send, c_recv)
        spread_z(r_all, l, r_send, r_recv)

    def stage_moments(l):
        drain(r_all.at[l, 0:zs - 1], r_recv.at[l])
        drain(c_all.at[l, 0:ds - 1], c_recv.at[l])
        drain(w_buf.at[l], w_in_sem.at[l])
        r_new = DECAY * r_pad[pl.ds(l, 1)] + (1.0 - DECAY) * (total(r_all, l) / cols_total)
        c_new = DECAY * c_buf[pl.ds(l, 1)] + (1.0 - DECAY) * (total(c_all, l) / rows_total)
        r_pad[pl.ds(l, 1)] = r_new
        r_buf[pl.ds(l, 1)] = r_new[:, 0:rows]
        c_buf[pl.ds(l, 1)] = c_new
        a = column(lax.rsqrt(r_new))
        b = lax.rsqrt(c_new)
        acc = jnp.zeros((1, LANES), jnp.float32)
        w_acc = jnp.zeros((1, LANES), jnp.float32)
        for t in range(cols // LANES):
            sl = slice(t * LANES, (t + 1) * LANES)
            u = own[l, 3, :, sl] * a * b[:, sl]
            acc = acc + jnp.sum(u * u, axis=0, keepdims=True)
            w = w_buf[l, :, sl]
            w_acc = w_acc + jnp.sum(w * w, axis=0, keepdims=True)
        s_all[l, z, :, 0:LANES] = acc
        s_all[l, z, :, LANES:2 * LANES] = w_acc
        spread_z(s_all, l, s_send, s_recv)

    def stage_gather(l):
        drain(s_all.at[l, 0:zs - 1], s_recv.at[l])
        t_all[l, d, :, 0:2 * LANES] = total(s_all, l)
        t_all[l, d, :, 2 * LANES:3 * LANES] = r_pad[pl.ds(l, 1)]
        spread_d(t_all, l, t_send, t_recv)

    def stage_update(l):
        drain(t_all.at[l, 0:ds - 1], t_recv.at[l])
        sums = total(t_all, l)
        count = rows_total * cols_total
        u_sum = jnp.sum(sums[:, 0:LANES], axis=1, keepdims=True)
        w_sum = jnp.sum(sums[:, LANES:2 * LANES], axis=1, keepdims=True)
        r_mean = jnp.sum(sums[:, 2 * LANES:3 * LANES], axis=1, keepdims=True) / rows_total
        u_rms = jnp.sqrt(u_sum / count * r_mean)
        clip = jnp.maximum(1.0, u_rms / CLIP_LIMIT)
        scale = lr_ref[0, 0] * jnp.maximum(SCALE_FLOOR, jnp.sqrt(w_sum / count))
        a = column(lax.rsqrt(r_pad[pl.ds(l, 1)] / r_mean))
        b = lax.rsqrt(c_buf[pl.ds(l, 1)]) / clip
        for t in range(cols // LANES):
            sl = slice(t * LANES, (t + 1) * LANES)
            u = own[l, 3, :, sl] * a * b[:, sl]
            w_buf[l, :, sl] = w_buf[l, :, sl] - scale * u

    def body(i, carry):
        @pl.when(i + AHEAD < layers)
        def _():
            load_own(i + AHEAD)
            send_pair(i + AHEAD)

        @pl.when(i < layers)
        def _():
            pltpu.make_async_copy(w_hbm.at[i], w_buf.at[i], w_in_sem.at[i]).start()
            stage_combine(i)

        @pl.when((i >= 1) & (i < layers + 1))
        def _():
            stage_forward(i - 1)

        @pl.when(i == 1)
        def _():
            norm_send()

        @pl.when((i >= 2) & (i < layers + 2))
        def _():
            stage_stats(i - 2)

        @pl.when(i == 3)
        def _():
            norm_stats()

        @pl.when((i >= 3) & (i < layers + 3))
        def _():
            stage_moments(i - 3)

        @pl.when((i >= 4) & (i < layers + 4))
        def _():
            stage_gather(i - 4)

        @pl.when(i == 5)
        def _():
            norm_update()

        @pl.when((i >= 5) & (i < layers + 5))
        def _():
            stage_update(i - 5)

        return carry

    lax.fori_loop(0, layers + 5, body, 0)

    def finish(l, carry):
        drain(peer.at[l], pair_send.at[l])
        x1(l).wait_send()
        y1(l).wait_send()
        x2(l).wait_send()
        y2(l).wait_send()
        drain(r_all.at[l, 0:zs - 1], r_send.at[l])
        drain(c_all.at[l, 0:ds - 1], c_send.at[l])
        drain(s_all.at[l, 0:zs - 1], s_send.at[l])
        drain(t_all.at[l, 0:ds - 1], t_send.at[l])
        return carry

    lax.fori_loop(0, layers, finish, 0)
    drain(h_all.at[0:ds - 1], h_send)
    drain(k_all.at[0:ds - 1], k_send)


def write_kernel(*refs):
    count = len(refs) // 2
    pairs = list(zip(refs[:count], refs[count:2 * count]))
    sem = refs[-1]
    for i, (src, dst) in enumerate(pairs):
        pltpu.make_async_copy(src, dst, sem.at[i]).start()
    for i, (src, dst) in enumerate(pairs):
        pltpu.make_async_copy(src, dst, sem.at[i]).wait()


def write_out(arrays):
    return pl.pallas_call(
        write_kernel,
        out_shape=[jax.ShapeDtypeStruct(a.shape, a.dtype) for a in arrays],
        in_specs=[pl.BlockSpec(memory_space=pltpu.MemorySpace.VMEM)] * len(arrays),
        out_specs=[pl.BlockSpec(memory_space=pltpu.MemorySpace.HBM)] * len(arrays),
        scratch_shapes=[pltpu.SemaphoreType.DMA((len(arrays),))],
        compiler_params=pltpu.CompilerParams(vmem_limit_bytes=1 << 20),
        name='write_out',
    )(*arrays)


def solution(mesh):
    ds = mesh.shape['dp']
    zs = mesh.shape['model']

    def local_step(weight, grad_parts, row_stat, col_stat, norm_scale, norm_grads, norm_stat, learn_rate):
        layers, rows, cols = weight.shape
        half = rows // 2
        f32 = jnp.float32
        grads = grad_parts.reshape(layers, ds, rows, cols)
        any_spec = pl.BlockSpec(memory_space=pltpu.MemorySpace.HBM)
        dma = pltpu.SemaphoreType.DMA
        per_layer = [dma((layers,))] * 21
        outs = pl.pallas_call(
            step_kernel,
            out_shape=[pltpu.VMEM(a.shape, f32) for a in (weight, row_stat, col_stat, norm_scale, norm_stat)],
            in_specs=[any_spec] * 7 + [pl.BlockSpec(memory_space=pltpu.SMEM)],
            out_specs=[pl.BlockSpec(memory_space=pltpu.MemorySpace.VMEM)] * 5,
            scratch_shapes=[
                pltpu.VMEM((layers, 4, rows, cols), f32),
                pltpu.VMEM((layers, 4, rows, cols), f32),
                pltpu.VMEM((layers, 2, half, cols), f32),
                pltpu.VMEM((layers, 2, half, cols), f32),
                pltpu.VMEM((layers, 2, half, cols), f32),
                pltpu.VMEM(norm_grads.shape, f32),
                pltpu.VMEM((layers, LANES), f32),
                pltpu.VMEM((layers, zs, 1, LANES), f32),
                pltpu.VMEM((layers, ds, 1, cols), f32),
                pltpu.VMEM((layers, zs, 1, 2 * LANES), f32),
                pltpu.VMEM((layers, ds, 1, 3 * LANES), f32),
                pltpu.VMEM((ds, layers, LANES), f32),
                pltpu.VMEM((ds, layers, LANES), f32),
                pltpu.VMEM((ds, 1, 2 * LANES), f32),
                *per_layer[:19],
                dma((layers,)), dma((5,)),
                dma, dma, dma, dma,
            ],
            compiler_params=pltpu.CompilerParams(collective_id=0, has_side_effects=True, vmem_limit_bytes=54 * 1000 * 1000),
            name='adafactor_step',
        )(weight, grads, row_stat, col_stat, norm_scale, norm_grads, norm_stat, learn_rate.reshape(1, 1))
        return write_out(outs)

    mat_spec = P(None, 'dp', 'model')
    row_spec = P(None, 'dp')
    col_spec = P(None, 'model')
    return jax.shard_map(local_step, mesh=mesh, in_specs=(mat_spec, mat_spec, row_spec, col_spec, row_spec, row_spec, row_spec, P()), out_specs=(mat_spec, row_spec, col_spec, row_spec, row_spec), check_vma=False)
```

```python
import functools

import jax
import jax.numpy as jnp
from jax import lax
from jax.experimental import pallas as pl
from jax.experimental.pallas import tpu as pltpu
from jax.sharding import PartitionSpec as P

STEP_COUNT = 4
DECAY_POWER = 0.8
EPS_FLOOR = 1e-30
SCALE_FLOOR = 1e-3
CLIP_LIMIT = 1.0
DECAY = 1.0 - STEP_COUNT ** -DECAY_POWER
MESH = pl.DeviceIdType.MESH
LANES = 128
AHEAD = 2


def step_kernel(w_hbm, g_hbm, r_hbm, c_hbm, n_hbm, ng_hbm, v_hbm, lr_ref,
                w_buf, r_buf, c_buf, n_buf, v_buf,
                own, peer, in1x, in1y, in2, ng_buf, r_pad,
                r_all, c_pair, c_all, c_last, s_all, t_all, h_out, h_pair, h_all, k_all,
                load_sem, pair_send, pair_x, pair_y, pair_rest,
                x1_send, x1_recv, y1_send, y1_recv, x2_send, x2_recv, y2_send, y2_recv,
                r_send, r_recv, cp_send, cp_recv, c_send, c_recv, s_send, s_recv, t_send, t_recv, w_sem,
                small_sem, h_send, h_recv, k_send, k_recv):
    layers, _, rows, cols = own.shape
    half = rows // 2
    last = layers - 1
    zs, ds = r_all.shape[1], c_last.shape[0]
    chips = ds // 2
    rows_total, cols_total = rows * ds, cols * zs
    z = lax.axis_index('model')
    d = lax.axis_index('dp')
    core = d % 2
    chip = d // 2
    dx = d + 2 - 4 * (chip % 2)
    dy = d + 4 - 8 * (d // 4)
    dxy = dx + dy - d
    dc = d + 1 - 2 * core
    blocks = (dx, dxy, dy, d)
    column_peers = []
    for j in range(1, 2 * zs):
        other = (2 * z + core + j) % (2 * zs)
        column_peers.append({'model': other // 2, 'dp': d - core + other % 2})
    z_peers = [{'model': (z + j) % zs} for j in range(1, zs)]
    d_peers = [{'dp': (d + j) % ds} for j in range(1, ds)]
    plane_peers = [{'dp': e} for e in (dx, dy, dxy)]

    def remote(src, dst, send, recv, where):
        return pltpu.make_async_remote_copy(src_ref=src, dst_ref=dst, send_sem=send, recv_sem=recv,
                                            device_id=where, device_id_type=MESH)

    def spread(ref, send, recv, peers):
        for where in peers:
            remote(ref, ref, send, recv, where).start()

    def drain(ref, sem):
        pltpu.make_async_copy(ref, ref, sem).wait()

    def load_own(l):
        for k in range(4):
            pltpu.make_async_copy(g_hbm.at[l, blocks[k]], own.at[l, k], load_sem.at[l]).start()

    def send_pair(l, source):
        pieces = ((0, 0, pair_x), (1, 0, pair_x), (1, half, pair_y), (2, half, pair_y),
                  (0, half, pair_rest), (2, 0, pair_rest), (3, 0, pair_rest), (3, half, pair_rest))
        for k, row, recv in pieces:
            part = pl.ds(row, half)
            remote(source(k).at[part], peer.at[l, k, part], pair_send.at[l], recv.at[l], {'dp': dc}).start()

    def from_hbm(l):
        return lambda k: g_hbm.at[l, blocks[k] + dc - d]

    def x1(l):
        return remote(own.at[l, 0:2, 0:half], in1x.at[l], x1_send.at[l], x1_recv.at[l], {'dp': dx})

    def y1(l):
        return remote(own.at[l, 1:3, half:rows], in1y.at[l], y1_send.at[l], y1_recv.at[l], {'dp': dy})

    def y2(l):
        return remote(own.at[l, 2, 0:half], in2.at[l, 0], y2_send.at[l], y2_recv.at[l], {'dp': dy})

    def x2(l):
        return remote(own.at[l, 0, half:rows], in2.at[l, 1], x2_send.at[l], x2_recv.at[l], {'dp': dx})

    def total(buf):
        acc = buf[0]
        for j in range(1, buf.shape[0]):
            acc = acc + buf[j]
        return acc

    def column(row):
        return jnp.transpose(jnp.broadcast_to(row, (LANES, LANES)))[0:rows]

    def fold(values):
        acc = values[:, 0:LANES]
        for t in range(1, cols // LANES):
            acc = acc + values[:, t * LANES:(t + 1) * LANES]
        return acc

    small = ((r_hbm, r_buf), (c_hbm, c_buf), (n_hbm, n_buf), (ng_hbm, ng_buf), (v_hbm, v_buf))
    for k in range(4):
        pltpu.make_async_copy(g_hbm.at[0, blocks[k] + dc - d], own.at[last, k], load_sem.at[last]).start()
    for l in range(AHEAD):
        load_own(l)
    for i, (src, dst) in enumerate(small):
        pltpu.make_async_copy(src, dst, small_sem.at[i]).start()

    barrier = pltpu.get_barrier_semaphore()
    everyone = d_peers + column_peers
    for where in everyone:
        pl.semaphore_signal(barrier, inc=1, device_id=where, device_id_type=MESH)
    pl.semaphore_wait(barrier, len(everyone))
    drain(own.at[last], load_sem.at[last])
    send_pair(0, lambda k: own.at[last, k])
    for l in range(1, AHEAD):
        send_pair(l, from_hbm(l))

    def norm_split():
        for i, (src, dst) in enumerate(small):
            pltpu.make_async_copy(src, dst, small_sem.at[i]).wait()
        r_pad[...] = jnp.zeros_like(r_pad)
        r_pad[:, 0:rows] = r_buf[...]
        h_out[...] = jnp.zeros_like(h_out)
        k_all[...] = jnp.zeros_like(k_all)
        for k in range(ds):
            h_out[k // 2, k % 2, :, 0:rows] = ng_buf[:, k * rows:(k + 1) * rows]
        remote(h_out.at[:, 1 - core], h_pair, h_send.at[0], h_recv.at[0], {'dp': dc}).start()

    def norm_send():
        remote(h_out.at[:, 1 - core], h_pair, h_send.at[0], h_recv.at[0], {'dp': dc}).wait()
        for k in range(chips):
            h_pair[k] = h_pair[k] + h_out[k, core]
        h_all[chip] = h_pair[chip]
        for e in (dx, dy, dxy):
            remote(h_pair.at[e // 2], h_all.at[chip], h_send.at[1], h_recv.at[1], {'dp': e}).start()

    def layer_sums(values):
        padded = jnp.concatenate([values, jnp.zeros((layers, LANES - rows), jnp.float32)], axis=1)
        return jnp.sum(jnp.transpose(padded), axis=0, keepdims=True)

    def norm_stats():
        drain(h_all.at[0:chips - 1], h_recv.at[1])
        h = total(h_all)[:, 0:rows]
        v_new = DECAY * v_buf[...] + (1.0 - DECAY) * (h * h + EPS_FLOOR)
        v_buf[...] = v_new
        zv = h * lax.rsqrt(v_new)
        nv = n_buf[...]
        k_all[d, :, 0:layers] = layer_sums(zv * zv)
        k_all[d, :, LANES:LANES + layers] = layer_sums(nv * nv)
        spread(k_all.at[d], k_send, k_recv, d_peers)

    def norm_update():
        drain(k_all.at[0:ds - 1], k_recv)
        acc = total(k_all)
        z_sq, n_sq = acc[:, 0:layers], acc[:, LANES:LANES + layers]
        clip = jnp.maximum(1.0, jnp.sqrt(z_sq / rows_total) / CLIP_LIMIT)
        scale = lr_ref[0, 0] * jnp.maximum(SCALE_FLOOR, jnp.sqrt(n_sq / rows_total))
        clip = jnp.transpose(jnp.broadcast_to(clip, (LANES, layers)))[:, 0:rows]
        scale = jnp.transpose(jnp.broadcast_to(scale, (LANES, layers)))[:, 0:rows]
        zv = total(h_all)[:, 0:rows] * lax.rsqrt(v_buf[...])
        n_buf[...] = n_buf[...] - scale * (zv / clip)

    def stage_combine(l):
        drain(own.at[l], load_sem.at[l])
        drain(in1x.at[l], pair_x.at[l])
        own[l, 0:2, 0:half] = own[l, 0:2, 0:half] + peer[l, 0:2, 0:half]
        x1(l).start()
        drain(in1y.at[l], pair_y.at[l])
        own[l, 1:3, half:rows] = own[l, 1:3, half:rows] + peer[l, 1:3, half:rows]
        y1(l).start()
        drain(peer.at[l, 0:2], pair_rest.at[l])
        own[l, 0, half:rows] = own[l, 0, half:rows] + peer[l, 0, half:rows]
        own[l, 2, 0:half] = own[l, 2, 0:half] + peer[l, 2, 0:half]
        own[l, 3] = own[l, 3] + peer[l, 3]

    def stage_forward(l):
        x1(l).wait_recv()
        own[l, 2, 0:half] = own[l, 2, 0:half] + in1x[l, 1]
        y1(l).wait_recv()
        own[l, 0, half:rows] = own[l, 0, half:rows] + in1y[l, 0]
        y2(l).start()
        own[l, 3, 0:half] = own[l, 3, 0:half] + in1x[l, 0]
        x2(l).start()
        own[l, 3, half:rows] = own[l, 3, half:rows] + in1y[l, 1]

    def stage_stats(l):
        y2(l).wait_recv()
        x2(l).wait_recv()
        g = own[l, 3] + in2[l].reshape(rows, cols)
        own[l, 3] = g
        q = g * g + EPS_FLOOR
        col = jnp.sum(q, axis=0, keepdims=True)
        c_pair[l, core] = col
        c_last[d] = col
        p = jnp.concatenate([fold(q), jnp.zeros((LANES - rows, LANES), jnp.float32)], axis=0)
        r_all[l, z] = jnp.sum(jnp.transpose(p), axis=0, keepdims=True)

        @pl.when(l < last)
        def _():
            spread(c_pair.at[l, core], cp_send.at[l], cp_recv.at[l], [{'dp': dc}])

        @pl.when(l == last)
        def _():
            spread(c_last.at[d], c_send.at[l], c_recv.at[l], d_peers)

        spread(r_all.at[l, z], r_send.at[l], r_recv.at[l], z_peers)

    def stage_columns(l):
        remote(c_pair.at[l, core], c_pair.at[l, core], cp_send.at[l], cp_recv.at[l], {'dp': dc}).wait()
        c_all[l, chip] = c_pair[l, 0] + c_pair[l, 1]
        spread(c_all.at[l, chip], c_send.at[l], c_recv.at[l], plane_peers)

    def stage_moments(l):
        @pl.when(l < last)
        def _():
            drain(c_all.at[l, 0:chips - 1], c_recv.at[l])

        @pl.when(l == last)
        def _():
            drain(c_last.at[0:ds - 1], c_recv.at[l])
            for k in range(chips):
                c_all[l, k] = c_last[2 * k] + c_last[2 * k + 1]

        if zs > 1:
            drain(r_all.at[l, 0:zs - 1], r_recv.at[l])
        drain(w_buf.at[l], w_sem.at[l])
        r_new = DECAY * r_pad[pl.ds(l, 1)] + (1.0 - DECAY) * (total(r_all.at[l]) / cols_total)
        c_new = DECAY * c_buf[pl.ds(l, 1)] + (1.0 - DECAY) * (total(c_all.at[l]) / rows_total)
        r_pad[pl.ds(l, 1)] = r_new
        r_buf[pl.ds(l, 1)] = r_new[:, 0:rows]
        c_buf[pl.ds(l, 1)] = c_new
        a = column(lax.rsqrt(r_new))
        b = lax.rsqrt(c_new)
        acc = jnp.zeros((1, LANES), jnp.float32)
        w_acc = jnp.zeros((1, LANES), jnp.float32)
        for t in range(cols // LANES):
            sl = slice(t * LANES, (t + 1) * LANES)
            u = own[l, 3, :, sl] * a * b[:, sl]
            acc = acc + jnp.sum(u * u, axis=0, keepdims=True)
            w = w_buf[l, :, sl]
            w_acc = w_acc + jnp.sum(w * w, axis=0, keepdims=True)
        lane = lax.broadcasted_iota(jnp.int32, (1, LANES), 1)
        row = jnp.where(lane == 0, jnp.sum(acc, axis=1, keepdims=True), 0.0)
        row = jnp.where(lane == 1, jnp.sum(w_acc, axis=1, keepdims=True), row)
        row = jnp.where(lane == 2, jnp.sum(r_new, axis=1, keepdims=True), row)
        s_all[l, 2 * z + core] = row
        spread(s_all.at[l, 2 * z + core], s_send.at[l], s_recv.at[l], column_peers)

    def stage_gather(l):
        drain(s_all.at[l, 0:2 * zs - 1], s_recv.at[l])
        t_all[l, chip] = total(s_all.at[l])
        spread(t_all.at[l, chip], t_send.at[l], t_recv.at[l], plane_peers)

    def stage_update(l):
        drain(t_all.at[l, 0:chips - 1], t_recv.at[l])
        sums = total(t_all.at[l])
        count = rows_total * cols_total
        r_mean = sums[:, 2:3] / (rows_total * zs)
        u_rms = jnp.sqrt(sums[:, 0:1] / count * r_mean)
        clip = jnp.maximum(1.0, u_rms / CLIP_LIMIT)
        scale = lr_ref[0, 0] * jnp.maximum(SCALE_FLOOR, jnp.sqrt(sums[:, 1:2] / count))
        a = column(lax.rsqrt(r_pad[pl.ds(l, 1)] / r_mean))
        b = lax.rsqrt(c_buf[pl.ds(l, 1)]) / clip
        for t in range(cols // LANES):
            sl = slice(t * LANES, (t + 1) * LANES)
            u = own[l, 3, :, sl] * a * b[:, sl]
            w_buf[l, :, sl] = w_buf[l, :, sl] - scale * u

    def drain_bulk(l):
        drain(peer.at[l], pair_send.at[l])
        x1(l).wait_send()
        y1(l).wait_send()
        x2(l).wait_send()
        y2(l).wait_send()

    def drain_sums(l):
        if zs > 1:
            drain(r_all.at[l, 0:zs - 1], r_send.at[l])

        @pl.when(l < last)
        def _():
            drain(c_all.at[l, 0:chips - 1], c_send.at[l])

        @pl.when(l == last)
        def _():
            drain(c_last.at[0:ds - 1], c_send.at[l])

        drain(s_all.at[l, 0:2 * zs - 1], s_send.at[l])
        drain(t_all.at[l, 0:chips - 1], t_send.at[l])

    def at(i, lag, stage):
        @pl.when((i >= lag) & (i < layers + lag))
        def _():
            stage(i - lag)

    def once(i, when, stage):
        @pl.when(i == when)
        def _():
            stage()

    def body(i, carry):
        @pl.when(i + AHEAD < layers)
        def _():
            load_own(i + AHEAD)
            send_pair(i + AHEAD, from_hbm(i + AHEAD))

        @pl.when(i < layers)
        def _():
            stage_combine(i)
            pltpu.make_async_copy(w_hbm.at[i], w_buf.at[i], w_sem.at[i]).start()

        at(i, 1, stage_forward)
        once(i, 1, norm_split)
        once(i, 2, norm_send)

        @pl.when((i >= 3) & (i < last + 3))
        def _():
            stage_columns(i - 3)

        at(i, 4, stage_moments)
        at(i, 5, stage_gather)
        at(i, 6, stage_update)
        at(i, 4, drain_bulk)
        at(i, 7, drain_sums)
        once(i, 4, norm_stats)
        once(i, 6, norm_update)
        at(i, 2, stage_stats)
        return carry

    lax.fori_loop(0, layers + 6, body, 0)
    for l in range(last, layers):
        drain_sums(l)
    drain(h_all.at[0:chips - 1], h_send.at[1])
    drain(k_all.at[0:ds - 1], k_send)


def write_kernel(*refs):
    count = len(refs) // 2
    pairs = list(zip(refs[:count], refs[count:2 * count]))
    sem = refs[-1]
    for i, (src, dst) in enumerate(pairs):
        pltpu.make_async_copy(src, dst, sem.at[i]).start()
    for i, (src, dst) in enumerate(pairs):
        pltpu.make_async_copy(src, dst, sem.at[i]).wait()


def write_out(arrays):
    return pl.pallas_call(
        write_kernel,
        out_shape=[jax.ShapeDtypeStruct(a.shape, a.dtype) for a in arrays],
        in_specs=[pl.BlockSpec(memory_space=pltpu.MemorySpace.VMEM)] * len(arrays),
        out_specs=[pl.BlockSpec(memory_space=pltpu.MemorySpace.HBM)] * len(arrays),
        scratch_shapes=[pltpu.SemaphoreType.DMA((len(arrays),))],
        compiler_params=pltpu.CompilerParams(vmem_limit_bytes=1 << 20),
        name='write_out',
    )(*arrays)


def solution(mesh):
    ds = mesh.shape['dp']
    zs = mesh.shape['model']

    def local_step(weight, grad_parts, row_stat, col_stat, norm_scale, norm_grads, norm_stat, learn_rate):
        layers, rows, cols = weight.shape
        half = rows // 2
        f32 = jnp.float32
        grads = grad_parts.reshape(layers, ds, rows, cols)
        any_spec = pl.BlockSpec(memory_space=pltpu.MemorySpace.HBM)
        dma = pltpu.SemaphoreType.DMA
        outs = pl.pallas_call(
            step_kernel,
            out_shape=[pltpu.VMEM(a.shape, f32) for a in (weight, row_stat, col_stat, norm_scale, norm_stat)],
            in_specs=[any_spec] * 7 + [pl.BlockSpec(memory_space=pltpu.SMEM)],
            out_specs=[pl.BlockSpec(memory_space=pltpu.MemorySpace.VMEM)] * 5,
            scratch_shapes=[
                pltpu.VMEM((layers, 4, rows, cols), f32),
                pltpu.VMEM((layers, 4, rows, cols), f32),
                pltpu.VMEM((layers, 2, half, cols), f32),
                pltpu.VMEM((layers, 2, half, cols), f32),
                pltpu.VMEM((layers, 2, half, cols), f32),
                pltpu.VMEM(norm_grads.shape, f32),
                pltpu.VMEM((layers, LANES), f32),
                pltpu.VMEM((layers, zs, 1, LANES), f32),
                pltpu.VMEM((layers, 2, 1, cols), f32),
                pltpu.VMEM((layers, ds // 2, 1, cols), f32),
                pltpu.VMEM((ds, 1, cols), f32),
                pltpu.VMEM((layers, 2 * zs, 1, LANES), f32),
                pltpu.VMEM((layers, ds // 2, 1, LANES), f32),
                pltpu.VMEM((ds // 2, 2, layers, LANES), f32),
                pltpu.VMEM((ds // 2, layers, LANES), f32),
                pltpu.VMEM((ds // 2, layers, LANES), f32),
                pltpu.VMEM((ds, 1, 2 * LANES), f32),
                *[dma((layers,))] * 24,
                dma((5,)), dma((2,)), dma((2,)), dma, dma,
            ],
            compiler_params=pltpu.CompilerParams(collective_id=0, has_side_effects=True, vmem_limit_bytes=54 * 1000 * 1000),
            name='adafactor_step',
        )(weight, grads, row_stat, col_stat, norm_scale, norm_grads, norm_stat, learn_rate.reshape(1, 1))
        return write_out(outs)

    mat_spec = P(None, 'dp', 'model')
    row_spec = P(None, 'dp')
    col_spec = P(None, 'model')
    return jax.shard_map(local_step, mesh=mesh, in_specs=(mat_spec, mat_spec, row_spec, col_spec, row_spec, row_spec, row_spec, P()), out_specs=(mat_spec, row_spec, col_spec, row_spec, row_spec), check_vma=False)
```

```python
import functools

import jax
import jax.numpy as jnp
from jax import lax
from jax.experimental import pallas as pl
from jax.experimental.pallas import tpu as pltpu
from jax.sharding import PartitionSpec as P

STEP_COUNT = 4
DECAY_POWER = 0.8
EPS_FLOOR = 1e-30
SCALE_FLOOR = 1e-3
CLIP_LIMIT = 1.0
DECAY = 1.0 - STEP_COUNT ** -DECAY_POWER
MESH = pl.DeviceIdType.MESH
LANES = 128
AHEAD = 2


def step_kernel(w_hbm, g_hbm, r_hbm, c_hbm, n_hbm, ng_hbm, v_hbm, lr_ref,
                w_buf, r_buf, c_buf, n_buf, v_buf,
                own, peer, in1x, in1y, in2, ng_buf, r_pad,
                r_all, c_pair, c_all, c_last, s_all, t_all, h_out, h_pair, h_all, k_all,
                load_sem, pair_send, pair_x, pair_y, pair_rest,
                one_send, x1_recv, y1_recv, two_send, x2_recv, y2_recv,
                r_send, r_recv, cp_send, cp_recv, c_send, c_recv, s_send, s_recv, t_send, t_recv, w_sem,
                small_sem, h_send, h_recv, k_send, k_recv, last_send, last_recv):
    layers, _, rows, cols = own.shape
    half = rows // 2
    last = layers - 1
    zs, ds = r_all.shape[1], c_last.shape[0]
    chips = ds // 2
    rows_total, cols_total = rows * ds, cols * zs
    z = lax.axis_index('model')
    d = lax.axis_index('dp')
    chip, core = lax.div(d, 2), lax.rem(d, 2)
    dx = d + 2 - 4 * lax.rem(chip, 2)
    dy = d + 4 - 8 * lax.div(d, 4)
    dxy = dx + dy - d
    dc = d + 1 - 2 * core
    blocks = (dx, dxy, dy, d)
    z_peers = [{'model': lax.rem(z + j, zs)} for j in range(1, zs)]
    d_peers = [{'dp': e} for e in (dc, dx, dx + dc - d, dy, dy + dc - d, dxy, dxy + dc - d)]
    column_peers = [{'dp': dc}] + [{'model': p['model'], 'dp': e} for p in z_peers for e in (d, dc)]
    plane_peers = [{'dp': e} for e in (dx, dy, dxy)]

    def ring(sem, l):
        return sem.at[lax.rem(l, sem.shape[0])]

    def remote(src, dst, send, recv, where):
        return pltpu.make_async_remote_copy(src_ref=src, dst_ref=dst, send_sem=send, recv_sem=recv,
                                            device_id=where, device_id_type=MESH)

    def spread(ref, send, recv, peers):
        for where in peers:
            remote(ref, ref, send, recv, where).start()

    def drain(ref, sem):
        pltpu.make_async_copy(ref, ref, sem).wait()

    def load_own(l):
        for k in range(4):
            pltpu.make_async_copy(g_hbm.at[l, blocks[k]], own.at[l, k], ring(load_sem, l)).start()

    def send_pair(l, source):
        pieces = ((0, 0, pair_x), (1, 0, pair_x), (1, half, pair_y), (2, half, pair_y),
                  (0, half, pair_rest), (2, 0, pair_rest), (3, 0, pair_rest), (3, half, pair_rest))
        for k, row, recv in pieces:
            part = pl.ds(row, half)
            remote(source(k).at[part], peer.at[l, k, part], ring(pair_send, l), ring(recv, l), {'dp': dc}).start()

    def from_hbm(l):
        return lambda k: g_hbm.at[l, blocks[k] + dc - d]

    def x1(l):
        return remote(own.at[l, 0:2, 0:half], in1x.at[l], ring(one_send, l), ring(x1_recv, l), {'dp': dx})

    def y1(l):
        return remote(own.at[l, 1:3, half:rows], in1y.at[l], ring(one_send, l), ring(y1_recv, l), {'dp': dy})

    def y2(l):
        return remote(own.at[l, 2, 0:half], in2.at[l, 0], ring(two_send, l), ring(y2_recv, l), {'dp': dy})

    def x2(l):
        return remote(own.at[l, 0, half:rows], in2.at[l, 1], ring(two_send, l), ring(x2_recv, l), {'dp': dx})

    def total(buf):
        acc = buf[0]
        for j in range(1, buf.shape[0]):
            acc = acc + buf[j]
        return acc

    def column(row):
        return jnp.transpose(jnp.broadcast_to(row, (LANES, LANES)))[0:rows]

    def fold(values):
        acc = values[:, 0:LANES]
        for t in range(1, cols // LANES):
            acc = acc + values[:, t * LANES:(t + 1) * LANES]
        return acc

    small = ((r_hbm, r_buf), (c_hbm, c_buf), (n_hbm, n_buf), (ng_hbm, ng_buf), (v_hbm, v_buf))
    for k in range(4):
        pltpu.make_async_copy(g_hbm.at[0, blocks[k] + dc - d], own.at[last, k], load_sem.at[AHEAD]).start()
    for l in range(AHEAD):
        load_own(l)
    for i, (src, dst) in enumerate(small):
        pltpu.make_async_copy(src, dst, small_sem.at[i]).start()

    barrier = pltpu.get_barrier_semaphore()
    everyone = d_peers + column_peers
    for where in everyone:
        pl.semaphore_signal(barrier, inc=1, device_id=where, device_id_type=MESH)
    pl.semaphore_wait(barrier, len(everyone))
    drain(own.at[last], load_sem.at[AHEAD])
    send_pair(0, lambda k: own.at[last, k])
    for l in range(1, AHEAD):
        send_pair(l, from_hbm(l))

    def norm_split():
        for i, (src, dst) in enumerate(small):
            pltpu.make_async_copy(src, dst, small_sem.at[i]).wait()
        r_pad[...] = jnp.zeros_like(r_pad)
        r_pad[:, 0:rows] = r_buf[...]
        h_out[...] = jnp.zeros_like(h_out)
        k_all[...] = jnp.zeros_like(k_all)
        for k in range(ds):
            h_out[k // 2, k % 2, :, 0:rows] = ng_buf[:, k * rows:(k + 1) * rows]
        remote(h_out.at[:, 1 - core], h_pair, h_send.at[0], h_recv.at[0], {'dp': dc}).start()

    def norm_send():
        remote(h_out.at[:, 1 - core], h_pair, h_send.at[0], h_recv.at[0], {'dp': dc}).wait()
        for k in range(chips):
            h_pair[k] = h_pair[k] + h_out[k, core]
        h_all[chip] = h_pair[chip]
        for e in (dx, dy, dxy):
            remote(h_pair.at[lax.div(e, 2)], h_all.at[chip], h_send.at[1], h_recv.at[1], {'dp': e}).start()

    def layer_sums(values):
        padded = jnp.concatenate([values, jnp.zeros((layers, LANES - rows), jnp.float32)], axis=1)
        return jnp.sum(jnp.transpose(padded), axis=0, keepdims=True)

    def norm_stats():
        drain(h_all.at[0:chips - 1], h_recv.at[1])
        h = total(h_all)[:, 0:rows]
        v_new = DECAY * v_buf[...] + (1.0 - DECAY) * (h * h + EPS_FLOOR)
        v_buf[...] = v_new
        zv = h * lax.rsqrt(v_new)
        nv = n_buf[...]
        k_all[d, :, 0:layers] = layer_sums(zv * zv)
        k_all[d, :, LANES:LANES + layers] = layer_sums(nv * nv)
        spread(k_all.at[d], k_send, k_recv, d_peers)

    def norm_update():
        drain(k_all.at[0:ds - 1], k_recv)
        acc = total(k_all)
        z_sq, n_sq = acc[:, 0:layers], acc[:, LANES:LANES + layers]
        clip = jnp.maximum(1.0, jnp.sqrt(z_sq / rows_total) / CLIP_LIMIT)
        scale = lr_ref[0, 0] * jnp.maximum(SCALE_FLOOR, jnp.sqrt(n_sq / rows_total))
        clip = jnp.transpose(jnp.broadcast_to(clip, (LANES, layers)))[:, 0:rows]
        scale = jnp.transpose(jnp.broadcast_to(scale, (LANES, layers)))[:, 0:rows]
        zv = total(h_all)[:, 0:rows] * lax.rsqrt(v_buf[...])
        n_buf[...] = n_buf[...] - scale * (zv / clip)

    def stage_combine(l):
        drain(own.at[l], ring(load_sem, l))
        drain(in1x.at[l], ring(pair_x, l))
        own[l, 0:2, 0:half] = own[l, 0:2, 0:half] + peer[l, 0:2, 0:half]
        x1(l).start()
        drain(in1y.at[l], ring(pair_y, l))
        own[l, 1:3, half:rows] = own[l, 1:3, half:rows] + peer[l, 1:3, half:rows]
        y1(l).start()
        drain(peer.at[l, 0:2], ring(pair_rest, l))
        own[l, 0, half:rows] = own[l, 0, half:rows] + peer[l, 0, half:rows]
        own[l, 2, 0:half] = own[l, 2, 0:half] + peer[l, 2, 0:half]
        own[l, 3] = own[l, 3] + peer[l, 3]
        drain(peer.at[l], ring(pair_send, l))

    def stage_forward(l):
        x1(l).wait_recv()
        own[l, 2, 0:half] = own[l, 2, 0:half] + in1x[l, 1]
        y1(l).wait_recv()
        own[l, 0, half:rows] = own[l, 0, half:rows] + in1y[l, 0]
        y2(l).start()
        own[l, 3, 0:half] = own[l, 3, 0:half] + in1x[l, 0]
        x2(l).start()
        own[l, 3, half:rows] = own[l, 3, half:rows] + in1y[l, 1]

    def stage_stats(l):
        pltpu.make_async_copy(w_hbm.at[l], w_buf.at[l], ring(w_sem, l)).start()
        y2(l).wait_recv()
        x2(l).wait_recv()
        g = own[l, 3] + in2[l].reshape(rows, cols)
        own[l, 3] = g
        q = g * g + EPS_FLOOR
        col = jnp.sum(q, axis=0, keepdims=True)
        c_pair[l, core] = col
        c_last[d] = col
        p = jnp.concatenate([fold(q), jnp.zeros((LANES - rows, LANES), jnp.float32)], axis=0)
        r_all[l, z] = jnp.sum(jnp.transpose(p), axis=0, keepdims=True)

        @pl.when(l < last)
        def _():
            spread(c_pair.at[l, core], ring(cp_send, l), ring(cp_recv, l), [{'dp': dc}])

        @pl.when(l == last)
        def _():
            spread(c_last.at[d], last_send, last_recv, d_peers)

        spread(r_all.at[l, z], ring(r_send, l), ring(r_recv, l), z_peers)

    def stage_columns(l):
        remote(c_pair.at[l, core], c_pair.at[l, core], ring(cp_send, l), ring(cp_recv, l), {'dp': dc}).wait()
        c_all[l, chip] = c_pair[l, 0] + c_pair[l, 1]
        spread(c_all.at[l, chip], ring(c_send, l), ring(c_recv, l), plane_peers)

    def stage_moments(l):
        @pl.when(l < last)
        def _():
            drain(c_all.at[l, 0:chips - 1], ring(c_recv, l))
            drain(c_all.at[l, 0:chips - 1], ring(c_send, l))

        @pl.when(l == last)
        def _():
            drain(c_last.at[0:ds - 1], last_recv)
            for k in range(chips):
                c_all[l, k] = c_last[2 * k] + c_last[2 * k + 1]

        if zs > 1:
            drain(r_all.at[l, 0:zs - 1], ring(r_recv, l))
            drain(r_all.at[l, 0:zs - 1], ring(r_send, l))
        drain(w_buf.at[l], ring(w_sem, l))
        r_new = DECAY * r_pad[pl.ds(l, 1)] + (1.0 - DECAY) * (total(r_all.at[l]) / cols_total)
        c_new = DECAY * c_buf[pl.ds(l, 1)] + (1.0 - DECAY) * (total(c_all.at[l]) / rows_total)
        r_pad[pl.ds(l, 1)] = r_new
        r_buf[pl.ds(l, 1)] = r_new[:, 0:rows]
        c_buf[pl.ds(l, 1)] = c_new
        a = column(lax.rsqrt(r_new))
        b = lax.rsqrt(c_new)
        acc = jnp.zeros((1, LANES), jnp.float32)
        w_acc = jnp.zeros((1, LANES), jnp.float32)
        for t in range(cols // LANES):
            sl = slice(t * LANES, (t + 1) * LANES)
            u = own[l, 3, :, sl] * a * b[:, sl]
            acc = acc + jnp.sum(u * u, axis=0, keepdims=True)
            w = w_buf[l, :, sl]
            w_acc = w_acc + jnp.sum(w * w, axis=0, keepdims=True)
        lane = lax.broadcasted_iota(jnp.int32, (1, LANES), 1)
        row = jnp.where(lane == 0, jnp.sum(acc, axis=1, keepdims=True), 0.0)
        row = jnp.where(lane == 1, jnp.sum(w_acc, axis=1, keepdims=True), row)
        row = jnp.where(lane == 2, jnp.sum(r_new, axis=1, keepdims=True), row)
        s_all[l, 2 * z + core] = row
        spread(s_all.at[l, 2 * z + core], ring(s_send, l), ring(s_recv, l), column_peers)

    def stage_gather(l):
        drain(s_all.at[l, 0:2 * zs - 1], ring(s_recv, l))
        drain(s_all.at[l, 0:2 * zs - 1], ring(s_send, l))
        t_all[l, chip] = total(s_all.at[l])
        spread(t_all.at[l, chip], ring(t_send, l), ring(t_recv, l), plane_peers)

    def stage_update(l):
        drain(t_all.at[l, 0:chips - 1], ring(t_recv, l))
        drain(t_all.at[l, 0:chips - 1], ring(t_send, l))
        sums = total(t_all.at[l])
        count = rows_total * cols_total
        r_mean = sums[:, 2:3] / (rows_total * zs)
        u_rms = jnp.sqrt(sums[:, 0:1] / count * r_mean)
        clip = jnp.maximum(1.0, u_rms / CLIP_LIMIT)
        scale = lr_ref[0, 0] * jnp.maximum(SCALE_FLOOR, jnp.sqrt(sums[:, 1:2] / count))
        a = column(lax.rsqrt(r_pad[pl.ds(l, 1)] / r_mean))
        b = lax.rsqrt(c_buf[pl.ds(l, 1)]) / clip
        for t in range(cols // LANES):
            sl = slice(t * LANES, (t + 1) * LANES)
            u = own[l, 3, :, sl] * a * b[:, sl]
            w_buf[l, :, sl] = w_buf[l, :, sl] - scale * u

    def drain_bulk(l):
        drain(in1x.at[0:2], ring(one_send, l))
        drain(in2.at[l], ring(two_send, l))

    def at(i, lag, stage):
        @pl.when((i >= lag) & (i < layers + lag))
        def _():
            stage(i - lag)

    def once(i, when, stage):
        @pl.when(i == when)
        def _():
            stage()

    def body(i, carry):
        @pl.when(i + AHEAD < layers)
        def _():
            load_own(i + AHEAD)
            send_pair(i + AHEAD, from_hbm(i + AHEAD))

        @pl.when(i < layers)
        def _():
            stage_combine(i)

        at(i, 1, stage_forward)
        once(i, 1, norm_split)
        once(i, 2, norm_send)

        @pl.when((i >= 3) & (i < last + 3))
        def _():
            stage_columns(i - 3)

        at(i, 4, stage_moments)
        at(i, 5, stage_gather)
        at(i, 6, stage_update)
        at(i, 4, drain_bulk)
        once(i, 4, norm_stats)
        once(i, 6, norm_update)
        at(i, 2, stage_stats)
        return carry

    lax.fori_loop(0, layers + 6, body, 0)
    drain(c_last.at[0:ds - 1], last_send)
    drain(h_all.at[0:chips - 1], h_send.at[1])
    drain(k_all.at[0:ds - 1], k_send)


def write_kernel(*refs):
    count = len(refs) // 2
    pairs = list(zip(refs[:count], refs[count:2 * count]))
    sem = refs[-1]
    for i, (src, dst) in enumerate(pairs):
        pltpu.make_async_copy(src, dst, sem.at[i]).start()
    for i, (src, dst) in enumerate(pairs):
        pltpu.make_async_copy(src, dst, sem.at[i]).wait()


def write_out(arrays):
    return pl.pallas_call(
        write_kernel,
        out_shape=[jax.ShapeDtypeStruct(a.shape, a.dtype) for a in arrays],
        in_specs=[pl.BlockSpec(memory_space=pltpu.MemorySpace.VMEM)] * len(arrays),
        out_specs=[pl.BlockSpec(memory_space=pltpu.MemorySpace.HBM)] * len(arrays),
        scratch_shapes=[pltpu.SemaphoreType.DMA((len(arrays),))],
        compiler_params=pltpu.CompilerParams(vmem_limit_bytes=1 << 20),
        name='write_out',
    )(*arrays)


def solution(mesh):
    ds = mesh.shape['dp']
    zs = mesh.shape['model']

    def local_step(weight, grad_parts, row_stat, col_stat, norm_scale, norm_grads, norm_stat, learn_rate):
        layers, rows, cols = weight.shape
        half = rows // 2
        f32 = jnp.float32
        grads = grad_parts.reshape(layers, ds, rows, cols)
        any_spec = pl.BlockSpec(memory_space=pltpu.MemorySpace.HBM)
        dma = pltpu.SemaphoreType.DMA
        outs = pl.pallas_call(
            step_kernel,
            out_shape=[pltpu.VMEM(a.shape, f32) for a in (weight, row_stat, col_stat, norm_scale, norm_stat)],
            in_specs=[any_spec] * 7 + [pl.BlockSpec(memory_space=pltpu.SMEM)],
            out_specs=[pl.BlockSpec(memory_space=pltpu.MemorySpace.VMEM)] * 5,
            scratch_shapes=[
                pltpu.VMEM((layers, 4, rows, cols), f32),
                pltpu.VMEM((layers, 4, rows, cols), f32),
                pltpu.VMEM((layers, 2, half, cols), f32),
                pltpu.VMEM((layers, 2, half, cols), f32),
                pltpu.VMEM((layers, 2, half, cols), f32),
                pltpu.VMEM(norm_grads.shape, f32),
                pltpu.VMEM((layers, LANES), f32),
                pltpu.VMEM((layers, zs, 1, LANES), f32),
                pltpu.VMEM((layers, 2, 1, cols), f32),
                pltpu.VMEM((layers, ds // 2, 1, cols), f32),
                pltpu.VMEM((ds, 1, cols), f32),
                pltpu.VMEM((layers, 2 * zs, 1, LANES), f32),
                pltpu.VMEM((layers, ds // 2, 1, LANES), f32),
                pltpu.VMEM((ds // 2, 2, layers, LANES), f32),
                pltpu.VMEM((ds // 2, layers, LANES), f32),
                pltpu.VMEM((ds // 2, layers, LANES), f32),
                pltpu.VMEM((ds, 1, 2 * LANES), f32),
                *[dma((n,)) for n in (4, 4, 8, 8, 8, 4, 4, 4, 4, 4, 4, 2, 4, 2, 2, 2, 4, 2, 4, 2, 4, 4)],
                dma((5,)), dma((2,)), dma((2,)), dma, dma, dma, dma,
            ],
            compiler_params=pltpu.CompilerParams(collective_id=0, has_side_effects=True, vmem_limit_bytes=54 * 1000 * 1000),
            name='adafactor_step',
        )(weight, grads, row_stat, col_stat, norm_scale, norm_grads, norm_stat, learn_rate.reshape(1, 1))
        return write_out(outs)

    mat_spec = P(None, 'dp', 'model')
    row_spec = P(None, 'dp')
    col_spec = P(None, 'model')
    return jax.shard_map(local_step, mesh=mesh, in_specs=(mat_spec, mat_spec, row_spec, col_spec, row_spec, row_spec, row_spec, P()), out_specs=(mat_spec, row_spec, col_spec, row_spec, row_spec), check_vma=False)
```

```python
import functools

import jax
import jax.numpy as jnp
from jax import lax
from jax.experimental import pallas as pl
from jax.experimental.pallas import tpu as pltpu
from jax.sharding import PartitionSpec as P

STEP_COUNT = 4
DECAY_POWER = 0.8
EPS_FLOOR = 1e-30
SCALE_FLOOR = 1e-3
CLIP_LIMIT = 1.0
DECAY = 1.0 - STEP_COUNT ** -DECAY_POWER
MESH = pl.DeviceIdType.MESH
LANES = 128
AHEAD = 2
DIRECT = 2


def step_kernel(w_hbm, g_hbm, r_hbm, c_hbm, n_hbm, ng_hbm, v_hbm, lr_ref,
                w_buf, r_buf, c_buf, n_buf, v_buf,
                own, peer, in1x, in1y, in2, ng_buf, r_pad,
                r_all, c_mine, c_pair, c_all, c_full, c_last, s_all, t_all, t_last, h_out, h_pair, h_all, k_all,
                load_sem, stage_sem, first_recv, pair_send, pair_recv, one_send, one_recv, two_send, two_recv,
                r_send, r_recv, cp_send, cp_recv, c_send, c_recv, cf_send, cf_recv,
                s_send, s_recv, t_send, t_recv, w_sem,
                cl_send, cl_recv, tl_send, tl_recv, small_sem, h_send, h_recv, k_send, k_recv):
    layers, _, rows, cols = own.shape
    half = rows // 2
    direct, ds = c_last.shape[0], c_last.shape[1]
    late = layers - direct
    zs = r_all.shape[1]
    chips = ds // 2
    rows_total, cols_total = rows * ds, cols * zs
    z = lax.axis_index('model')
    d = lax.axis_index('dp')
    chip, core = lax.div(d, 2), lax.rem(d, 2)
    dx = d + 2 - 4 * lax.rem(chip, 2)
    dy = d + 4 - 8 * lax.div(d, 4)
    dxy = dx + dy - d
    dc = d + 1 - 2 * core
    blocks = (dx, dxy, dy, d)
    z_peers = [{'model': lax.rem(z + j, zs)} for j in range(1, zs)]
    d_peers = [{'dp': e} for e in (dc, dx, dx + dc - d, dy, dy + dc - d, dxy, dxy + dc - d)]
    column_peers = [{'dp': dc}] + [{'model': p['model'], 'dp': e} for p in z_peers for e in (d, dc)]
    plane_peers = [{'dp': e} for e in (dx, dy, dxy)]
    others = [{'model': p['model'], **q} for q in d_peers[::-1] for p in z_peers] + d_peers[::-1] + z_peers

    def ring(sem, l):
        return sem.at[lax.rem(l, sem.shape[0])]

    def remote(src, dst, send, recv, where):
        return pltpu.make_async_remote_copy(src_ref=src, dst_ref=dst, send_sem=send, recv_sem=recv,
                                            device_id=where, device_id_type=MESH)

    def spread(ref, send, recv, peers):
        for where in peers:
            remote(ref, ref, send, recv, where).start()

    def drain(ref, sem):
        pltpu.make_async_copy(ref, ref, sem).wait()

    def load_own(l):
        for k in range(4):
            pltpu.make_async_copy(g_hbm.at[l, blocks[k]], own.at[l, k], ring(load_sem, l)).start()

    def pair_copy(l, k, row, source, recv):
        part = pl.ds(row, half)
        return remote(source.at[part], peer.at[l, k, part], ring(pair_send, l), recv, {'dp': dc})

    def from_hbm(l, k):
        return g_hbm.at[l, blocks[k] + dc - d]

    def send_pair(l):
        for k in range(4):
            remote(from_hbm(l, k), peer.at[l, k], ring(pair_send, l), ring(pair_recv, l), {'dp': dc}).start()

    def x1(l):
        return remote(own.at[l, 0:2, 0:half], in1x.at[l], ring(one_send, l), ring(one_recv, l), {'dp': dx})

    def y1(l):
        return remote(own.at[l, 1:3, half:rows], in1y.at[l], ring(one_send, l), ring(one_recv, l), {'dp': dy})

    def y2(l):
        return remote(own.at[l, 2, 0:half], in2.at[l, 0], ring(two_send, l), ring(two_recv, l), {'dp': dy})

    def x2(l):
        return remote(own.at[l, 0, half:rows], in2.at[l, 1], ring(two_send, l), ring(two_recv, l), {'dp': dx})

    def total(buf):
        parts = [buf[j] for j in range(buf.shape[0])]
        while len(parts) > 1:
            parts = [a + b for a, b in zip(parts[::2], parts[1::2])]
        return parts[0]

    def column(row):
        return jnp.transpose(jnp.broadcast_to(row, (LANES, LANES)))[0:rows]

    def fold(values):
        acc = values[:, 0:LANES]
        for t in range(1, cols // LANES):
            acc = acc + values[:, t * LANES:(t + 1) * LANES]
        return acc

    small = ((r_hbm, r_buf), (c_hbm, c_buf), (n_hbm, n_buf), (ng_hbm, ng_buf), (v_hbm, v_buf))
    groups = (((0, 0), (1, 0)), ((1, half), (2, half)))
    for i, group in enumerate(groups):
        for k, row in group:
            part = pl.ds(row, half)
            pltpu.make_async_copy(from_hbm(0, k).at[part], own.at[layers - 1, i, pl.ds((k - i) * half, half)], stage_sem.at[i]).start()
    for l in range(AHEAD):
        load_own(l)
    for i, (src, dst) in enumerate(small):
        pltpu.make_async_copy(src, dst, small_sem.at[i]).start()

    barrier = pltpu.get_barrier_semaphore()
    known = d_peers + column_peers[1:]
    for where in known:
        pl.semaphore_signal(barrier, inc=1, device_id=where, device_id_type=MESH)
    pl.semaphore_wait(barrier, len(known))
    for i, group in enumerate(groups):
        drain(own.at[layers - 1, i], stage_sem.at[i])
        for k, row in group:
            part = pl.ds(row, half)
            remote(own.at[layers - 1, i, pl.ds((k - i) * half, half)], peer.at[0, k, part],
                   pair_send.at[0], first_recv.at[i], {'dp': dc}).start()
    for k, row in ((0, half), (2, 0), (3, 0), (3, half)):
        pair_copy(0, k, row, from_hbm(0, k), first_recv.at[2]).start()
    for l in range(1, AHEAD):
        send_pair(l)

    def norm_split():
        for i, (src, dst) in enumerate(small):
            pltpu.make_async_copy(src, dst, small_sem.at[i]).wait()
        r_pad[...] = jnp.zeros_like(r_pad)
        r_pad[:, 0:rows] = r_buf[...]
        h_out[...] = jnp.zeros_like(h_out)
        k_all[...] = jnp.zeros_like(k_all)
        for k in range(ds):
            h_out[k // 2, k % 2, :, 0:rows] = ng_buf[:, k * rows:(k + 1) * rows]
        remote(h_out.at[:, 1 - core], h_pair, h_send.at[0], h_recv.at[0], {'dp': dc}).start()

    def norm_send():
        remote(h_out.at[:, 1 - core], h_pair, h_send.at[0], h_recv.at[0], {'dp': dc}).wait()
        for k in range(chips):
            h_pair[k] = h_pair[k] + h_out[k, core]
        h_all[chip] = h_pair[chip]
        for e in (dx, dy, dxy):
            remote(h_pair.at[lax.div(e, 2)], h_all.at[chip], h_send.at[1], h_recv.at[1], {'dp': e}).start()

    def layer_sums(values):
        padded = jnp.concatenate([values, jnp.zeros((layers, LANES - rows), jnp.float32)], axis=1)
        return jnp.sum(jnp.transpose(padded), axis=0, keepdims=True)

    def norm_stats():
        drain(h_all.at[0:chips - 1], h_recv.at[1])
        h = total(h_all)[:, 0:rows]
        v_new = DECAY * v_buf[...] + (1.0 - DECAY) * (h * h + EPS_FLOOR)
        v_buf[...] = v_new
        zv = h * lax.rsqrt(v_new)
        nv = n_buf[...]
        k_all[d, :, 0:layers] = layer_sums(zv * zv)
        k_all[d, :, LANES:LANES + layers] = layer_sums(nv * nv)
        spread(k_all.at[d], k_send, k_recv, d_peers)

    def norm_update():
        drain(k_all.at[0:ds - 1], k_recv)
        acc = total(k_all)
        z_sq, n_sq = acc[:, 0:layers], acc[:, LANES:LANES + layers]
        clip = jnp.maximum(1.0, jnp.sqrt(z_sq / rows_total) / CLIP_LIMIT)
        scale = lr_ref[0, 0] * jnp.maximum(SCALE_FLOOR, jnp.sqrt(n_sq / rows_total))
        clip = jnp.transpose(jnp.broadcast_to(clip, (LANES, layers)))[:, 0:rows]
        scale = jnp.transpose(jnp.broadcast_to(scale, (LANES, layers)))[:, 0:rows]
        zv = total(h_all)[:, 0:rows] * lax.rsqrt(v_buf[...])
        n_buf[...] = n_buf[...] - scale * (zv / clip)

    def combine(l, k, part):
        own[l, k, part] = own[l, k, part] + peer[l, k, part]

    first, second = slice(0, half), slice(half, rows)

    def stage_first():
        drain(own.at[0], load_sem.at[0])
        drain(in1x.at[0], first_recv.at[0])
        combine(0, slice(0, 2), first)
        x1(0).start()
        drain(in1y.at[0], first_recv.at[1])
        combine(0, slice(1, 3), second)
        y1(0).start()
        drain(peer.at[0, 0:2], first_recv.at[2])
        combine(0, 0, second)
        combine(0, 2, first)
        combine(0, 3, slice(0, rows))
        drain(peer.at[0], pair_send.at[0])

    def stage_combine(l):
        drain(own.at[l], ring(load_sem, l))
        drain(peer.at[l], ring(pair_recv, l))
        combine(l, slice(0, 2), first)
        x1(l).start()
        combine(l, slice(1, 3), second)
        y1(l).start()
        combine(l, 0, second)
        combine(l, 2, first)
        combine(l, 3, slice(0, rows))
        drain(peer.at[l], ring(pair_send, l))

    def stage_forward(l):
        drain(in1x.at[0:2], ring(one_recv, l))
        own[l, 2, 0:half] = own[l, 2, 0:half] + in1x[l, 1]
        own[l, 0, half:rows] = own[l, 0, half:rows] + in1y[l, 0]
        y2(l).start()
        own[l, 3, 0:half] = own[l, 3, 0:half] + in1x[l, 0]
        x2(l).start()
        own[l, 3, half:rows] = own[l, 3, half:rows] + in1y[l, 1]

    def stage_stats(l):
        pltpu.make_async_copy(w_hbm.at[l], w_buf.at[l], ring(w_sem, l)).start()
        drain(in2.at[l], ring(two_recv, l))
        g = own[l, 3] + in2[l].reshape(rows, cols)
        own[l, 3] = g
        q = g * g + EPS_FLOOR
        col = jnp.sum(q, axis=0, keepdims=True)

        @pl.when(l < late)
        def _():
            c_mine[l, 0] = col[:, 0:cols // 2]
            c_mine[l, 1] = col[:, cols // 2:cols]

        @pl.when(l >= late)
        def _():
            c_last[l - late, d] = col

        p = jnp.concatenate([fold(q), jnp.zeros((LANES - rows, LANES), jnp.float32)], axis=0)
        r_all[l, z] = jnp.sum(jnp.transpose(p), axis=0, keepdims=True)

        @pl.when(l < late)
        def _():
            pair_columns(l).start()

        @pl.when(l >= late)
        def _():
            e = l - late
            spread(c_last.at[e, d], cl_send.at[e], cl_recv.at[e], d_peers)

        spread(r_all.at[l, z], ring(r_send, l), ring(r_recv, l), z_peers)

    def pair_columns(l):
        return remote(c_mine.at[l, 1 - core], c_pair.at[l], ring(cp_send, l), ring(cp_recv, l), {'dp': dc})

    def full_columns(l):
        return remote(c_full.at[l, core], c_full.at[l, core], ring(cf_send, l), ring(cf_recv, l), {'dp': dc})

    def stage_columns(l):
        pair_columns(l).wait()
        c_all[l, chip] = c_mine[l, core] + c_pair[l]
        spread(c_all.at[l, chip], ring(c_send, l), ring(c_recv, l), plane_peers)

    def stage_share(l):
        drain(c_all.at[l, 0:chips - 1], ring(c_recv, l))
        drain(c_all.at[l, 0:chips - 1], ring(c_send, l))
        c_full[l, core] = total(c_all.at[l])
        full_columns(l).start()

    def stage_moments(l):
        @pl.when(l < late)
        def _():
            full_columns(l).wait()

        @pl.when(l >= late)
        def _():
            e = l - late
            drain(c_last.at[e, 0:ds - 1], cl_recv.at[e])
            drain(c_last.at[e, 0:ds - 1], cl_send.at[e])
            col = total(c_last.at[e])
            c_full[l, 0] = col[:, 0:cols // 2]
            c_full[l, 1] = col[:, cols // 2:cols]

        if zs > 1:
            drain(r_all.at[l, 0:zs - 1], ring(r_recv, l))
            drain(r_all.at[l, 0:zs - 1], ring(r_send, l))
        drain(w_buf.at[l], ring(w_sem, l))
        col = jnp.concatenate([c_full[l, 0], c_full[l, 1]], axis=1)
        r_new = DECAY * r_pad[pl.ds(l, 1)] + (1.0 - DECAY) * (total(r_all.at[l]) / cols_total)
        c_new = DECAY * c_buf[pl.ds(l, 1)] + (1.0 - DECAY) * (col / rows_total)
        r_pad[pl.ds(l, 1)] = r_new
        r_buf[pl.ds(l, 1)] = r_new[:, 0:rows]
        c_buf[pl.ds(l, 1)] = c_new
        a = column(lax.rsqrt(r_new))
        b = lax.rsqrt(c_new)
        acc = jnp.zeros((1, LANES), jnp.float32)
        w_acc = jnp.zeros((1, LANES), jnp.float32)
        for t in range(cols // LANES):
            sl = slice(t * LANES, (t + 1) * LANES)
            u = own[l, 3, :, sl] * a * b[:, sl]
            acc = acc + jnp.sum(u * u, axis=0, keepdims=True)
            w = w_buf[l, :, sl]
            w_acc = w_acc + jnp.sum(w * w, axis=0, keepdims=True)
        lane = lax.broadcasted_iota(jnp.int32, (1, LANES), 1)
        row = jnp.where(lane == 0, jnp.sum(acc, axis=1, keepdims=True), 0.0)
        row = jnp.where(lane == 1, jnp.sum(w_acc, axis=1, keepdims=True), row)
        row = jnp.where(lane == 2, jnp.sum(r_new, axis=1, keepdims=True), row)

        @pl.when(l < late)
        def _():
            s_all[l, 2 * z + core] = row
            spread(s_all.at[l, 2 * z + core], ring(s_send, l), ring(s_recv, l), column_peers)

        @pl.when(l >= late)
        def _():
            e = l - late
            me = ds * z + d
            t_last[e, me] = row
            spread(t_last.at[e, me], tl_send.at[e], tl_recv.at[e], others)

    def stage_gather(l):
        drain(s_all.at[l, 0:2 * zs - 1], ring(s_recv, l))
        drain(s_all.at[l, 0:2 * zs - 1], ring(s_send, l))
        t_all[l, chip] = total(s_all.at[l])
        spread(t_all.at[l, chip], ring(t_send, l), ring(t_recv, l), plane_peers)

    def stage_update(l):
        drain(t_all.at[l, 0:chips - 1], ring(t_recv, l))
        drain(t_all.at[l, 0:chips - 1], ring(t_send, l))
        apply(l, total(t_all.at[l]))

    def stage_final(e):
        drain(t_last.at[e, 0:ds * zs - 1], tl_recv.at[e])
        drain(t_last.at[e, 0:ds * zs - 1], tl_send.at[e])
        apply(e + late, total(t_last.at[e]))

    def apply(l, sums):
        count = rows_total * cols_total
        r_mean = sums[:, 2:3] / (rows_total * zs)
        u_rms = jnp.sqrt(sums[:, 0:1] / count * r_mean)
        clip = jnp.maximum(1.0, u_rms / CLIP_LIMIT)
        scale = lr_ref[0, 0] * jnp.maximum(SCALE_FLOOR, jnp.sqrt(sums[:, 1:2] / count))
        a = column(lax.rsqrt(r_pad[pl.ds(l, 1)] / r_mean))
        b = lax.rsqrt(c_buf[pl.ds(l, 1)]) / clip
        for t in range(cols // LANES):
            sl = slice(t * LANES, (t + 1) * LANES)
            u = own[l, 3, :, sl] * a * b[:, sl]
            w_buf[l, :, sl] = w_buf[l, :, sl] - scale * u

    def drain_bulk(l):
        drain(in1x.at[0:2], ring(one_send, l))
        drain(in2.at[l], ring(two_send, l))

    def at(i, lag, stage, begin=0, end=layers):
        @pl.when((i >= begin + lag) & (i < end + lag))
        def _():
            stage(i - lag)

    def once(i, when, stage):
        @pl.when(i == when)
        def _():
            stage()

    def prefetch(l):
        load_own(l)
        send_pair(l)

    def body(i, carry):
        at(i, -AHEAD, prefetch)
        at(i, 0, stage_combine, 1)
        once(i, 0, stage_first)
        at(i, 1, stage_forward)
        once(i, 1, norm_split)
        once(i, 2, norm_send)
        at(i, 3, stage_columns, 0, late)
        at(i, 4, stage_share, 0, late)
        at(i, 5, stage_moments)
        at(i, 7, stage_gather, 0, late)
        at(i, 8, stage_update, 0, late)
        at(i, 4, drain_bulk)
        once(i, 4, norm_stats)
        once(i, 6, norm_update)
        at(i, 2, stage_stats)
        return carry

    lax.fori_loop(0, late + 8, body, 0)
    for e in range(direct):
        stage_final(e)
    drain(h_all.at[0:chips - 1], h_send.at[1])
    drain(k_all.at[0:ds - 1], k_send)


def write_kernel(*refs):
    count = len(refs) // 2
    pairs = list(zip(refs[:count], refs[count:2 * count]))
    sem = refs[-1]
    for i, (src, dst) in enumerate(pairs):
        pltpu.make_async_copy(src, dst, sem.at[i]).start()
    for i, (src, dst) in enumerate(pairs):
        pltpu.make_async_copy(src, dst, sem.at[i]).wait()


def write_out(arrays):
    return pl.pallas_call(
        write_kernel,
        out_shape=[jax.ShapeDtypeStruct(a.shape, a.dtype) for a in arrays],
        in_specs=[pl.BlockSpec(memory_space=pltpu.MemorySpace.VMEM)] * len(arrays),
        out_specs=[pl.BlockSpec(memory_space=pltpu.MemorySpace.HBM)] * len(arrays),
        scratch_shapes=[pltpu.SemaphoreType.DMA((len(arrays),))],
        compiler_params=pltpu.CompilerParams(vmem_limit_bytes=1 << 20),
        name='write_out',
    )(*arrays)


def solution(mesh):
    ds = mesh.shape['dp']
    zs = mesh.shape['model']

    def local_step(weight, grad_parts, row_stat, col_stat, norm_scale, norm_grads, norm_stat, learn_rate):
        layers, rows, cols = weight.shape
        half = rows // 2
        f32 = jnp.float32
        grads = grad_parts.reshape(layers, ds, rows, cols)
        any_spec = pl.BlockSpec(memory_space=pltpu.MemorySpace.HBM)
        dma = pltpu.SemaphoreType.DMA
        outs = pl.pallas_call(
            step_kernel,
            out_shape=[pltpu.VMEM(a.shape, f32) for a in (weight, row_stat, col_stat, norm_scale, norm_stat)],
            in_specs=[any_spec] * 7 + [pl.BlockSpec(memory_space=pltpu.SMEM)],
            out_specs=[pl.BlockSpec(memory_space=pltpu.MemorySpace.VMEM)] * 5,
            scratch_shapes=[
                pltpu.VMEM((layers, 4, rows, cols), f32),
                pltpu.VMEM((layers, 4, rows, cols), f32),
                pltpu.VMEM((layers, 2, half, cols), f32),
                pltpu.VMEM((layers, 2, half, cols), f32),
                pltpu.VMEM((layers, 2, half, cols), f32),
                pltpu.VMEM(norm_grads.shape, f32),
                pltpu.VMEM((layers, LANES), f32),
                pltpu.VMEM((layers, zs, 1, LANES), f32),
                pltpu.VMEM((layers, 2, 1, cols // 2), f32),
                pltpu.VMEM((layers, 1, cols // 2), f32),
                pltpu.VMEM((layers, ds // 2, 1, cols // 2), f32),
                pltpu.VMEM((layers, 2, 1, cols // 2), f32),
                pltpu.VMEM((DIRECT, ds, 1, cols), f32),
                pltpu.VMEM((layers, 2 * zs, 1, LANES), f32),
                pltpu.VMEM((layers, ds // 2, 1, LANES), f32),
                pltpu.VMEM((DIRECT, ds * zs, 1, LANES), f32),
                pltpu.VMEM((ds // 2, 2, layers, LANES), f32),
                pltpu.VMEM((ds // 2, layers, LANES), f32),
                pltpu.VMEM((ds // 2, layers, LANES), f32),
                pltpu.VMEM((ds, 1, 2 * LANES), f32),
                *[dma((n,)) for n in (3, 2, 3, 3, 4, 4, 4, 4, 4, 3, 6, 2, 2, 2, 4, 2, 4, 3, 6, 2, 4, 3)],
                *[dma((DIRECT,))] * 4, dma((5,)), dma((2,)), dma((2,)), dma, dma,
            ],
            compiler_params=pltpu.CompilerParams(collective_id=0, has_side_effects=True, vmem_limit_bytes=54 * 1000 * 1000),
            name='adafactor_step',
        )(weight, grads, row_stat, col_stat, norm_scale, norm_grads, norm_stat, learn_rate.reshape(1, 1))
        return write_out(outs)

    mat_spec = P(None, 'dp', 'model')
    row_spec = P(None, 'dp')
    col_spec = P(None, 'model')
    return jax.shard_map(local_step, mesh=mesh, in_specs=(mat_spec, mat_spec, row_spec, col_spec, row_spec, row_spec, row_spec, P()), out_specs=(mat_spec, row_spec, col_spec, row_spec, row_spec), check_vma=False)
```

```python
import functools

import jax
import jax.numpy as jnp
from jax import lax
from jax.experimental import pallas as pl
from jax.experimental.pallas import tpu as pltpu
from jax.sharding import PartitionSpec as P

STEP_COUNT = 4
DECAY_POWER = 0.8
EPS_FLOOR = 1e-30
SCALE_FLOOR = 1e-3
CLIP_LIMIT = 1.0
DECAY = 1.0 - STEP_COUNT ** -DECAY_POWER
MESH = pl.DeviceIdType.MESH
LANES = 128
AHEAD = 2
DIRECT = 2


def step_kernel(w_hbm, g_hbm, r_hbm, c_hbm, n_hbm, ng_hbm, v_hbm,
                w_buf, d_buf, r_buf, c_buf, n_buf, dn_buf, v_buf,
                own, peer, in1x, in1y, in2, ng_buf, r_pad, w_sq,
                r_all, c_mine, c_pair, c_all, c_full, c_last, s_all, t_all, t_last, h_out, h_pair, h_all, k_all,
                load_sem, stage_sem, first_recv, pair_send, pair_recv, one_send, one_recv, two_send, two_recv,
                r_send, r_recv, cp_send, cp_recv, c_send, c_recv, cf_send, cf_recv,
                s_send, s_recv, t_send, t_recv, w_sem,
                cl_send, cl_recv, tl_send, tl_recv, small_sem, h_send, h_recv, k_send, k_recv):
    layers, _, rows, cols = own.shape
    half = rows // 2
    last, ds = layers - 1, c_last.shape[0]
    late = layers - DIRECT
    zs = r_all.shape[1]
    chips = ds // 2
    rows_total, cols_total = rows * ds, cols * zs
    z = lax.axis_index('model')
    d = lax.axis_index('dp')
    chip, core = lax.div(d, 2), lax.rem(d, 2)
    dx = d + 2 - 4 * lax.rem(chip, 2)
    dy = d + 4 - 8 * lax.div(d, 4)
    dxy = dx + dy - d
    dc = d + 1 - 2 * core
    blocks = (dx, dxy, dy, d)
    z_peers = [{'model': lax.rem(z + j, zs)} for j in range(1, zs)]
    d_peers = [{'dp': e} for e in (dc, dx, dx + dc - d, dy, dy + dc - d, dxy, dxy + dc - d)]
    column_peers = [{'dp': dc}] + [{'model': p['model'], 'dp': e} for p in z_peers for e in (d, dc)]
    plane_peers = [{'dp': e} for e in (dx, dy, dxy)]
    others = [{'model': p['model'], **q} for q in d_peers[::-1] for p in z_peers] + d_peers[::-1] + z_peers

    def ring(sem, l):
        return sem.at[lax.rem(l, sem.shape[0])]

    def remote(src, dst, send, recv, where):
        return pltpu.make_async_remote_copy(src_ref=src, dst_ref=dst, send_sem=send, recv_sem=recv,
                                            device_id=where, device_id_type=MESH)

    def spread(ref, send, recv, peers):
        for where in peers:
            remote(ref, ref, send, recv, where).start()

    def drain(ref, sem):
        pltpu.make_async_copy(ref, ref, sem).wait()

    def load_own(l):
        for k in range(3):
            pltpu.make_async_copy(g_hbm.at[l, blocks[k]], own.at[l, k], ring(load_sem, l)).start()
        pltpu.make_async_copy(g_hbm.at[l, d], d_buf.at[l], ring(load_sem, l)).start()

    def pair_copy(l, k, row, source, recv):
        part = pl.ds(row, half)
        return remote(source.at[part], peer.at[l, k, part], ring(pair_send, l), recv, {'dp': dc})

    def from_hbm(l, k):
        return g_hbm.at[l, blocks[k] + dc - d]

    def send_pair(l):
        for k in range(4):
            remote(from_hbm(l, k), peer.at[l, k], ring(pair_send, l), ring(pair_recv, l), {'dp': dc}).start()

    def x1(l):
        return remote(own.at[l, 0:2, 0:half], in1x.at[l], ring(one_send, l), ring(one_recv, l), {'dp': dx})

    def y1(l):
        return remote(own.at[l, 1:3, half:rows], in1y.at[l], ring(one_send, l), ring(one_recv, l), {'dp': dy})

    def y2(l):
        return remote(own.at[l, 2, 0:half], in2.at[l, 0], ring(two_send, l), ring(two_recv, l), {'dp': dy})

    def x2(l):
        return remote(own.at[l, 0, half:rows], in2.at[l, 1], ring(two_send, l), ring(two_recv, l), {'dp': dx})

    def total(buf):
        parts = [buf[j] for j in range(buf.shape[0])]
        while len(parts) > 1:
            parts = [a + b for a, b in zip(parts[::2], parts[1::2])]
        return parts[0]

    def column(row):
        return jnp.transpose(jnp.broadcast_to(row, (LANES, LANES)))[0:rows]

    def fold(values):
        acc = values[:, 0:LANES]
        for t in range(1, cols // LANES):
            acc = acc + values[:, t * LANES:(t + 1) * LANES]
        return acc

    small = ((r_hbm, r_buf), (c_hbm, c_buf), (n_hbm, n_buf), (ng_hbm, ng_buf), (v_hbm, v_buf))
    groups = (((0, 0), (1, 0)), ((1, half), (2, half)))
    for i, group in enumerate(groups):
        for k, row in group:
            part = pl.ds(row, half)
            pltpu.make_async_copy(from_hbm(0, k).at[part], own.at[layers - 1, i, pl.ds((k - i) * half, half)], stage_sem.at[i]).start()
    load_own(0)
    for i, (src, dst) in enumerate(small):
        pltpu.make_async_copy(src, dst, small_sem.at[i]).start()

    barrier = pltpu.get_barrier_semaphore()
    known = d_peers + column_peers[1:]
    for where in known:
        pl.semaphore_signal(barrier, inc=1, device_id=where, device_id_type=MESH)
    pl.semaphore_wait(barrier, len(known))
    for i, group in enumerate(groups):
        drain(own.at[layers - 1, i], stage_sem.at[i])
        for k, row in group:
            part = pl.ds(row, half)
            remote(own.at[layers - 1, i, pl.ds((k - i) * half, half)], peer.at[0, k, part],
                   pair_send.at[0], first_recv.at[i], {'dp': dc}).start()
    for k, row in ((0, half), (2, 0), (3, 0), (3, half)):
        pair_copy(0, k, row, from_hbm(0, k), first_recv.at[2]).start()
    for l in range(1, AHEAD):
        send_pair(l)
        load_own(l)

    def norm_split():
        for i, (src, dst) in enumerate(small):
            pltpu.make_async_copy(src, dst, small_sem.at[i]).wait()
        r_pad[...] = jnp.zeros_like(r_pad)
        r_pad[:, 0:rows] = r_buf[...]
        h_out[...] = jnp.zeros_like(h_out)
        k_all[...] = jnp.zeros_like(k_all)
        for k in range(ds):
            h_out[k // 2, k % 2, :, 0:rows] = ng_buf[:, k * rows:(k + 1) * rows]
        remote(h_out.at[:, 1 - core], h_pair, h_send.at[0], h_recv.at[0], {'dp': dc}).start()

    def norm_send():
        remote(h_out.at[:, 1 - core], h_pair, h_send.at[0], h_recv.at[0], {'dp': dc}).wait()
        for k in range(chips):
            h_pair[k] = h_pair[k] + h_out[k, core]
        h_all[chip] = h_pair[chip]
        for e in (dx, dy, dxy):
            remote(h_pair.at[lax.div(e, 2)], h_all.at[chip], h_send.at[1], h_recv.at[1], {'dp': e}).start()

    def layer_sums(values):
        padded = jnp.concatenate([values, jnp.zeros((layers, LANES - rows), jnp.float32)], axis=1)
        return jnp.sum(jnp.transpose(padded), axis=0, keepdims=True)

    def norm_stats():
        drain(h_all.at[0:chips - 1], h_recv.at[1])
        h = total(h_all)[:, 0:rows]
        v_new = DECAY * v_buf[...] + (1.0 - DECAY) * (h * h + EPS_FLOOR)
        v_buf[...] = v_new
        zv = h * lax.rsqrt(v_new)
        nv = n_buf[...]
        k_all[d, :, 0:layers] = layer_sums(zv * zv)
        k_all[d, :, LANES:LANES + layers] = layer_sums(nv * nv)
        spread(k_all.at[d], k_send, k_recv, d_peers)

    def norm_update():
        drain(k_all.at[0:ds - 1], k_recv)
        acc = total(k_all)
        z_sq, n_sq = acc[:, 0:layers], acc[:, LANES:LANES + layers]
        clip = jnp.maximum(1.0, jnp.sqrt(z_sq / rows_total) / CLIP_LIMIT)
        scale = jnp.maximum(SCALE_FLOOR, jnp.sqrt(n_sq / rows_total))
        clip = jnp.transpose(jnp.broadcast_to(clip, (LANES, layers)))[:, 0:rows]
        scale = jnp.transpose(jnp.broadcast_to(scale, (LANES, layers)))[:, 0:rows]
        zv = total(h_all)[:, 0:rows] * lax.rsqrt(v_buf[...])
        dn_buf[...] = scale * (zv / clip)

    def combine(l, k, part):
        own[l, k, part] = own[l, k, part] + peer[l, k, part]

    first, second = slice(0, half), slice(half, rows)

    def stage_first():
        drain(peer.at[0], load_sem.at[0])
        drain(in1x.at[0], first_recv.at[0])
        combine(0, slice(0, 2), first)
        x1(0).start()
        drain(in1y.at[0], first_recv.at[1])
        combine(0, slice(1, 3), second)
        y1(0).start()
        drain(peer.at[0, 0:2], first_recv.at[2])
        combine(0, 0, second)
        combine(0, 2, first)
        d_buf[0] = d_buf[0] + peer[0, 3]
        drain(peer.at[0], pair_send.at[0])

    def stage_combine(l):
        drain(peer.at[l], ring(load_sem, l))
        drain(peer.at[l], ring(pair_recv, l))
        combine(l, slice(0, 2), first)
        x1(l).start()
        combine(l, slice(1, 3), second)
        y1(l).start()
        combine(l, 0, second)
        combine(l, 2, first)
        d_buf[l] = d_buf[l] + peer[l, 3]
        drain(peer.at[l], ring(pair_send, l))

    def stage_forward(l):
        pltpu.make_async_copy(w_hbm.at[l], w_buf.at[l], ring(w_sem, l)).start()
        drain(in1x.at[0:2], ring(one_recv, l))
        own[l, 2, 0:half] = own[l, 2, 0:half] + in1x[l, 1]
        own[l, 0, half:rows] = own[l, 0, half:rows] + in1y[l, 0]
        y2(l).start()
        d_buf[l, 0:half] = d_buf[l, 0:half] + in1x[l, 0]
        x2(l).start()
        d_buf[l, half:rows] = d_buf[l, half:rows] + in1y[l, 1]

    def stage_stats(l):
        drain(w_buf.at[l], ring(w_sem, l))
        w = w_buf[l]
        w_sq[pl.ds(l, 1)] = fold(jnp.sum(w * w, axis=0, keepdims=True))
        drain(in2.at[l], ring(two_recv, l))
        g = d_buf[l] + in2[l].reshape(rows, cols)
        d_buf[l] = g
        q = g * g + EPS_FLOOR
        col = jnp.sum(q, axis=0, keepdims=True)

        @pl.when(l < last)
        def _():
            c_mine[l, 0] = col[:, 0:cols // 2]
            c_mine[l, 1] = col[:, cols // 2:cols]

        @pl.when(l == last)
        def _():
            c_last[d] = col

        p = jnp.concatenate([fold(q), jnp.zeros((LANES - rows, LANES), jnp.float32)], axis=0)
        r_all[l, z] = jnp.sum(jnp.transpose(p), axis=0, keepdims=True)

        @pl.when(l < last)
        def _():
            pair_columns(l).start()

        @pl.when(l == last)
        def _():
            spread(c_last.at[d], cl_send, cl_recv, d_peers)

        spread(r_all.at[l, z], ring(r_send, l), ring(r_recv, l), z_peers)

    def pair_columns(l):
        return remote(c_mine.at[l, 1 - core], c_pair.at[l], ring(cp_send, l), ring(cp_recv, l), {'dp': dc})

    def full_columns(l):
        return remote(c_full.at[l, core], c_full.at[l, core], ring(cf_send, l), ring(cf_recv, l), {'dp': dc})

    def stage_columns(l):
        pair_columns(l).wait()
        c_all[l, chip] = c_mine[l, core] + c_pair[l]
        spread(c_all.at[l, chip], ring(c_send, l), ring(c_recv, l), plane_peers)

    def stage_share(l):
        drain(c_all.at[l, 0:chips - 1], ring(c_recv, l))
        drain(c_all.at[l, 0:chips - 1], ring(c_send, l))
        c_full[l, core] = total(c_all.at[l])
        full_columns(l).start()

    def stage_moments(l):
        @pl.when(l < last)
        def _():
            full_columns(l).wait()

        @pl.when(l == last)
        def _():
            drain(c_last.at[0:ds - 1], cl_recv)
            drain(c_last.at[0:ds - 1], cl_send)
            col = total(c_last)
            c_full[l, 0] = col[:, 0:cols // 2]
            c_full[l, 1] = col[:, cols // 2:cols]

        if zs > 1:
            drain(r_all.at[l, 0:zs - 1], ring(r_recv, l))
            drain(r_all.at[l, 0:zs - 1], ring(r_send, l))
        col = jnp.concatenate([c_full[l, 0], c_full[l, 1]], axis=1)
        r_new = DECAY * r_pad[pl.ds(l, 1)] + (1.0 - DECAY) * (total(r_all.at[l]) / cols_total)
        c_new = DECAY * c_buf[pl.ds(l, 1)] + (1.0 - DECAY) * (col / rows_total)
        r_pad[pl.ds(l, 1)] = r_new
        r_buf[pl.ds(l, 1)] = r_new[:, 0:rows]
        c_buf[pl.ds(l, 1)] = c_new
        a = column(lax.rsqrt(r_new))
        b = lax.rsqrt(c_new)
        acc = jnp.zeros((1, LANES), jnp.float32)
        for t in range(cols // LANES):
            sl = slice(t * LANES, (t + 1) * LANES)
            u = d_buf[l, :, sl] * a * b[:, sl]
            acc = acc + jnp.sum(u * u, axis=0, keepdims=True)
        lane = lax.broadcasted_iota(jnp.int32, (1, LANES), 1)
        row = jnp.where(lane == 0, jnp.sum(acc, axis=1, keepdims=True), 0.0)
        row = jnp.where(lane == 1, jnp.sum(w_sq[pl.ds(l, 1)], axis=1, keepdims=True), row)
        row = jnp.where(lane == 2, jnp.sum(r_new, axis=1, keepdims=True), row)

        @pl.when(l < late)
        def _():
            s_all[l, 2 * z + core] = row
            spread(s_all.at[l, 2 * z + core], ring(s_send, l), ring(s_recv, l), column_peers)

        @pl.when(l >= late)
        def _():
            e = l - late
            me = ds * z + d
            t_last[e, me] = row
            spread(t_last.at[e, me], tl_send.at[e], tl_recv.at[e], others)

    def stage_gather(l):
        drain(s_all.at[l, 0:2 * zs - 1], ring(s_recv, l))
        drain(s_all.at[l, 0:2 * zs - 1], ring(s_send, l))
        t_all[l, chip] = total(s_all.at[l])
        spread(t_all.at[l, chip], ring(t_send, l), ring(t_recv, l), plane_peers)

    def stage_update(l):
        drain(t_all.at[l, 0:chips - 1], ring(t_recv, l))
        drain(t_all.at[l, 0:chips - 1], ring(t_send, l))
        apply(l, total(t_all.at[l]))

    def stage_final(e):
        drain(t_last.at[e, 0:ds * zs - 1], tl_recv.at[e])
        drain(t_last.at[e, 0:ds * zs - 1], tl_send.at[e])
        apply(e + late, total(t_last.at[e]))

    def apply(l, sums):
        count = rows_total * cols_total
        r_mean = sums[:, 2:3] / (rows_total * zs)
        u_rms = jnp.sqrt(sums[:, 0:1] / count * r_mean)
        clip = jnp.maximum(1.0, u_rms / CLIP_LIMIT)
        scale = jnp.maximum(SCALE_FLOOR, jnp.sqrt(sums[:, 1:2] / count))
        a = column(lax.rsqrt(r_pad[pl.ds(l, 1)] / r_mean))
        b = lax.rsqrt(c_buf[pl.ds(l, 1)])
        for t in range(cols // LANES):
            sl = slice(t * LANES, (t + 1) * LANES)
            d_buf[l, :, sl] = d_buf[l, :, sl] * a * (b[:, sl] / clip) * scale

    def drain_bulk(l):
        drain(in1x.at[0:2], ring(one_send, l))
        drain(in2.at[l], ring(two_send, l))

    def at(i, lag, stage, begin=0, end=layers):
        @pl.when((i >= begin + lag) & (i < end + lag))
        def _():
            stage(i - lag)

    def once(i, when, stage):
        @pl.when(i == when)
        def _():
            stage()

    def prefetch(l):
        load_own(l)
        send_pair(l)

    def body(i, carry):
        at(i, -AHEAD, prefetch)
        at(i, 0, stage_combine, 1)
        once(i, 0, stage_first)
        at(i, 1, stage_forward)
        once(i, 1, norm_split)
        once(i, 2, norm_send)
        at(i, 3, stage_columns, 0, last)
        at(i, 4, stage_share, 0, last)
        at(i, 5, stage_moments)
        at(i, 7, stage_gather, 0, late)
        at(i, 8, stage_update, 0, late)
        at(i, 4, drain_bulk)
        once(i, 4, norm_stats)
        once(i, 6, norm_update)
        at(i, 2, stage_stats)
        return carry

    lax.fori_loop(0, late + 8, body, 0)
    for e in range(DIRECT):
        stage_final(e)
    drain(h_all.at[0:chips - 1], h_send.at[1])
    drain(k_all.at[0:ds - 1], k_send)


def write_kernel(lr_ref, w, d, r, c, n, dn, v, wo, ro, co, no, vo, w_new, n_new, sem):
    layers = w.shape[0]
    rate = lr_ref[...]
    pairs = ((r, ro), (c, co), (v, vo), (n_new, no))
    for i in range(3):
        pltpu.make_async_copy(*pairs[i], sem.at[i]).start()
    n_new[...] = n[...] - rate * dn[...]
    for l in range(layers + 1):
        if l < layers:
            w_new[l] = w[l] - rate * d[l]
        if l == 1:
            pltpu.make_async_copy(*pairs[3], sem.at[3]).start()
        if l >= 1:
            pltpu.make_async_copy(w_new.at[l - 1], wo.at[l - 1], sem.at[4]).start()
    for i, pair in enumerate(pairs):
        pltpu.make_async_copy(*pair, sem.at[i]).wait()
    pltpu.make_async_copy(w_new, wo, sem.at[4]).wait()


def write_out(rate, w, d, r, c, n, dn, v):
    return pl.pallas_call(
        write_kernel,
        out_shape=[jax.ShapeDtypeStruct(a.shape, a.dtype) for a in (w, r, c, n, v)],
        in_specs=[pl.BlockSpec(memory_space=pltpu.MemorySpace.SMEM)] + [pl.BlockSpec(memory_space=pltpu.MemorySpace.VMEM)] * 7,
        out_specs=[pl.BlockSpec(memory_space=pltpu.MemorySpace.HBM)] * 5,
        scratch_shapes=[pltpu.VMEM(w.shape, w.dtype), pltpu.VMEM(n.shape, n.dtype), pltpu.SemaphoreType.DMA((5,))],
        compiler_params=pltpu.CompilerParams(vmem_limit_bytes=8 << 20),
        name='write_out',
    )(rate, w, d, r, c, n, dn, v)


def solution(mesh):
    ds = mesh.shape['dp']
    zs = mesh.shape['model']

    def local_step(weight, grad_parts, row_stat, col_stat, norm_scale, norm_grads, norm_stat, learn_rate):
        layers, rows, cols = weight.shape
        half = rows // 2
        f32 = jnp.float32
        grads = grad_parts.reshape(layers, ds, rows, cols)
        any_spec = pl.BlockSpec(memory_space=pltpu.MemorySpace.HBM)
        dma = pltpu.SemaphoreType.DMA
        outs = pl.pallas_call(
            step_kernel,
            out_shape=[pltpu.VMEM(a.shape, f32) for a in (weight, weight, row_stat, col_stat, norm_scale, norm_scale, norm_stat)],
            in_specs=[any_spec] * 7,
            out_specs=[pl.BlockSpec(memory_space=pltpu.MemorySpace.VMEM)] * 7,
            scratch_shapes=[
                pltpu.VMEM((layers, 3, rows, cols), f32),
                pltpu.VMEM((layers, 4, rows, cols), f32),
                pltpu.VMEM((layers, 2, half, cols), f32),
                pltpu.VMEM((layers, 2, half, cols), f32),
                pltpu.VMEM((layers, 2, half, cols), f32),
                pltpu.VMEM(norm_grads.shape, f32),
                pltpu.VMEM((layers, LANES), f32),
                pltpu.VMEM((layers, LANES), f32),
                pltpu.VMEM((layers, zs, 1, LANES), f32),
                pltpu.VMEM((layers, 2, 1, cols // 2), f32),
                pltpu.VMEM((layers, 1, cols // 2), f32),
                pltpu.VMEM((layers, ds // 2, 1, cols // 2), f32),
                pltpu.VMEM((layers, 2, 1, cols // 2), f32),
                pltpu.VMEM((ds, 1, cols), f32),
                pltpu.VMEM((layers, 2 * zs, 1, LANES), f32),
                pltpu.VMEM((layers, ds // 2, 1, LANES), f32),
                pltpu.VMEM((DIRECT, ds * zs, 1, LANES), f32),
                pltpu.VMEM((ds // 2, 2, layers, LANES), f32),
                pltpu.VMEM((ds // 2, layers, LANES), f32),
                pltpu.VMEM((ds // 2, layers, LANES), f32),
                pltpu.VMEM((ds, 1, 2 * LANES), f32),
                *[dma((n,)) for n in (3, 2, 3, 3, 4, 4, 4, 4, 4, 3, 6, 2, 2, 2, 4, 2, 4, 3, 6, 2, 4, 2)],
                dma, dma, dma((DIRECT,)), dma((DIRECT,)), dma((5,)), dma((2,)), dma((2,)), dma, dma,
            ],
            compiler_params=pltpu.CompilerParams(collective_id=0, has_side_effects=True, vmem_limit_bytes=50 * 1000 * 1000),
            name='adafactor_step',
        )(weight, grads, row_stat, col_stat, norm_scale, norm_grads, norm_stat)
        return write_out(learn_rate, *outs)

    mat_spec = P(None, 'dp', 'model')
    row_spec = P(None, 'dp')
    col_spec = P(None, 'model')
    return jax.shard_map(local_step, mesh=mesh, in_specs=(mat_spec, mat_spec, row_spec, col_spec, row_spec, row_spec, row_spec, P()), out_specs=(mat_spec, row_spec, col_spec, row_spec, row_spec), check_vma=False)
```

```python
import functools

import jax
import jax.numpy as jnp
from jax import lax
from jax.experimental import pallas as pl
from jax.experimental.pallas import tpu as pltpu
from jax.sharding import PartitionSpec as P

STEP_COUNT = 4
DECAY_POWER = 0.8
EPS_FLOOR = 1e-30
SCALE_FLOOR = 1e-3
CLIP_LIMIT = 1.0
DECAY = 1.0 - STEP_COUNT ** -DECAY_POWER
MESH = pl.DeviceIdType.MESH
LANES = 128
AHEAD = 2
DIRECT = 2


def step_kernel(w_hbm, g_hbm, r_hbm, c_hbm, n_hbm, ng_hbm, v_hbm,
                w_buf, d_buf, r_buf, c_buf, n_buf, dn_buf, v_buf,
                own, peer, in1x, in1y, in2, ng_buf, r_pad, w_sq,
                r_all, c_mine, c_pair, c_all, c_full, c_last, s_all, t_all, t_last, h_out, h_pair, h_all, k_all,
                load_sem, stage_sem, first_recv, pair_send, pair_recv, one_send, one_recv, two_send, two_recv,
                r_send, r_recv, cp_send, cp_recv, c_send, c_recv, cf_send, cf_recv,
                s_send, s_recv, t_send, t_recv, w_sem,
                cl_send, cl_recv, tl_send, tl_recv, small_sem, h_send, h_recv, k_send, k_recv):
    layers, _, rows, cols = own.shape
    half = rows // 2
    last, ds = layers - 1, c_last.shape[1]
    late = layers - DIRECT
    zs = r_all.shape[1]
    chips = ds // 2
    rows_total, cols_total = rows * ds, cols * zs
    z = lax.axis_index('model')
    d = lax.axis_index('dp')
    chip, core = lax.div(d, 2), lax.rem(d, 2)
    dx = d + 2 - 4 * lax.rem(chip, 2)
    dy = d + 4 - 8 * lax.div(d, 4)
    dxy = dx + dy - d
    dc = d + 1 - 2 * core
    blocks = (dx, dxy, dy, d)
    z_peers = [{'model': lax.rem(z + j, zs)} for j in range(1, zs)]
    d_peers = [{'dp': e} for e in (dc, dx, dx + dc - d, dy, dy + dc - d, dxy, dxy + dc - d)]
    column_peers = [{'dp': dc}] + [{'model': p['model'], 'dp': e} for p in z_peers for e in (d, dc)]
    plane_peers = [{'dp': e} for e in (dx, dy, dxy)]
    others = [{'model': p['model'], **q} for q in d_peers[::-1] for p in z_peers] + d_peers[::-1] + z_peers

    def ring(sem, l):
        return sem.at[lax.rem(l, sem.shape[0])]

    def remote(src, dst, send, recv, where):
        return pltpu.make_async_remote_copy(src_ref=src, dst_ref=dst, send_sem=send, recv_sem=recv,
                                            device_id=where, device_id_type=MESH)

    def spread(ref, send, recv, peers):
        for where in peers:
            remote(ref, ref, send, recv, where).start()

    def drain(ref, sem):
        pltpu.make_async_copy(ref, ref, sem).wait()

    def load_own(l):
        for k in range(3):
            pltpu.make_async_copy(g_hbm.at[l, blocks[k]], own.at[l, k], ring(load_sem, l)).start()
        pltpu.make_async_copy(g_hbm.at[l, d], d_buf.at[l], ring(load_sem, l)).start()

    def pair_copy(l, k, row, source, recv):
        part = pl.ds(row, half)
        return remote(source.at[part], peer.at[l, k, part], ring(pair_send, l), recv, {'dp': dc})

    def from_hbm(l, k):
        return g_hbm.at[l, blocks[k] + dc - d]

    def send_pair(l):
        for k in range(4):
            remote(from_hbm(l, k), peer.at[l, k], ring(pair_send, l), ring(pair_recv, l), {'dp': dc}).start()

    def x1(l):
        return remote(own.at[l, 0:2, 0:half], in1x.at[l], ring(one_send, l), ring(one_recv, l), {'dp': dx})

    def y1(l):
        return remote(own.at[l, 1:3, half:rows], in1y.at[l], ring(one_send, l), ring(one_recv, l), {'dp': dy})

    def y2(l):
        return remote(own.at[l, 2, 0:half], in2.at[l, 0], ring(two_send, l), ring(two_recv, l), {'dp': dy})

    def x2(l):
        return remote(own.at[l, 0, half:rows], in2.at[l, 1], ring(two_send, l), ring(two_recv, l), {'dp': dx})

    def total(buf):
        parts = [buf[j] for j in range(buf.shape[0])]
        while len(parts) > 1:
            parts = [a + b for a, b in zip(parts[::2], parts[1::2])]
        return parts[0]

    def column(row):
        return jnp.transpose(jnp.broadcast_to(row, (LANES, LANES)))[0:rows]

    def fold(values):
        acc = values[:, 0:LANES]
        for t in range(1, cols // LANES):
            acc = acc + values[:, t * LANES:(t + 1) * LANES]
        return acc

    small = ((r_hbm, r_buf), (c_hbm, c_buf), (n_hbm, n_buf), (ng_hbm, ng_buf), (v_hbm, v_buf))
    groups = (((0, 0), (1, 0)), ((1, half), (2, half)))
    for i, group in enumerate(groups):
        for k, row in group:
            part = pl.ds(row, half)
            pltpu.make_async_copy(from_hbm(0, k).at[part], own.at[layers - 1, i, pl.ds((k - i) * half, half)], stage_sem.at[i]).start()
    load_own(0)
    for i, (src, dst) in enumerate(small):
        pltpu.make_async_copy(src, dst, small_sem.at[i]).start()

    barrier = pltpu.get_barrier_semaphore()
    known = d_peers + column_peers[1:]
    for where in known:
        pl.semaphore_signal(barrier, inc=1, device_id=where, device_id_type=MESH)
    pl.semaphore_wait(barrier, len(known))
    for i, group in enumerate(groups):
        drain(own.at[layers - 1, i], stage_sem.at[i])
        for k, row in group:
            part = pl.ds(row, half)
            remote(own.at[layers - 1, i, pl.ds((k - i) * half, half)], peer.at[0, k, part],
                   pair_send.at[0], first_recv.at[i], {'dp': dc}).start()
    for k, row in ((0, half), (2, 0), (3, 0), (3, half)):
        pair_copy(0, k, row, from_hbm(0, k), first_recv.at[2]).start()
    for l in range(1, AHEAD):
        send_pair(l)
        load_own(l)

    def norm_split():
        for i, (src, dst) in enumerate(small):
            pltpu.make_async_copy(src, dst, small_sem.at[i]).wait()
        r_pad[...] = jnp.zeros_like(r_pad)
        r_pad[:, 0:rows] = r_buf[...]
        h_out[...] = jnp.zeros_like(h_out)
        k_all[...] = jnp.zeros_like(k_all)
        for k in range(ds):
            h_out[k // 2, k % 2, :, 0:rows] = ng_buf[:, k * rows:(k + 1) * rows]
        remote(h_out.at[:, 1 - core], h_pair, h_send.at[0], h_recv.at[0], {'dp': dc}).start()

    def norm_send():
        remote(h_out.at[:, 1 - core], h_pair, h_send.at[0], h_recv.at[0], {'dp': dc}).wait()
        for k in range(chips):
            h_pair[k] = h_pair[k] + h_out[k, core]
        h_all[chip] = h_pair[chip]
        for e in (dx, dy, dxy):
            remote(h_pair.at[lax.div(e, 2)], h_all.at[chip], h_send.at[1], h_recv.at[1], {'dp': e}).start()

    def layer_sums(values):
        padded = jnp.concatenate([values, jnp.zeros((layers, LANES - rows), jnp.float32)], axis=1)
        return jnp.sum(jnp.transpose(padded), axis=0, keepdims=True)

    def norm_stats():
        drain(h_all.at[0:chips - 1], h_recv.at[1])
        h = total(h_all)[:, 0:rows]
        v_new = DECAY * v_buf[...] + (1.0 - DECAY) * (h * h + EPS_FLOOR)
        v_buf[...] = v_new
        zv = h * lax.rsqrt(v_new)
        nv = n_buf[...]
        k_all[d, :, 0:layers] = layer_sums(zv * zv)
        k_all[d, :, LANES:LANES + layers] = layer_sums(nv * nv)
        spread(k_all.at[d], k_send, k_recv, d_peers)

    def norm_update():
        drain(k_all.at[0:ds - 1], k_recv)
        acc = total(k_all)
        z_sq, n_sq = acc[:, 0:layers], acc[:, LANES:LANES + layers]
        clip = jnp.maximum(1.0, jnp.sqrt(z_sq / rows_total) / CLIP_LIMIT)
        scale = jnp.maximum(SCALE_FLOOR, jnp.sqrt(n_sq / rows_total))
        clip = jnp.transpose(jnp.broadcast_to(clip, (LANES, layers)))[:, 0:rows]
        scale = jnp.transpose(jnp.broadcast_to(scale, (LANES, layers)))[:, 0:rows]
        zv = total(h_all)[:, 0:rows] * lax.rsqrt(v_buf[...])
        dn_buf[...] = scale * (zv / clip)

    def combine(l, k, part):
        own[l, k, part] = own[l, k, part] + peer[l, k, part]

    first, second = slice(0, half), slice(half, rows)

    def stage_first():
        drain(peer.at[0], load_sem.at[0])
        drain(in1x.at[0], first_recv.at[0])
        combine(0, slice(0, 2), first)
        x1(0).start()
        drain(in1y.at[0], first_recv.at[1])
        combine(0, slice(1, 3), second)
        y1(0).start()
        drain(peer.at[0, 0:2], first_recv.at[2])
        combine(0, 0, second)
        combine(0, 2, first)
        d_buf[0] = d_buf[0] + peer[0, 3]
        drain(peer.at[0], pair_send.at[0])

    def stage_combine(l):
        drain(peer.at[l], ring(load_sem, l))
        drain(peer.at[l], ring(pair_recv, l))
        combine(l, slice(0, 2), first)
        x1(l).start()
        combine(l, slice(1, 3), second)
        y1(l).start()
        combine(l, 0, second)
        combine(l, 2, first)
        d_buf[l] = d_buf[l] + peer[l, 3]
        drain(peer.at[l], ring(pair_send, l))

    def stage_forward(l):
        pltpu.make_async_copy(w_hbm.at[l], w_buf.at[l], ring(w_sem, l)).start()
        drain(in1x.at[0:2], ring(one_recv, l))
        own[l, 2, 0:half] = own[l, 2, 0:half] + in1x[l, 1]
        own[l, 0, half:rows] = own[l, 0, half:rows] + in1y[l, 0]
        y2(l).start()
        d_buf[l, 0:half] = d_buf[l, 0:half] + in1x[l, 0]
        x2(l).start()
        d_buf[l, half:rows] = d_buf[l, half:rows] + in1y[l, 1]

    def stage_stats(l):
        drain(w_buf.at[l], ring(w_sem, l))
        w = w_buf[l]
        w_sq[pl.ds(l, 1)] = fold(jnp.sum(w * w, axis=0, keepdims=True))
        drain(in2.at[l], ring(two_recv, l))
        g = d_buf[l] + in2[l].reshape(rows, cols)
        d_buf[l] = g
        q = g * g + EPS_FLOOR
        col = jnp.sum(q, axis=0, keepdims=True)

        @pl.when(l < late)
        def _():
            c_mine[l, 0] = col[:, 0:cols // 2]
            c_mine[l, 1] = col[:, cols // 2:cols]

        @pl.when(l >= late)
        def _():
            c_last[l - late, d] = col

        p = jnp.concatenate([fold(q), jnp.zeros((LANES - rows, LANES), jnp.float32)], axis=0)
        r_all[l, z] = jnp.sum(jnp.transpose(p), axis=0, keepdims=True)

        @pl.when(l < late)
        def _():
            pair_columns(l).start()

        @pl.when(l >= late)
        def _():
            e = l - late
            spread(c_last.at[e, d], cl_send.at[e], cl_recv.at[e], d_peers)

        spread(r_all.at[l, z], ring(r_send, l), ring(r_recv, l), z_peers)

    def pair_columns(l):
        return remote(c_mine.at[l, 1 - core], c_pair.at[l], ring(cp_send, l), ring(cp_recv, l), {'dp': dc})

    def full_columns(l):
        return remote(c_full.at[l, core], c_full.at[l, core], ring(cf_send, l), ring(cf_recv, l), {'dp': dc})

    def stage_columns(l):
        pair_columns(l).wait()
        c_all[l, chip] = c_mine[l, core] + c_pair[l]
        spread(c_all.at[l, chip], ring(c_send, l), ring(c_recv, l), plane_peers)

    def stage_share(l):
        drain(c_all.at[l, 0:chips - 1], ring(c_recv, l))
        drain(c_all.at[l, 0:chips - 1], ring(c_send, l))
        c_full[l, core] = total(c_all.at[l])
        full_columns(l).start()

    def stage_moments(l):
        @pl.when(l < late)
        def _():
            full_columns(l).wait()

        @pl.when(l >= late)
        def _():
            e = l - late
            drain(c_last.at[e, 0:ds - 1], cl_recv.at[e])
            drain(c_last.at[e, 0:ds - 1], cl_send.at[e])
            col = total(c_last.at[e])
            c_full[l, 0] = col[:, 0:cols // 2]
            c_full[l, 1] = col[:, cols // 2:cols]

        if zs > 1:
            drain(r_all.at[l, 0:zs - 1], ring(r_recv, l))
            drain(r_all.at[l, 0:zs - 1], ring(r_send, l))
        col = jnp.concatenate([c_full[l, 0], c_full[l, 1]], axis=1)
        r_new = DECAY * r_pad[pl.ds(l, 1)] + (1.0 - DECAY) * (total(r_all.at[l]) / cols_total)
        c_new = DECAY * c_buf[pl.ds(l, 1)] + (1.0 - DECAY) * (col / rows_total)
        r_pad[pl.ds(l, 1)] = r_new
        r_buf[pl.ds(l, 1)] = r_new[:, 0:rows]
        c_buf[pl.ds(l, 1)] = c_new
        a = column(lax.rsqrt(r_new))
        b = lax.rsqrt(c_new)
        acc = jnp.zeros((1, LANES), jnp.float32)
        for t in range(cols // LANES):
            sl = slice(t * LANES, (t + 1) * LANES)
            u = d_buf[l, :, sl] * a * b[:, sl]
            acc = acc + jnp.sum(u * u, axis=0, keepdims=True)
        lane = lax.broadcasted_iota(jnp.int32, (1, LANES), 1)
        row = jnp.where(lane == 0, jnp.sum(acc, axis=1, keepdims=True), 0.0)
        row = jnp.where(lane == 1, jnp.sum(w_sq[pl.ds(l, 1)], axis=1, keepdims=True), row)
        row = jnp.where(lane == 2, jnp.sum(r_new, axis=1, keepdims=True), row)

        @pl.when(l < last)
        def _():
            s_all[l, 2 * z + core] = row
            spread(s_all.at[l, 2 * z + core], ring(s_send, l), ring(s_recv, l), column_peers)

        @pl.when(l == last)
        def _():
            me = ds * z + d
            t_last[me] = row
            spread(t_last.at[me], tl_send, tl_recv, others)

    def stage_gather(l):
        drain(s_all.at[l, 0:2 * zs - 1], ring(s_recv, l))
        drain(s_all.at[l, 0:2 * zs - 1], ring(s_send, l))
        t_all[l, chip] = total(s_all.at[l])
        spread(t_all.at[l, chip], ring(t_send, l), ring(t_recv, l), plane_peers)

    def stage_update(l):
        drain(t_all.at[l, 0:chips - 1], ring(t_recv, l))
        drain(t_all.at[l, 0:chips - 1], ring(t_send, l))
        apply(l, total(t_all.at[l]))

    def stage_final():
        drain(t_last.at[0:ds * zs - 1], tl_recv)
        drain(t_last.at[0:ds * zs - 1], tl_send)
        apply(last, total(t_last))

    def apply(l, sums):
        count = rows_total * cols_total
        r_mean = sums[:, 2:3] / (rows_total * zs)
        u_rms = jnp.sqrt(sums[:, 0:1] / count * r_mean)
        clip = jnp.maximum(1.0, u_rms / CLIP_LIMIT)
        scale = jnp.maximum(SCALE_FLOOR, jnp.sqrt(sums[:, 1:2] / count))
        a = column(lax.rsqrt(r_pad[pl.ds(l, 1)] / r_mean))
        b = lax.rsqrt(c_buf[pl.ds(l, 1)])
        for t in range(cols // LANES):
            sl = slice(t * LANES, (t + 1) * LANES)
            d_buf[l, :, sl] = d_buf[l, :, sl] * a * (b[:, sl] / clip) * scale

    def drain_bulk(l):
        drain(in1x.at[0:2], ring(one_send, l))
        drain(in2.at[l], ring(two_send, l))

    def at(i, lag, stage, begin=0, end=layers):
        @pl.when((i >= begin + lag) & (i < end + lag))
        def _():
            stage(i - lag)

    def once(i, when, stage):
        @pl.when(i == when)
        def _():
            stage()

    def prefetch(l):
        load_own(l)
        send_pair(l)

    def body(i, carry):
        at(i, -AHEAD, prefetch)
        at(i, 0, stage_combine, 1)
        once(i, 0, stage_first)
        at(i, 1, stage_forward)
        once(i, 1, norm_split)
        once(i, 2, norm_send)
        at(i, 3, stage_columns, 0, late)
        at(i, 4, stage_share, 0, late)
        at(i, 5, stage_moments)
        at(i, 7, stage_gather, 0, last)
        at(i, 8, stage_update, 0, last)
        at(i, 4, drain_bulk)
        once(i, 4, norm_stats)
        once(i, 6, norm_update)
        at(i, 2, stage_stats)
        return carry

    lax.fori_loop(0, last + 8, body, 0)
    stage_final()
    drain(h_all.at[0:chips - 1], h_send.at[1])
    drain(k_all.at[0:ds - 1], k_send)


def write_kernel(lr_ref, w, d, r, c, n, dn, v, wo, ro, co, no, vo, w_new, n_new, sem):
    layers = w.shape[0]
    rate = lr_ref[...]
    pairs = ((r, ro), (c, co), (v, vo), (n_new, no))
    for i in range(3):
        pltpu.make_async_copy(*pairs[i], sem.at[i]).start()
    n_new[...] = n[...] - rate * dn[...]
    for l in range(layers + 1):
        if l < layers:
            w_new[l] = w[l] - rate * d[l]
        if l == 1:
            pltpu.make_async_copy(*pairs[3], sem.at[3]).start()
        if l >= 1:
            pltpu.make_async_copy(w_new.at[l - 1], wo.at[l - 1], sem.at[4]).start()
    for i, pair in enumerate(pairs):
        pltpu.make_async_copy(*pair, sem.at[i]).wait()
    pltpu.make_async_copy(w_new, wo, sem.at[4]).wait()


def write_out(rate, w, d, r, c, n, dn, v):
    return pl.pallas_call(
        write_kernel,
        out_shape=[jax.ShapeDtypeStruct(a.shape, a.dtype) for a in (w, r, c, n, v)],
        in_specs=[pl.BlockSpec(memory_space=pltpu.MemorySpace.SMEM)] + [pl.BlockSpec(memory_space=pltpu.MemorySpace.VMEM)] * 7,
        out_specs=[pl.BlockSpec(memory_space=pltpu.MemorySpace.HBM)] * 5,
        scratch_shapes=[pltpu.VMEM(w.shape, w.dtype), pltpu.VMEM(n.shape, n.dtype), pltpu.SemaphoreType.DMA((5,))],
        compiler_params=pltpu.CompilerParams(vmem_limit_bytes=8 << 20),
        name='write_out',
    )(rate, w, d, r, c, n, dn, v)


def solution(mesh):
    ds = mesh.shape['dp']
    zs = mesh.shape['model']

    def local_step(weight, grad_parts, row_stat, col_stat, norm_scale, norm_grads, norm_stat, learn_rate):
        layers, rows, cols = weight.shape
        half = rows // 2
        f32 = jnp.float32
        grads = grad_parts.reshape(layers, ds, rows, cols)
        any_spec = pl.BlockSpec(memory_space=pltpu.MemorySpace.HBM)
        dma = pltpu.SemaphoreType.DMA
        outs = pl.pallas_call(
            step_kernel,
            out_shape=[pltpu.VMEM(a.shape, f32) for a in (weight, weight, row_stat, col_stat, norm_scale, norm_scale, norm_stat)],
            in_specs=[any_spec] * 7,
            out_specs=[pl.BlockSpec(memory_space=pltpu.MemorySpace.VMEM)] * 7,
            scratch_shapes=[
                pltpu.VMEM((layers, 3, rows, cols), f32),
                pltpu.VMEM((layers, 4, rows, cols), f32),
                pltpu.VMEM((layers, 2, half, cols), f32),
                pltpu.VMEM((layers, 2, half, cols), f32),
                pltpu.VMEM((layers, 2, half, cols), f32),
                pltpu.VMEM(norm_grads.shape, f32),
                pltpu.VMEM((layers, LANES), f32),
                pltpu.VMEM((layers, LANES), f32),
                pltpu.VMEM((layers, zs, 1, LANES), f32),
                pltpu.VMEM((layers, 2, 1, cols // 2), f32),
                pltpu.VMEM((layers, 1, cols // 2), f32),
                pltpu.VMEM((layers, ds // 2, 1, cols // 2), f32),
                pltpu.VMEM((layers, 2, 1, cols // 2), f32),
                pltpu.VMEM((DIRECT, ds, 1, cols), f32),
                pltpu.VMEM((layers, 2 * zs, 1, LANES), f32),
                pltpu.VMEM((layers, ds // 2, 1, LANES), f32),
                pltpu.VMEM((ds * zs, 1, LANES), f32),
                pltpu.VMEM((ds // 2, 2, layers, LANES), f32),
                pltpu.VMEM((ds // 2, layers, LANES), f32),
                pltpu.VMEM((ds // 2, layers, LANES), f32),
                pltpu.VMEM((ds, 1, 2 * LANES), f32),
                *[dma((n,)) for n in (3, 2, 3, 3, 4, 4, 4, 4, 4, 3, 6, 2, 2, 2, 4, 2, 4, 3, 6, 2, 4, 2)],
                dma((DIRECT,)), dma((DIRECT,)), dma, dma, dma((5,)), dma((2,)), dma((2,)), dma, dma,
            ],
            compiler_params=pltpu.CompilerParams(collective_id=0, has_side_effects=True, vmem_limit_bytes=50 * 1000 * 1000),
            name='adafactor_step',
        )(weight, grads, row_stat, col_stat, norm_scale, norm_grads, norm_stat)
        return write_out(learn_rate, *outs)

    mat_spec = P(None, 'dp', 'model')
    row_spec = P(None, 'dp')
    col_spec = P(None, 'model')
    return jax.shard_map(local_step, mesh=mesh, in_specs=(mat_spec, mat_spec, row_spec, col_spec, row_spec, row_spec, row_spec, P()), out_specs=(mat_spec, row_spec, col_spec, row_spec, row_spec), check_vma=False)
```

```python
import functools

import jax
import jax.numpy as jnp
from jax import lax
from jax.experimental import pallas as pl
from jax.experimental.pallas import tpu as pltpu
from jax.sharding import PartitionSpec as P

STEP_COUNT = 4
DECAY_POWER = 0.8
EPS_FLOOR = 1e-30
SCALE_FLOOR = 1e-3
CLIP_LIMIT = 1.0
DECAY = 1.0 - STEP_COUNT ** -DECAY_POWER
MESH = pl.DeviceIdType.MESH
LANES = 128
AHEAD = 2
DIRECT = 2


def column(row, rows):
    return jnp.transpose(jnp.broadcast_to(row, (LANES, LANES)))[0:rows]


def factors(sums, r_row, rows, zs, rows_total, cols_total):
    count = rows_total * cols_total
    r_mean = sums[:, 2:3] / (rows_total * zs)
    u_rms = jnp.sqrt(sums[:, 0:1] / count * r_mean)
    clip = jnp.maximum(1.0, u_rms / CLIP_LIMIT)
    scale = jnp.maximum(SCALE_FLOOR, jnp.sqrt(sums[:, 1:2] / count))
    return scale, clip, column(lax.rsqrt(r_row / r_mean), rows)


def step_kernel(w_hbm, g_hbm, r_hbm, c_hbm, n_hbm, ng_hbm, v_hbm,
                w_buf, d_buf, r_buf, c_buf, n_buf, dn_buf, v_buf, r_pad, sums_out,
                own, peer, in1x, in1y, in2, ng_buf, w_sq,
                r_all, c_mine, c_pair, c_all, c_full, c_last, s_all, t_all, t_last, h_out, h_pair, h_all, k_all,
                load_sem, pair_send, pair_recv, one_send, one_recv, two_send, two_recv,
                r_send, r_recv, cp_send, cp_recv, c_send, c_recv, cf_send, cf_recv,
                s_send, s_recv, t_send, t_recv, w_sem,
                cl_send, cl_recv, tl_send, tl_recv):
    layers, _, rows, cols = own.shape
    half = rows // 2
    ds = c_last.shape[1]
    late = layers - DIRECT
    zs = r_all.shape[1]
    chips = ds // 2
    rows_total, cols_total = rows * ds, cols * zs
    z = lax.axis_index('model')
    d = lax.axis_index('dp')
    chip, core = lax.div(d, 2), lax.rem(d, 2)
    dx = d + 2 - 4 * lax.rem(chip, 2)
    dy = d + 4 - 8 * lax.div(d, 4)
    dxy = dx + dy - d
    dc = d + 1 - 2 * core
    blocks = (dx, dxy, dy, d)
    z_peers = [{'model': lax.rem(z + j, zs)} for j in range(1, zs)]
    d_peers = [{'dp': e} for e in (dc, dx, dx + dc - d, dy, dy + dc - d, dxy, dxy + dc - d)]
    column_peers = [{'dp': dc}] + [{'model': p['model'], 'dp': e} for p in z_peers for e in (d, dc)]
    plane_peers = [{'dp': e} for e in (dx, dy, dxy)]
    others = [{'model': p['model'], **q} for q in d_peers[::-1] for p in z_peers] + d_peers[::-1] + z_peers

    def ring(sem, l):
        return sem.at[lax.rem(l, sem.shape[0])]

    def remote(src, dst, send, recv, where):
        return pltpu.make_async_remote_copy(src_ref=src, dst_ref=dst, send_sem=send, recv_sem=recv,
                                            device_id=where, device_id_type=MESH)

    def spread(ref, send, recv, peers):
        for where in peers:
            remote(ref, ref, send, recv, where).start()

    def drain(ref, sem):
        pltpu.make_async_copy(ref, ref, sem).wait()

    def load_own(l):
        for k in range(3):
            pltpu.make_async_copy(g_hbm.at[l, blocks[k]], own.at[l, k], ring(load_sem, l)).start()
        pltpu.make_async_copy(g_hbm.at[l, d], d_buf.at[l], ring(load_sem, l)).start()

    def pair_copy(l, k, row, source, recv):
        part = pl.ds(row, half)
        return remote(source.at[part], peer.at[l, k, part], ring(pair_send, l), recv, {'dp': dc})

    def from_hbm(l, k):
        return g_hbm.at[l, blocks[k] + dc - d]

    def send_pair(l):
        for k in range(4):
            remote(from_hbm(l, k), peer.at[l, k], ring(pair_send, l), ring(pair_recv, l), {'dp': dc}).start()

    def x1(l):
        return remote(own.at[l, 0:2, 0:half], in1x.at[l], ring(one_send, l), ring(one_recv, l), {'dp': dx})

    def y1(l):
        return remote(own.at[l, 1:3, half:rows], in1y.at[l], ring(one_send, l), ring(one_recv, l), {'dp': dy})

    def y2(l):
        return remote(own.at[l, 2, 0:half], in2.at[l, 0], ring(two_send, l), ring(two_recv, l), {'dp': dy})

    def x2(l):
        return remote(own.at[l, 0, half:rows], in2.at[l, 1], ring(two_send, l), ring(two_recv, l), {'dp': dx})

    def total(buf):
        parts = [buf[j] for j in range(buf.shape[0])]
        while len(parts) > 1:
            parts = [a + b for a, b in zip(parts[::2], parts[1::2])]
        return parts[0]

    def fold(values):
        acc = values[:, 0:LANES]
        for t in range(1, cols // LANES):
            acc = acc + values[:, t * LANES:(t + 1) * LANES]
        return acc

    small = ((r_hbm, r_buf), (c_hbm, c_buf), (n_hbm, n_buf), (ng_hbm, ng_buf), (v_hbm, v_buf))
    groups = (((0, 0), (1, 0)), ((1, half), (2, half)))
    for i, group in enumerate(groups):
        for k, row in group:
            part = pl.ds(row, half)
            pltpu.make_async_copy(from_hbm(0, k).at[part], own.at[layers - 1, i, pl.ds((k - i) * half, half)], w_sem.at[i]).start()
    load_own(0)

    barrier = pltpu.get_barrier_semaphore()
    known = d_peers + column_peers[1:]
    for where in known:
        pl.semaphore_signal(barrier, inc=1, device_id=where, device_id_type=MESH)
    pl.semaphore_wait(barrier, len(known))
    for i, group in enumerate(groups):
        drain(own.at[layers - 1, i], w_sem.at[i])
        for k, row in group:
            part = pl.ds(row, half)
            remote(own.at[layers - 1, i, pl.ds((k - i) * half, half)], peer.at[0, k, part],
                   pair_send.at[0], two_recv.at[i + 1], {'dp': dc}).start()
    for k, row in ((0, half), (2, 0), (3, 0), (3, half)):
        pair_copy(0, k, row, from_hbm(0, k), two_recv.at[3]).start()
    for l in range(1, AHEAD):
        send_pair(l)
        load_own(l)

    def norm_split():
        for src, dst in small:
            copy = pltpu.make_async_copy(src, dst, w_sem.at[1])
            copy.start()
            copy.wait()
        r_pad[...] = jnp.zeros_like(r_pad)
        r_pad[:, 0:rows] = r_buf[...]
        h_out[...] = jnp.zeros_like(h_out)
        k_all[...] = jnp.zeros_like(k_all)
        for k in range(ds):
            h_out[k // 2, k % 2, :, 0:rows] = ng_buf[:, k * rows:(k + 1) * rows]
        remote(h_out.at[:, 1 - core], h_pair, cl_send.at[0], cl_recv.at[0], {'dp': dc}).start()

    def norm_send():
        remote(h_out.at[:, 1 - core], h_pair, cl_send.at[0], cl_recv.at[0], {'dp': dc}).wait()
        for k in range(chips):
            h_pair[k] = h_pair[k] + h_out[k, core]
        h_all[chip] = h_pair[chip]
        for e in (dx, dy, dxy):
            remote(h_pair.at[lax.div(e, 2)], h_all.at[chip], cl_send.at[1], cl_recv.at[1], {'dp': e}).start()

    def layer_sums(values):
        padded = jnp.concatenate([values, jnp.zeros((layers, LANES - rows), jnp.float32)], axis=1)
        return jnp.sum(jnp.transpose(padded), axis=0, keepdims=True)

    def norm_stats():
        drain(h_all.at[0:chips - 1], cl_recv.at[1])
        drain(h_all.at[0:chips - 1], cl_send.at[1])
        h = total(h_all)[:, 0:rows]
        v_new = DECAY * v_buf[...] + (1.0 - DECAY) * (h * h + EPS_FLOOR)
        v_buf[...] = v_new
        zv = h * lax.rsqrt(v_new)
        nv = n_buf[...]
        k_all[d, :, 0:layers] = layer_sums(zv * zv)
        k_all[d, :, LANES:LANES + layers] = layer_sums(nv * nv)
        spread(k_all.at[d], tl_send.at[0], tl_recv.at[0], d_peers)

    def norm_update():
        drain(k_all.at[0:ds - 1], tl_recv.at[0])
        drain(k_all.at[0:ds - 1], tl_send.at[0])
        acc = total(k_all)
        z_sq, n_sq = acc[:, 0:layers], acc[:, LANES:LANES + layers]
        clip = jnp.maximum(1.0, jnp.sqrt(z_sq / rows_total) / CLIP_LIMIT)
        scale = jnp.maximum(SCALE_FLOOR, jnp.sqrt(n_sq / rows_total))
        clip = jnp.transpose(jnp.broadcast_to(clip, (LANES, layers)))[:, 0:rows]
        scale = jnp.transpose(jnp.broadcast_to(scale, (LANES, layers)))[:, 0:rows]
        zv = total(h_all)[:, 0:rows] * lax.rsqrt(v_buf[...])
        dn_buf[...] = scale * (zv / clip)

    def combine(l, k, part):
        own[l, k, part] = own[l, k, part] + peer[l, k, part]

    first, second = slice(0, half), slice(half, rows)

    def stage_first():
        drain(peer.at[0], load_sem.at[0])
        drain(in1x.at[0], two_recv.at[1])
        combine(0, slice(0, 2), first)
        x1(0).start()
        drain(in1y.at[0], two_recv.at[2])
        combine(0, slice(1, 3), second)
        y1(0).start()
        drain(peer.at[0, 0:2], two_recv.at[3])
        combine(0, 0, second)
        combine(0, 2, first)
        d_buf[0] = d_buf[0] + peer[0, 3]
        drain(peer.at[0], pair_send.at[0])

    def stage_combine(l):
        drain(peer.at[l], ring(load_sem, l))
        drain(peer.at[l], ring(pair_recv, l))
        combine(l, slice(0, 2), first)
        x1(l).start()
        combine(l, slice(1, 3), second)
        y1(l).start()
        combine(l, 0, second)
        combine(l, 2, first)
        d_buf[l] = d_buf[l] + peer[l, 3]
        drain(peer.at[l], ring(pair_send, l))

    def stage_forward(l):
        pltpu.make_async_copy(w_hbm.at[l], w_buf.at[l], ring(w_sem, l)).start()
        drain(in1x.at[0:2], ring(one_recv, l))
        own[l, 2, 0:half] = own[l, 2, 0:half] + in1x[l, 1]
        own[l, 0, half:rows] = own[l, 0, half:rows] + in1y[l, 0]
        y2(l).start()
        d_buf[l, 0:half] = d_buf[l, 0:half] + in1x[l, 0]
        x2(l).start()
        d_buf[l, half:rows] = d_buf[l, half:rows] + in1y[l, 1]

    def stage_stats(l):
        drain(w_buf.at[l], ring(w_sem, l))
        w = w_buf[l]
        w_sq[pl.ds(l, 1)] = fold(jnp.sum(w * w, axis=0, keepdims=True))
        drain(in2.at[l], ring(two_recv, l))
        g = d_buf[l] + in2[l].reshape(rows, cols)
        d_buf[l] = g
        q = g * g + EPS_FLOOR
        col = jnp.sum(q, axis=0, keepdims=True)

        @pl.when(l < late)
        def _():
            c_mine[l, 0] = col[:, 0:cols // 2]
            c_mine[l, 1] = col[:, cols // 2:cols]

        @pl.when(l >= late)
        def _():
            c_last[l - late, d] = col

        p = jnp.concatenate([fold(q), jnp.zeros((LANES - rows, LANES), jnp.float32)], axis=0)
        r_all[l, z] = jnp.sum(jnp.transpose(p), axis=0, keepdims=True)

        @pl.when(l < late)
        def _():
            pair_columns(l).start()

        @pl.when(l >= late)
        def _():
            e = l - late
            spread(c_last.at[e, d], cl_send.at[e], cl_recv.at[e], d_peers)

        spread(r_all.at[l, z], ring(r_send, l), ring(r_recv, l), z_peers)

    def pair_columns(l):
        return remote(c_mine.at[l, 1 - core], c_pair.at[l], ring(cp_send, l), ring(cp_recv, l), {'dp': dc})

    def full_columns(l):
        return remote(c_full.at[l, core], c_full.at[l, core], ring(cf_send, l), ring(cf_recv, l), {'dp': dc})

    def drain_rows(l):
        if zs > 1:
            drain(r_all.at[l, 0:zs - 1], ring(r_recv, l))
            drain(r_all.at[l, 0:zs - 1], ring(r_send, l))

    def stage_columns(l):
        pair_columns(l).wait()
        drain_rows(l)
        c_all[l, chip] = c_mine[l, core] + c_pair[l]
        spread(c_all.at[l, chip], ring(c_send, l), ring(c_recv, l), plane_peers)

    def stage_share(l):
        drain(c_all.at[l, 0:chips - 1], ring(c_recv, l))
        drain(c_all.at[l, 0:chips - 1], ring(c_send, l))
        c_full[l, core] = total(c_all.at[l])
        full_columns(l).start()

    def stage_moments(l):
        @pl.when(l < late)
        def _():
            full_columns(l).wait()

        @pl.when(l >= late)
        def _():
            e = l - late
            drain(c_last.at[e, 0:ds - 1], cl_recv.at[e])
            drain(c_last.at[e, 0:ds - 1], cl_send.at[e])
            drain_rows(l)
            col = total(c_last.at[e])
            c_full[l, 0] = col[:, 0:cols // 2]
            c_full[l, 1] = col[:, cols // 2:cols]

        col = jnp.concatenate([c_full[l, 0], c_full[l, 1]], axis=1)
        r_new = DECAY * r_pad[pl.ds(l, 1)] + (1.0 - DECAY) * (total(r_all.at[l]) / cols_total)
        c_new = DECAY * c_buf[pl.ds(l, 1)] + (1.0 - DECAY) * (col / rows_total)
        r_pad[pl.ds(l, 1)] = r_new
        r_buf[pl.ds(l, 1)] = r_new[:, 0:rows]
        c_buf[pl.ds(l, 1)] = c_new
        a = column(lax.rsqrt(r_new), rows)
        b = lax.rsqrt(c_new)
        acc = jnp.zeros((1, LANES), jnp.float32)
        for t in range(cols // LANES):
            sl = slice(t * LANES, (t + 1) * LANES)
            u = d_buf[l, :, sl] * a * b[:, sl]
            acc = acc + jnp.sum(u * u, axis=0, keepdims=True)
        lane = lax.broadcasted_iota(jnp.int32, (1, LANES), 1)
        row = jnp.where(lane == 0, jnp.sum(acc, axis=1, keepdims=True), 0.0)
        row = jnp.where(lane == 1, jnp.sum(w_sq[pl.ds(l, 1)], axis=1, keepdims=True), row)
        row = jnp.where(lane == 2, jnp.sum(r_new, axis=1, keepdims=True), row)

        @pl.when(l < late)
        def _():
            s_all[l, 2 * z + core] = row
            spread(s_all.at[l, 2 * z + core], ring(s_send, l), ring(s_recv, l), column_peers)

        @pl.when(l >= late)
        def _():
            e = l - late
            me = ds * z + d
            t_last[e, me] = row
            spread(t_last.at[e, me], tl_send.at[e], tl_recv.at[e], others)

    def stage_gather(l):
        drain(s_all.at[l, 0:2 * zs - 1], ring(s_recv, l))
        drain(s_all.at[l, 0:2 * zs - 1], ring(s_send, l))
        t_all[l, chip] = total(s_all.at[l])
        spread(t_all.at[l, chip], ring(t_send, l), ring(t_recv, l), plane_peers)

    def stage_update(l):
        drain(t_all.at[l, 0:chips - 1], ring(t_recv, l))
        drain(t_all.at[l, 0:chips - 1], ring(t_send, l))
        scale, clip, a = factors(total(t_all.at[l]), r_pad[pl.ds(l, 1)], rows, zs, rows_total, cols_total)
        b = lax.rsqrt(c_buf[pl.ds(l, 1)]) / clip
        for t in range(cols // LANES):
            sl = slice(t * LANES, (t + 1) * LANES)
            d_buf[l, :, sl] = d_buf[l, :, sl] * a * b[:, sl] * scale

    def stage_final(e):
        drain(t_last.at[e, 0:ds * zs - 1], tl_recv.at[e])
        drain(t_last.at[e, 0:ds * zs - 1], tl_send.at[e])
        sums_out[e] = total(t_last.at[e])

    def drain_one(l):
        drain(in1x.at[0:2], ring(one_send, l))

    def drain_two(l):
        drain(in2.at[l], ring(two_send, l))

    def at(i, lag, stage, begin=0, end=layers):
        @pl.when((i >= begin + lag) & (i < end + lag))
        def _():
            stage(i - lag)

    def once(i, when, stage):
        @pl.when(i == when)
        def _():
            stage()

    def prefetch(l):
        load_own(l)
        send_pair(l)

    def body(i, carry):
        at(i, -AHEAD, prefetch)
        at(i, 0, stage_combine, 1)
        once(i, 0, stage_first)
        at(i, 1, stage_forward)
        once(i, 1, norm_split)
        once(i, 2, norm_send)
        at(i, 3, stage_columns, 0, late)
        at(i, 4, stage_share, 0, late)
        at(i, 5, stage_moments)
        at(i, 7, stage_gather, 0, late)
        at(i, 8, stage_update, 0, late)
        at(i, 2, drain_one)
        at(i, 3, drain_two)
        once(i, 4, norm_stats)
        once(i, 6, norm_update)
        at(i, 2, stage_stats)
        return carry

    lax.fori_loop(0, late + 8, body, 0)
    for e in range(DIRECT):
        stage_final(e)


def write_kernel(ds, zs, rate_ref, w, d, r, c, n, dn, v, r_pad, sums, wo, ro, co, no, vo, w_new, n_new, sem):
    layers, rows, cols = w.shape
    late = layers - DIRECT
    rate = rate_ref[...]
    pairs = ((r, ro), (c, co), (v, vo), (n_new, no))
    for i in range(3):
        pltpu.make_async_copy(*pairs[i], sem.at[i]).start()
    n_new[...] = n[...] - rate * dn[...]
    for l in range(layers + 1):
        if l < late:
            w_new[l] = w[l] - rate * d[l]
        elif l < layers:
            scale, clip, a = factors(sums[l - late], r_pad[l:l + 1], rows, zs, rows * ds, cols * zs)
            b = lax.rsqrt(c[l:l + 1]) / clip
            for t in range(cols // LANES):
                sl = slice(t * LANES, (t + 1) * LANES)
                w_new[l, :, sl] = w[l, :, sl] - rate * (d[l, :, sl] * a * b[:, sl] * scale)
        if l == 1:
            pltpu.make_async_copy(*pairs[3], sem.at[3]).start()
        if l >= 1:
            pltpu.make_async_copy(w_new.at[l - 1], wo.at[l - 1], sem.at[4]).start()
    for i, pair in enumerate(pairs):
        pltpu.make_async_copy(*pair, sem.at[i]).wait()
    pltpu.make_async_copy(w_new, wo, sem.at[4]).wait()


def write_out(ds, zs, rate, w, d, r, c, n, dn, v, r_pad, sums):
    return pl.pallas_call(
        functools.partial(write_kernel, ds, zs),
        out_shape=[jax.ShapeDtypeStruct(a.shape, a.dtype) for a in (w, r, c, n, v)],
        in_specs=[pl.BlockSpec(memory_space=pltpu.MemorySpace.SMEM)] + [pl.BlockSpec(memory_space=pltpu.MemorySpace.VMEM)] * 9,
        out_specs=[pl.BlockSpec(memory_space=pltpu.MemorySpace.HBM)] * 5,
        scratch_shapes=[pltpu.VMEM(w.shape, w.dtype), pltpu.VMEM(n.shape, n.dtype), pltpu.SemaphoreType.DMA((5,))],
        compiler_params=pltpu.CompilerParams(vmem_limit_bytes=8 << 20),
        name='write_out',
    )(rate, w, d, r, c, n, dn, v, r_pad, sums)


def solution(mesh):
    ds = mesh.shape['dp']
    zs = mesh.shape['model']

    def local_step(weight, grad_parts, row_stat, col_stat, norm_scale, norm_grads, norm_stat, learn_rate):
        layers, rows, cols = weight.shape
        half = rows // 2
        f32 = jnp.float32
        grads = grad_parts.reshape(layers, ds, rows, cols)
        any_spec = pl.BlockSpec(memory_space=pltpu.MemorySpace.HBM)
        dma = pltpu.SemaphoreType.DMA
        outs = pl.pallas_call(
            step_kernel,
            out_shape=[pltpu.VMEM(a.shape, f32) for a in (weight, weight, row_stat, col_stat, norm_scale, norm_scale, norm_stat)]
            + [pltpu.VMEM((layers, LANES), f32), pltpu.VMEM((DIRECT, 1, LANES), f32)],
            in_specs=[any_spec] * 7,
            out_specs=[pl.BlockSpec(memory_space=pltpu.MemorySpace.VMEM)] * 9,
            scratch_shapes=[
                pltpu.VMEM((layers, 3, rows, cols), f32),
                pltpu.VMEM((layers, 4, rows, cols), f32),
                pltpu.VMEM((layers, 2, half, cols), f32),
                pltpu.VMEM((layers, 2, half, cols), f32),
                pltpu.VMEM((layers, 2, half, cols), f32),
                pltpu.VMEM(norm_grads.shape, f32),
                pltpu.VMEM((layers, LANES), f32),
                pltpu.VMEM((layers, zs, 1, LANES), f32),
                pltpu.VMEM((layers, 2, 1, cols // 2), f32),
                pltpu.VMEM((layers, 1, cols // 2), f32),
                pltpu.VMEM((layers, ds // 2, 1, cols // 2), f32),
                pltpu.VMEM((layers, 2, 1, cols // 2), f32),
                pltpu.VMEM((DIRECT, ds, 1, cols), f32),
                pltpu.VMEM((layers, 2 * zs, 1, LANES), f32),
                pltpu.VMEM((layers, ds // 2, 1, LANES), f32),
                pltpu.VMEM((DIRECT, ds * zs, 1, LANES), f32),
                pltpu.VMEM((ds // 2, 2, layers, LANES), f32),
                pltpu.VMEM((ds // 2, layers, LANES), f32),
                pltpu.VMEM((ds // 2, layers, LANES), f32),
                pltpu.VMEM((ds, 1, 2 * LANES), f32),
                *[dma((n,)) for n in (3, 3, 4, 3, 3, 3, 4, 4, 4, 2, 2, 2, 4, 2, 4, 3, 6, 2, 4, 2)],
                *[dma((DIRECT,))] * 4,
            ],
            compiler_params=pltpu.CompilerParams(collective_id=0, has_side_effects=True, vmem_limit_bytes=50 * 1000 * 1000),
            name='adafactor_step',
        )(weight, grads, row_stat, col_stat, norm_scale, norm_grads, norm_stat)
        return write_out(ds, zs, learn_rate, *outs)

    mat_spec = P(None, 'dp', 'model')
    row_spec = P(None, 'dp')
    col_spec = P(None, 'model')
    return jax.shard_map(local_step, mesh=mesh, in_specs=(mat_spec, mat_spec, row_spec, col_spec, row_spec, row_spec, row_spec, P()), out_specs=(mat_spec, row_spec, col_spec, row_spec, row_spec), check_vma=False)
```

```python
import functools

import jax
import jax.numpy as jnp
from jax import lax
from jax.experimental import pallas as pl
from jax.experimental.pallas import tpu as pltpu
from jax.sharding import PartitionSpec as P

STEP_COUNT = 4
DECAY_POWER = 0.8
EPS_FLOOR = 1e-30
SCALE_FLOOR = 1e-3
CLIP_LIMIT = 1.0
DECAY = 1.0 - STEP_COUNT ** -DECAY_POWER
MESH = pl.DeviceIdType.MESH
LANES = 128
AHEAD = 2
DIRECT = 2
EARLY = 8


def column(row, rows):
    return jnp.transpose(jnp.broadcast_to(row, (LANES, LANES)))[0:rows]


def factors(sums, r_row, rows, zs, rows_total, cols_total):
    count = rows_total * cols_total
    r_mean = sums[:, 2:3] / (rows_total * zs)
    u_rms = jnp.sqrt(sums[:, 0:1] / count * r_mean)
    clip = jnp.maximum(1.0, u_rms / CLIP_LIMIT)
    scale = jnp.maximum(SCALE_FLOOR, jnp.sqrt(sums[:, 1:2] / count))
    return scale, clip, column(lax.rsqrt(r_row / r_mean), rows)


def step_kernel(w_hbm, g_hbm, r_hbm, c_hbm, n_hbm, ng_hbm, v_hbm,
                w_buf, d_buf, r_buf, c_buf, n_buf, dn_buf, v_buf, r_pad, sums_out,
                own, peer, in1x, in1y, in2, early, ng_buf, w_sq,
                r_all, c_mine, c_pair, c_all, c_full, c_last, s_all, t_all, t_last, h_out, h_pair, h_all, k_all,
                load_sem, pair_send, pair_recv, one_send, one_recv, two_send, two_recv,
                r_send, r_recv, cp_send, cp_recv, c_send, c_recv, cf_send, cf_recv,
                s_send, s_recv, t_send, t_recv, w_sem,
                cl_send, cl_recv, tl_send, tl_recv):
    layers, _, rows, cols = own.shape
    half = rows // 2
    ds = c_last.shape[1]
    late = layers - DIRECT
    zs = r_all.shape[1]
    chips = ds // 2
    rows_total, cols_total = rows * ds, cols * zs
    z = lax.axis_index('model')
    d = lax.axis_index('dp')
    chip, core = lax.div(d, 2), lax.rem(d, 2)
    dx = d + 2 - 4 * lax.rem(chip, 2)
    dy = d + 4 - 8 * lax.div(d, 4)
    dxy = dx + dy - d
    dc = d + 1 - 2 * core
    blocks = (dx, dxy, dy, d)
    z_peers = [{'model': lax.rem(z + j, zs)} for j in range(1, zs)]
    d_peers = [{'dp': e} for e in (dc, dx, dx + dc - d, dy, dy + dc - d, dxy, dxy + dc - d)]
    column_peers = [{'dp': dc}] + [{'model': p['model'], 'dp': e} for p in z_peers for e in (d, dc)]
    plane_peers = [{'dp': e} for e in (dx, dy, dxy)]
    others = [{'model': p['model'], **q} for q in d_peers[::-1] for p in z_peers] + d_peers[::-1] + z_peers

    def ring(sem, l):
        return sem.at[lax.rem(l, sem.shape[0])]

    def remote(src, dst, send, recv, where):
        return pltpu.make_async_remote_copy(src_ref=src, dst_ref=dst, send_sem=send, recv_sem=recv,
                                            device_id=where, device_id_type=MESH)

    def spread(ref, send, recv, peers):
        for where in peers:
            remote(ref, ref, send, recv, where).start()

    def drain(ref, sem):
        pltpu.make_async_copy(ref, ref, sem).wait()

    def load_own(l):
        for k in range(3):
            pltpu.make_async_copy(g_hbm.at[l, blocks[k]], own.at[l, k], ring(load_sem, l)).start()
        pltpu.make_async_copy(g_hbm.at[l, d], d_buf.at[l], ring(load_sem, l)).start()

    def pair_copy(l, k, row, source, recv):
        part = pl.ds(row, half)
        return remote(source.at[part], peer.at[l, k, part], ring(pair_send, l), recv, {'dp': dc})

    def from_hbm(l, k):
        return g_hbm.at[l, blocks[k] + dc - d]

    def send_pair(l):
        for k in range(4):
            remote(from_hbm(l, k), peer.at[l, k], ring(pair_send, l), ring(pair_recv, l), {'dp': dc}).start()

    def x1(l):
        return remote(own.at[l, 0:2, 0:half], in1x.at[l], ring(one_send, l), ring(one_recv, l), {'dp': dx})

    def y1(l):
        return remote(own.at[l, 1:3, half:rows], in1y.at[l], ring(one_send, l), ring(one_recv, l), {'dp': dy})

    def y2(l):
        return remote(own.at[l, 2, 0:half], in2.at[l, 0], ring(two_send, l), ring(two_recv, l), {'dp': dy})

    def x2(l):
        return remote(own.at[l, 0, half:rows], in2.at[l, 1], ring(two_send, l), ring(two_recv, l), {'dp': dx})

    def total(buf):
        parts = [buf[j] for j in range(buf.shape[0])]
        while len(parts) > 1:
            parts = [a + b for a, b in zip(parts[::2], parts[1::2])]
        return parts[0]

    def fold(values):
        acc = values[:, 0:LANES]
        for t in range(1, cols // LANES):
            acc = acc + values[:, t * LANES:(t + 1) * LANES]
        return acc

    small = ((r_hbm, r_buf), (c_hbm, c_buf), (n_hbm, n_buf), (ng_hbm, ng_buf), (v_hbm, v_buf))
    groups = (((0, 0), (1, 0)), ((1, half), (2, half)))
    for i, group in enumerate(groups):
        for k, row in group:
            part = pl.ds(row, half)
            pltpu.make_async_copy(from_hbm(0, k).at[part], own.at[layers - 1, i, pl.ds((k - i) * half, half)], w_sem.at[i]).start()
    load_own(0)
    small_sems = (r_send.at[0], r_send.at[1], r_send.at[2], r_send.at[3], cl_send.at[0])
    for (src, dst), sem in zip(small, small_sems):
        pltpu.make_async_copy(src, dst, sem).start()

    barrier = pltpu.get_barrier_semaphore()
    known = d_peers + column_peers[1:]
    for where in known:
        pl.semaphore_signal(barrier, inc=1, device_id=where, device_id_type=MESH)
    pl.semaphore_wait(barrier, len(known))
    for i, (near, row) in enumerate(((dx, 0), (dy, half))):
        for e in (near, near + dc - d):
            remote(g_hbm.at[0, e, pl.ds(row, EARLY)], early.at[i, core], tl_send.at[1], tl_recv.at[1], {'dp': e}).start()
    for i, group in enumerate(groups):
        drain(own.at[layers - 1, i], w_sem.at[i])
        for k, row in group:
            part = pl.ds(row, half)
            remote(own.at[layers - 1, i, pl.ds((k - i) * half, half)], peer.at[0, k, part],
                   pair_send.at[0], two_recv.at[i + 1], {'dp': dc}).start()
    for k, row in ((0, half), (2, 0), (3, 0), (3, half)):
        pair_copy(0, k, row, from_hbm(0, k), two_recv.at[3]).start()
    for l in range(1, AHEAD):
        send_pair(l)
        load_own(l)

    def norm_split():
        for (src, dst), sem in zip(small, small_sems):
            pltpu.make_async_copy(src, dst, sem).wait()
        r_pad[...] = jnp.zeros_like(r_pad)
        r_pad[:, 0:rows] = r_buf[...]
        h_out[...] = jnp.zeros_like(h_out)
        k_all[...] = jnp.zeros_like(k_all)
        for k in range(ds):
            h_out[k // 2, k % 2, :, 0:rows] = ng_buf[:, k * rows:(k + 1) * rows]
        remote(h_out.at[:, 1 - core], h_pair, cl_send.at[0], cl_recv.at[0], {'dp': dc}).start()

    def norm_send():
        remote(h_out.at[:, 1 - core], h_pair, cl_send.at[0], cl_recv.at[0], {'dp': dc}).wait()
        for k in range(chips):
            h_pair[k] = h_pair[k] + h_out[k, core]
        h_all[chip] = h_pair[chip]
        for e in (dx, dy, dxy):
            remote(h_pair.at[lax.div(e, 2)], h_all.at[chip], cl_send.at[1], cl_recv.at[1], {'dp': e}).start()

    def layer_sums(values):
        padded = jnp.concatenate([values, jnp.zeros((layers, LANES - rows), jnp.float32)], axis=1)
        return jnp.sum(jnp.transpose(padded), axis=0, keepdims=True)

    def norm_stats():
        drain(h_all.at[0:chips - 1], cl_recv.at[1])
        drain(h_all.at[0:chips - 1], cl_send.at[1])
        h = total(h_all)[:, 0:rows]
        v_new = DECAY * v_buf[...] + (1.0 - DECAY) * (h * h + EPS_FLOOR)
        v_buf[...] = v_new
        zv = h * lax.rsqrt(v_new)
        nv = n_buf[...]
        k_all[d, :, 0:layers] = layer_sums(zv * zv)
        k_all[d, :, LANES:LANES + layers] = layer_sums(nv * nv)
        spread(k_all.at[d], tl_send.at[0], tl_recv.at[0], d_peers)

    def norm_update():
        drain(k_all.at[0:ds - 1], tl_recv.at[0])
        drain(k_all.at[0:ds - 1], tl_send.at[0])
        acc = total(k_all)
        z_sq, n_sq = acc[:, 0:layers], acc[:, LANES:LANES + layers]
        clip = jnp.maximum(1.0, jnp.sqrt(z_sq / rows_total) / CLIP_LIMIT)
        scale = jnp.maximum(SCALE_FLOOR, jnp.sqrt(n_sq / rows_total))
        clip = jnp.transpose(jnp.broadcast_to(clip, (LANES, layers)))[:, 0:rows]
        scale = jnp.transpose(jnp.broadcast_to(scale, (LANES, layers)))[:, 0:rows]
        zv = total(h_all)[:, 0:rows] * lax.rsqrt(v_buf[...])
        dn_buf[...] = scale * (zv / clip)

    def combine(l, k, part):
        own[l, k, part] = own[l, k, part] + peer[l, k, part]

    first, second = slice(0, half), slice(half, rows)

    def stage_first():
        drain(peer.at[0], load_sem.at[0])
        drain(in1x.at[0], two_recv.at[1])
        combine(0, slice(0, 2), first)
        for k, row in ((0, EARLY), (1, 0)):
            part = pl.ds(row, half - row)
            remote(own.at[0, k, part], in1x.at[0, k, part], one_send.at[0], one_recv.at[0], {'dp': dx}).start()
        drain(in1y.at[0], two_recv.at[2])
        combine(0, slice(1, 3), second)
        for k, row in ((0, 0), (1, EARLY)):
            remote(own.at[0, k + 1, pl.ds(half + row, half - row)], in1y.at[0, k, pl.ds(row, half - row)],
                   one_send.at[0], one_recv.at[0], {'dp': dy}).start()
        drain(peer.at[0, 0:2], two_recv.at[3])
        combine(0, 0, second)
        combine(0, 2, first)
        d_buf[0] = d_buf[0] + peer[0, 3]
        drain(peer.at[0], pair_send.at[0])

    def stage_combine(l):
        drain(peer.at[l], ring(load_sem, l))
        drain(peer.at[l], ring(pair_recv, l))
        combine(l, slice(0, 2), first)
        x1(l).start()
        combine(l, slice(1, 3), second)
        y1(l).start()
        combine(l, 0, second)
        combine(l, 2, first)
        d_buf[l] = d_buf[l] + peer[l, 3]
        drain(peer.at[l], ring(pair_send, l))

    def stage_forward(l):
        pltpu.make_async_copy(w_hbm.at[l], w_buf.at[l], ring(w_sem, l)).start()
        drain(in1x.at[0:2], ring(one_recv, l))
        own[l, 2, 0:half] = own[l, 2, 0:half] + in1x[l, 1]
        own[l, 0, half:rows] = own[l, 0, half:rows] + in1y[l, 0]
        y2(l).start()
        d_buf[l, 0:half] = d_buf[l, 0:half] + in1x[l, 0]
        x2(l).start()
        d_buf[l, half:rows] = d_buf[l, half:rows] + in1y[l, 1]

    first_part = w_buf.at[0:half // 4 - EARLY // 8, 0:16]

    def forward_first():
        drain(first_part, one_recv.at[0])
        own[0, 2, first] = own[0, 2, first] + in1x[0, 1]
        own[0, 0, second] = own[0, 0, second] + in1y[0, 0]
        y2(0).start()
        x2(0).start()
        pltpu.make_async_copy(w_hbm.at[0], w_buf.at[0], w_sem.at[0]).start()
        drain(early, tl_recv.at[1])
        drain(early, tl_send.at[1])
        rest = slice(EARLY, half)
        d_buf[0, 0:EARLY] = d_buf[0, 0:EARLY] + (early[0, 0] + early[0, 1])
        d_buf[0, rest] = d_buf[0, rest] + in1x[0, 0, rest]
        d_buf[0, half:half + EARLY] = d_buf[0, half:half + EARLY] + (early[1, 0] + early[1, 1])
        d_buf[0, half + EARLY:rows] = d_buf[0, half + EARLY:rows] + in1y[0, 1, rest]

    def stage_stats(l):
        drain(w_buf.at[l], ring(w_sem, l))
        w = w_buf[l]
        w_sq[pl.ds(l, 1)] = fold(jnp.sum(w * w, axis=0, keepdims=True))
        drain(in2.at[l], ring(two_recv, l))
        g = d_buf[l] + in2[l].reshape(rows, cols)
        d_buf[l] = g
        q = g * g + EPS_FLOOR
        col = jnp.sum(q, axis=0, keepdims=True)

        @pl.when(l < late)
        def _():
            c_mine[l, 0] = col[:, 0:cols // 2]
            c_mine[l, 1] = col[:, cols // 2:cols]

        @pl.when(l >= late)
        def _():
            c_last[l - late, d] = col

        p = jnp.concatenate([fold(q), jnp.zeros((LANES - rows, LANES), jnp.float32)], axis=0)
        r_all[l, z] = jnp.sum(jnp.transpose(p), axis=0, keepdims=True)

        @pl.when(l < late)
        def _():
            pair_columns(l).start()

        @pl.when(l >= late)
        def _():
            e = l - late
            spread(c_last.at[e, d], cl_send.at[e], cl_recv.at[e], d_peers)

        spread(r_all.at[l, z], ring(r_send, l), ring(r_recv, l), z_peers)

    def pair_columns(l):
        return remote(c_mine.at[l, 1 - core], c_pair.at[l], ring(cp_send, l), ring(cp_recv, l), {'dp': dc})

    def full_columns(l):
        return remote(c_full.at[l, core], c_full.at[l, core], ring(cf_send, l), ring(cf_recv, l), {'dp': dc})

    def drain_rows(l):
        if zs > 1:
            drain(r_all.at[l, 0:zs - 1], ring(r_recv, l))
            drain(r_all.at[l, 0:zs - 1], ring(r_send, l))

    def stage_columns(l):
        pair_columns(l).wait()
        drain_rows(l)
        c_all[l, chip] = c_mine[l, core] + c_pair[l]
        spread(c_all.at[l, chip], ring(c_send, l), ring(c_recv, l), plane_peers)

    def stage_share(l):
        drain(c_all.at[l, 0:chips - 1], ring(c_recv, l))
        drain(c_all.at[l, 0:chips - 1], ring(c_send, l))
        c_full[l, core] = total(c_all.at[l])
        full_columns(l).start()

    def stage_moments(l):
        @pl.when(l < late)
        def _():
            full_columns(l).wait()

        @pl.when(l >= late)
        def _():
            e = l - late
            drain(c_last.at[e, 0:ds - 1], cl_recv.at[e])
            drain(c_last.at[e, 0:ds - 1], cl_send.at[e])
            drain_rows(l)
            col = total(c_last.at[e])
            c_full[l, 0] = col[:, 0:cols // 2]
            c_full[l, 1] = col[:, cols // 2:cols]

        col = jnp.concatenate([c_full[l, 0], c_full[l, 1]], axis=1)
        r_new = DECAY * r_pad[pl.ds(l, 1)] + (1.0 - DECAY) * (total(r_all.at[l]) / cols_total)
        c_new = DECAY * c_buf[pl.ds(l, 1)] + (1.0 - DECAY) * (col / rows_total)
        r_pad[pl.ds(l, 1)] = r_new
        r_buf[pl.ds(l, 1)] = r_new[:, 0:rows]
        c_buf[pl.ds(l, 1)] = c_new
        a = column(lax.rsqrt(r_new), rows)
        b = lax.rsqrt(c_new)
        acc = jnp.zeros((1, LANES), jnp.float32)
        for t in range(cols // LANES):
            sl = slice(t * LANES, (t + 1) * LANES)
            u = d_buf[l, :, sl] * a * b[:, sl]
            acc = acc + jnp.sum(u * u, axis=0, keepdims=True)
        lane = lax.broadcasted_iota(jnp.int32, (1, LANES), 1)
        row = jnp.where(lane == 0, jnp.sum(acc, axis=1, keepdims=True), 0.0)
        row = jnp.where(lane == 1, jnp.sum(w_sq[pl.ds(l, 1)], axis=1, keepdims=True), row)
        row = jnp.where(lane == 2, jnp.sum(r_new, axis=1, keepdims=True), row)

        @pl.when(l < late)
        def _():
            s_all[l, 2 * z + core] = row
            spread(s_all.at[l, 2 * z + core], ring(s_send, l), ring(s_recv, l), column_peers)

        @pl.when(l >= late)
        def _():
            e = l - late
            me = ds * z + d
            t_last[e, me] = row
            spread(t_last.at[e, me], tl_send.at[e], tl_recv.at[e], others)

    def stage_gather(l):
        drain(s_all.at[l, 0:2 * zs - 1], ring(s_recv, l))
        drain(s_all.at[l, 0:2 * zs - 1], ring(s_send, l))
        t_all[l, chip] = total(s_all.at[l])
        spread(t_all.at[l, chip], ring(t_send, l), ring(t_recv, l), plane_peers)

    def stage_update(l):
        drain(t_all.at[l, 0:chips - 1], ring(t_recv, l))
        drain(t_all.at[l, 0:chips - 1], ring(t_send, l))
        scale, clip, a = factors(total(t_all.at[l]), r_pad[pl.ds(l, 1)], rows, zs, rows_total, cols_total)
        b = lax.rsqrt(c_buf[pl.ds(l, 1)]) / clip
        for t in range(cols // LANES):
            sl = slice(t * LANES, (t + 1) * LANES)
            d_buf[l, :, sl] = d_buf[l, :, sl] * a * b[:, sl] * scale

    def stage_final(e):
        drain(t_last.at[e, 0:ds * zs - 1], tl_recv.at[e])
        drain(t_last.at[e, 0:ds * zs - 1], tl_send.at[e])
        sums_out[e] = total(t_last.at[e])

    def drain_one(l):
        drain(in1x.at[0:2], ring(one_send, l))

    def drain_two(l):
        drain(in2.at[l], ring(two_send, l))

    def at(i, lag, stage, begin=0, end=layers):
        @pl.when((i >= begin + lag) & (i < end + lag))
        def _():
            stage(i - lag)

    def once(i, when, stage):
        @pl.when(i == when)
        def _():
            stage()

    def prefetch(l):
        load_own(l)
        send_pair(l)

    def body(i, carry):
        at(i, -AHEAD, prefetch)
        at(i, 0, stage_combine, 1)
        once(i, 0, stage_first)
        at(i, 1, stage_forward, 1)
        once(i, 1, forward_first)
        once(i, 1, norm_split)
        once(i, 2, norm_send)
        at(i, 3, stage_columns, 0, late)
        at(i, 4, stage_share, 0, late)
        at(i, 5, stage_moments)
        at(i, 7, stage_gather, 0, late)
        at(i, 8, stage_update, 0, late)
        at(i, 2, drain_one, 1)
        once(i, 2, lambda: drain(first_part, one_send.at[0]))
        at(i, 3, drain_two)
        once(i, 4, norm_stats)
        once(i, 6, norm_update)
        at(i, 2, stage_stats)
        return carry

    lax.fori_loop(0, late + 8, body, 0)
    for e in range(DIRECT):
        stage_final(e)


def write_kernel(ds, zs, rate_ref, w, d, r, c, n, dn, v, r_pad, sums, wo, ro, co, no, vo, w_new, n_new, sem):
    layers, rows, cols = w.shape
    late = layers - DIRECT
    rate = rate_ref[...]
    pairs = ((r, ro), (c, co), (v, vo), (n_new, no))
    for i in range(3):
        pltpu.make_async_copy(*pairs[i], sem.at[i]).start()
    n_new[...] = n[...] - rate * dn[...]
    for l in range(layers + 1):
        if l < late:
            w_new[l] = w[l] - rate * d[l]
        elif l < layers:
            scale, clip, a = factors(sums[l - late], r_pad[l:l + 1], rows, zs, rows * ds, cols * zs)
            b = lax.rsqrt(c[l:l + 1]) / clip
            for t in range(cols // LANES):
                sl = slice(t * LANES, (t + 1) * LANES)
                w_new[l, :, sl] = w[l, :, sl] - rate * (d[l, :, sl] * a * b[:, sl] * scale)
        if l == 1:
            pltpu.make_async_copy(*pairs[3], sem.at[3]).start()
        if l >= 1:
            pltpu.make_async_copy(w_new.at[l - 1], wo.at[l - 1], sem.at[4]).start()
    for i, pair in enumerate(pairs):
        pltpu.make_async_copy(*pair, sem.at[i]).wait()
    pltpu.make_async_copy(w_new, wo, sem.at[4]).wait()


def write_out(ds, zs, rate, w, d, r, c, n, dn, v, r_pad, sums):
    return pl.pallas_call(
        functools.partial(write_kernel, ds, zs),
        out_shape=[jax.ShapeDtypeStruct(a.shape, a.dtype) for a in (w, r, c, n, v)],
        in_specs=[pl.BlockSpec(memory_space=pltpu.MemorySpace.SMEM)] + [pl.BlockSpec(memory_space=pltpu.MemorySpace.VMEM)] * 9,
        out_specs=[pl.BlockSpec(memory_space=pltpu.MemorySpace.HBM)] * 5,
        scratch_shapes=[pltpu.VMEM(w.shape, w.dtype), pltpu.VMEM(n.shape, n.dtype), pltpu.SemaphoreType.DMA((5,))],
        compiler_params=pltpu.CompilerParams(vmem_limit_bytes=8 << 20),
        name='write_out',
    )(rate, w, d, r, c, n, dn, v, r_pad, sums)


def solution(mesh):
    ds = mesh.shape['dp']
    zs = mesh.shape['model']

    def local_step(weight, grad_parts, row_stat, col_stat, norm_scale, norm_grads, norm_stat, learn_rate):
        layers, rows, cols = weight.shape
        half = rows // 2
        f32 = jnp.float32
        grads = grad_parts.reshape(layers, ds, rows, cols)
        any_spec = pl.BlockSpec(memory_space=pltpu.MemorySpace.HBM)
        dma = pltpu.SemaphoreType.DMA
        outs = pl.pallas_call(
            step_kernel,
            out_shape=[pltpu.VMEM(a.shape, f32) for a in (weight, weight, row_stat, col_stat, norm_scale, norm_scale, norm_stat)]
            + [pltpu.VMEM((layers, LANES), f32), pltpu.VMEM((DIRECT, 1, LANES), f32)],
            in_specs=[any_spec] * 7,
            out_specs=[pl.BlockSpec(memory_space=pltpu.MemorySpace.VMEM)] * 9,
            scratch_shapes=[
                pltpu.VMEM((layers, 3, rows, cols), f32),
                pltpu.VMEM((layers, 4, rows, cols), f32),
                pltpu.VMEM((layers, 2, half, cols), f32),
                pltpu.VMEM((layers, 2, half, cols), f32),
                pltpu.VMEM((layers, 2, half, cols), f32),
                pltpu.VMEM((2, 2, EARLY, cols), f32),
                pltpu.VMEM(norm_grads.shape, f32),
                pltpu.VMEM((layers, LANES), f32),
                pltpu.VMEM((layers, zs, 1, LANES), f32),
                pltpu.VMEM((layers, 2, 1, cols // 2), f32),
                pltpu.VMEM((layers, 1, cols // 2), f32),
                pltpu.VMEM((layers, ds // 2, 1, cols // 2), f32),
                pltpu.VMEM((layers, 2, 1, cols // 2), f32),
                pltpu.VMEM((DIRECT, ds, 1, cols), f32),
                pltpu.VMEM((layers, 2 * zs, 1, LANES), f32),
                pltpu.VMEM((layers, ds // 2, 1, LANES), f32),
                pltpu.VMEM((DIRECT, ds * zs, 1, LANES), f32),
                pltpu.VMEM((ds // 2, 2, layers, LANES), f32),
                pltpu.VMEM((ds // 2, layers, LANES), f32),
                pltpu.VMEM((ds // 2, layers, LANES), f32),
                pltpu.VMEM((ds, 1, 2 * LANES), f32),
                *[dma((n,)) for n in (3, 3, 4, 3, 3, 3, 4, 4, 4, 2, 2, 2, 4, 2, 4, 3, 6, 2, 4, 2)],
                *[dma((DIRECT,))] * 4,
            ],
            compiler_params=pltpu.CompilerParams(collective_id=0, has_side_effects=True, vmem_limit_bytes=50 * 1000 * 1000),
            name='adafactor_step',
        )(weight, grads, row_stat, col_stat, norm_scale, norm_grads, norm_stat)
        return write_out(ds, zs, learn_rate, *outs)

    mat_spec = P(None, 'dp', 'model')
    row_spec = P(None, 'dp')
    col_spec = P(None, 'model')
    return jax.shard_map(local_step, mesh=mesh, in_specs=(mat_spec, mat_spec, row_spec, col_spec, row_spec, row_spec, row_spec, P()), out_specs=(mat_spec, row_spec, col_spec, row_spec, row_spec), check_vma=False)
```

```python
import functools

import jax
import jax.numpy as jnp
from jax import lax
from jax.experimental import pallas as pl
from jax.experimental.pallas import tpu as pltpu
from jax.sharding import PartitionSpec as P

STEP_COUNT = 4
DECAY_POWER = 0.8
EPS_FLOOR = 1e-30
SCALE_FLOOR = 1e-3
CLIP_LIMIT = 1.0
DECAY = 1.0 - STEP_COUNT ** -DECAY_POWER
MESH = pl.DeviceIdType.MESH
LANES = 128
AHEAD = 2
DIRECT = 2
EARLY = 8


def column(row, rows):
    return jnp.transpose(jnp.broadcast_to(row, (LANES, LANES)))[0:rows]


def factors(sums, r_row, rate, rows, zs, rows_total, cols_total):
    count = rows_total * cols_total
    r_mean = sums[:, 2:3] / (rows_total * zs)
    u_rms = jnp.sqrt(sums[:, 0:1] / count * r_mean)
    clip = jnp.maximum(1.0, u_rms / CLIP_LIMIT)
    scale = rate * jnp.maximum(SCALE_FLOOR, jnp.sqrt(sums[:, 1:2] / count))
    return scale, clip, column(lax.rsqrt(r_row / r_mean), rows)


def step_kernel(w_hbm, g_hbm, r_hbm, c_hbm, n_hbm, ng_hbm, v_hbm, rate_ref,
                w_buf, d_buf, r_buf, c_buf, n_buf, v_buf, r_pad, sums_out,
                own, peer, in1x, in1y, in2, early, ng_buf, w_sq,
                r_all, c_mine, c_pair, c_all, c_full, c_last, s_all, t_all, t_last, held, h_out, h_all, k_all,
                load_sem, pair_send, pair_recv, one_send, one_recv, two_send, two_recv,
                r_send, r_recv, cp_send, cp_recv, c_send, c_recv, cf_send, cf_recv,
                s_send, s_recv, t_send, t_recv, w_sem,
                cl_send, cl_recv, tl_send, tl_recv):
    layers, _, rows, cols = own.shape
    half = rows // 2
    last, ds = layers - 1, c_last.shape[0]
    late = layers - DIRECT
    zs = r_all.shape[1]
    chips = ds // 2
    rows_total, cols_total = rows * ds, cols * zs
    z = lax.axis_index('model')
    d = lax.axis_index('dp')
    chip, core = lax.div(d, 2), lax.rem(d, 2)
    dx = d + 2 - 4 * lax.rem(chip, 2)
    dy = d + 4 - 8 * lax.div(d, 4)
    dxy = dx + dy - d
    dc = d + 1 - 2 * core
    blocks = (dx, dxy, dy, d)
    z_peers = [{'model': lax.rem(z + j, zs)} for j in range(1, zs)]
    d_peers = [{'dp': e} for e in (dc, dx, dx + dc - d, dy, dy + dc - d, dxy, dxy + dc - d)]
    column_peers = [{'dp': dc}] + [{'model': p['model'], 'dp': e} for p in z_peers for e in (d, dc)]
    plane_peers = [{'dp': e} for e in (dx, dy, dxy)]
    others = [{'model': p['model'], **q} for q in d_peers[::-1] for p in z_peers] + d_peers[::-1] + z_peers

    def ring(sem, l):
        return sem.at[lax.rem(l, sem.shape[0])]

    def remote(src, dst, send, recv, where):
        return pltpu.make_async_remote_copy(src_ref=src, dst_ref=dst, send_sem=send, recv_sem=recv,
                                            device_id=where, device_id_type=MESH)

    def spread(ref, send, recv, peers):
        for where in peers:
            remote(ref, ref, send, recv, where).start()

    def drain(ref, sem):
        pltpu.make_async_copy(ref, ref, sem).wait()

    def load_own(l):
        for k in range(3):
            pltpu.make_async_copy(g_hbm.at[l, blocks[k]], own.at[l, k], ring(load_sem, l)).start()
        pltpu.make_async_copy(g_hbm.at[l, d], d_buf.at[l], ring(load_sem, l)).start()

    def pair_copy(l, k, row, source, recv):
        part = pl.ds(row, half)
        return remote(source.at[part], peer.at[l, k, part], ring(pair_send, l), recv, {'dp': dc})

    def from_hbm(l, k):
        return g_hbm.at[l, blocks[k] + dc - d]

    def send_pair(l):
        for k in range(4):
            remote(from_hbm(l, k), peer.at[l, k], ring(pair_send, l), ring(pair_recv, l), {'dp': dc}).start()

    def x1(l):
        return remote(own.at[l, 0:2, 0:half], in1x.at[l], ring(one_send, l), ring(one_recv, l), {'dp': dx})

    def y1(l):
        return remote(own.at[l, 1:3, half:rows], in1y.at[l], ring(one_send, l), ring(one_recv, l), {'dp': dy})

    def y2(l):
        return remote(own.at[l, 2, 0:half], in2.at[l, 0], ring(two_send, l), ring(two_recv, l), {'dp': dy})

    def x2(l):
        return remote(own.at[l, 0, half:rows], in2.at[l, 1], ring(two_send, l), ring(two_recv, l), {'dp': dx})

    def total(buf):
        parts = [buf[j] for j in range(buf.shape[0])]
        while len(parts) > 1:
            parts = [a + b for a, b in zip(parts[::2], parts[1::2])]
        return parts[0]

    def fold(values):
        acc = values[:, 0:LANES]
        for t in range(1, cols // LANES):
            acc = acc + values[:, t * LANES:(t + 1) * LANES]
        return acc

    small = ((r_hbm, r_buf), (c_hbm, c_buf), (n_hbm, n_buf), (ng_hbm, ng_buf), (v_hbm, v_buf))
    groups = (((0, 0), (1, 0)), ((1, half), (2, half)))
    for i, group in enumerate(groups):
        for k, row in group:
            part = pl.ds(row, half)
            pltpu.make_async_copy(from_hbm(0, k).at[part], own.at[layers - 1, i, pl.ds((k - i) * half, half)], w_sem.at[i]).start()
    load_own(0)
    small_sems = (r_send.at[0], r_send.at[1], r_send.at[2], r_send.at[3], cl_send.at[0])
    for (src, dst), sem in zip(small, small_sems):
        pltpu.make_async_copy(src, dst, sem).start()

    barrier = pltpu.get_barrier_semaphore()
    known = d_peers + column_peers[1:]
    for where in known:
        pl.semaphore_signal(barrier, inc=1, device_id=where, device_id_type=MESH)
    pl.semaphore_wait(barrier, len(known))
    for i, (near, row) in enumerate(((dx, 0), (dy, half))):
        for e in (near, near + dc - d):
            remote(g_hbm.at[0, e, pl.ds(row, EARLY)], early.at[i, core], tl_send.at[1], tl_recv.at[1], {'dp': e}).start()
    for i, group in enumerate(groups):
        drain(own.at[layers - 1, i], w_sem.at[i])
        for k, row in group:
            part = pl.ds(row, half)
            remote(own.at[layers - 1, i, pl.ds((k - i) * half, half)], peer.at[0, k, part],
                   pair_send.at[0], two_recv.at[i + 1], {'dp': dc}).start()
    for k, row in ((0, half), (2, 0), (3, 0), (3, half)):
        pair_copy(0, k, row, from_hbm(0, k), two_recv.at[3]).start()
    for l in range(1, AHEAD):
        send_pair(l)
        load_own(l)

    def norm_split():
        for i in (0, 1, 2, 4):
            pltpu.make_async_copy(*small[i], small_sems[i]).wait()
        r_pad[...] = jnp.zeros_like(r_pad)
        r_pad[:, 0:rows] = r_buf[...]
        k_all[...] = jnp.zeros_like(k_all)

    h_out[...] = jnp.zeros_like(h_out)
    pltpu.make_async_copy(*small[3], small_sems[3]).wait()
    for k in range(ds):
        h_out[k, :, 0:rows] = ng_buf[:, k * rows:(k + 1) * rows]
    h_all[d] = h_out[d]
    for where in d_peers:
        remote(h_out.at[where['dp']], h_all.at[d], cl_send.at[1], cl_recv.at[1], where).start()

    def layer_sums(values):
        padded = jnp.concatenate([values, jnp.zeros((layers, LANES - rows), jnp.float32)], axis=1)
        return jnp.sum(jnp.transpose(padded), axis=0, keepdims=True)

    def norm_stats():
        drain(h_all.at[0:ds - 1], cl_recv.at[1])
        drain(h_all.at[0:ds - 1], cl_send.at[1])
        h = total(h_all)[:, 0:rows]
        v_new = DECAY * v_buf[...] + (1.0 - DECAY) * (h * h + EPS_FLOOR)
        v_buf[...] = v_new
        zv = h * lax.rsqrt(v_new)
        nv = n_buf[...]
        k_all[d, :, 0:layers] = layer_sums(zv * zv)
        k_all[d, :, LANES:LANES + layers] = layer_sums(nv * nv)
        spread(k_all.at[d], tl_send.at[0], tl_recv.at[0], d_peers)

    def norm_update():
        drain(k_all.at[0:ds - 1], tl_recv.at[0])
        drain(k_all.at[0:ds - 1], tl_send.at[0])
        acc = total(k_all)
        z_sq, n_sq = acc[:, 0:layers], acc[:, LANES:LANES + layers]
        clip = jnp.maximum(1.0, jnp.sqrt(z_sq / rows_total) / CLIP_LIMIT)
        scale = rate_ref[...] * jnp.maximum(SCALE_FLOOR, jnp.sqrt(n_sq / rows_total))
        clip = jnp.transpose(jnp.broadcast_to(clip, (LANES, layers)))[:, 0:rows]
        scale = jnp.transpose(jnp.broadcast_to(scale, (LANES, layers)))[:, 0:rows]
        zv = total(h_all)[:, 0:rows] * lax.rsqrt(v_buf[...])
        n_buf[...] = n_buf[...] - scale * (zv / clip)

    def combine(l, k, part):
        own[l, k, part] = own[l, k, part] + peer[l, k, part]

    first, second = slice(0, half), slice(half, rows)

    def stage_first():
        drain(peer.at[0], load_sem.at[0])
        drain(in1x.at[0], two_recv.at[1])
        combine(0, slice(0, 2), first)
        for k, row in ((0, EARLY), (1, 0)):
            part = pl.ds(row, half - row)
            remote(own.at[0, k, part], in1x.at[0, k, part], one_send.at[0], one_recv.at[0], {'dp': dx}).start()
        drain(in1y.at[0], two_recv.at[2])
        combine(0, slice(1, 3), second)
        for k, row in ((0, 0), (1, EARLY)):
            remote(own.at[0, k + 1, pl.ds(half + row, half - row)], in1y.at[0, k, pl.ds(row, half - row)],
                   one_send.at[0], one_recv.at[0], {'dp': dy}).start()
        drain(peer.at[0, 0:2], two_recv.at[3])
        combine(0, 0, second)
        combine(0, 2, first)
        d_buf[0] = d_buf[0] + peer[0, 3]
        drain(peer.at[0], pair_send.at[0])

    def stage_combine(l):
        drain(peer.at[l], ring(load_sem, l))
        drain(peer.at[l], ring(pair_recv, l))
        combine(l, slice(0, 2), first)
        x1(l).start()
        combine(l, slice(1, 3), second)
        y1(l).start()
        combine(l, 0, second)
        combine(l, 2, first)
        d_buf[l] = d_buf[l] + peer[l, 3]
        drain(peer.at[l], ring(pair_send, l))

    def stage_forward(l):
        pltpu.make_async_copy(w_hbm.at[l], w_buf.at[l], ring(w_sem, l)).start()
        drain(in1x.at[0:2], ring(one_recv, l))
        own[l, 2, 0:half] = own[l, 2, 0:half] + in1x[l, 1]
        own[l, 0, half:rows] = own[l, 0, half:rows] + in1y[l, 0]
        y2(l).start()
        d_buf[l, 0:half] = d_buf[l, 0:half] + in1x[l, 0]
        x2(l).start()
        d_buf[l, half:rows] = d_buf[l, half:rows] + in1y[l, 1]

    first_part = w_buf.at[0:half // 4 - EARLY // 8, 0:16]

    def forward_first():
        drain(first_part, one_recv.at[0])
        own[0, 2, first] = own[0, 2, first] + in1x[0, 1]
        own[0, 0, second] = own[0, 0, second] + in1y[0, 0]
        y2(0).start()
        x2(0).start()
        pltpu.make_async_copy(w_hbm.at[0], w_buf.at[0], w_sem.at[0]).start()
        drain(early, tl_recv.at[1])
        drain(early, tl_send.at[1])
        rest = slice(EARLY, half)
        d_buf[0, 0:EARLY] = d_buf[0, 0:EARLY] + (early[0, 0] + early[0, 1])
        d_buf[0, rest] = d_buf[0, rest] + in1x[0, 0, rest]
        d_buf[0, half:half + EARLY] = d_buf[0, half:half + EARLY] + (early[1, 0] + early[1, 1])
        d_buf[0, half + EARLY:rows] = d_buf[0, half + EARLY:rows] + in1y[0, 1, rest]

    def stage_stats(l):
        drain(w_buf.at[l], ring(w_sem, l))
        w = w_buf[l]
        w_sq[pl.ds(l, 1)] = fold(jnp.sum(w * w, axis=0, keepdims=True))
        drain(in2.at[l], ring(two_recv, l))
        g = d_buf[l] + in2[l].reshape(rows, cols)
        d_buf[l] = g
        q = g * g + EPS_FLOOR
        col = jnp.sum(q, axis=0, keepdims=True)

        @pl.when(l < last)
        def _():
            c_mine[l, 0] = col[:, 0:cols // 2]
            c_mine[l, 1] = col[:, cols // 2:cols]

        @pl.when(l == last)
        def _():
            c_last[d] = col

        p = jnp.concatenate([fold(q), jnp.zeros((LANES - rows, LANES), jnp.float32)], axis=0)
        r_all[l, z] = jnp.sum(jnp.transpose(p), axis=0, keepdims=True)

        @pl.when(l < last)
        def _():
            pair_columns(l).start()

        @pl.when(l == last)
        def _():
            spread(c_last.at[d], cl_send.at[0], cl_recv.at[0], d_peers)

        spread(r_all.at[l, z], ring(r_send, l), ring(r_recv, l), z_peers)

    def pair_columns(l):
        return remote(c_mine.at[l, 1 - core], c_pair.at[l], ring(cp_send, l), ring(cp_recv, l), {'dp': dc})

    def full_columns(l):
        return remote(c_full.at[l, core], c_full.at[l, core], ring(cf_send, l), ring(cf_recv, l), {'dp': dc})

    def drain_rows(l):
        if zs > 1:
            drain(r_all.at[l, 0:zs - 1], ring(r_recv, l))
            drain(r_all.at[l, 0:zs - 1], ring(r_send, l))

    def stage_columns(l):
        pair_columns(l).wait()
        drain_rows(l)
        c_all[l, chip] = c_mine[l, core] + c_pair[l]
        spread(c_all.at[l, chip], ring(c_send, l), ring(c_recv, l), plane_peers)

    def stage_share(l):
        drain(c_all.at[l, 0:chips - 1], ring(c_recv, l))
        drain(c_all.at[l, 0:chips - 1], ring(c_send, l))
        c_full[l, core] = total(c_all.at[l])
        full_columns(l).start()

    def stage_moments(l):
        @pl.when(l < last)
        def _():
            full_columns(l).wait()

        @pl.when(l == last)
        def _():
            drain(c_last.at[0:ds - 1], cl_recv.at[0])
            drain(c_last.at[0:ds - 1], cl_send.at[0])
            drain_rows(l)
            col = total(c_last)
            c_full[l, 0] = col[:, 0:cols // 2]
            c_full[l, 1] = col[:, cols // 2:cols]

        col = jnp.concatenate([c_full[l, 0], c_full[l, 1]], axis=1)
        r_new = DECAY * r_pad[pl.ds(l, 1)] + (1.0 - DECAY) * (total(r_all.at[l]) / cols_total)
        c_new = DECAY * c_buf[pl.ds(l, 1)] + (1.0 - DECAY) * (col / rows_total)
        r_pad[pl.ds(l, 1)] = r_new
        r_buf[pl.ds(l, 1)] = r_new[:, 0:rows]
        c_buf[pl.ds(l, 1)] = c_new
        a = column(lax.rsqrt(r_new), rows)
        b = lax.rsqrt(c_new)
        acc = jnp.zeros((1, LANES), jnp.float32)
        for t in range(cols // LANES):
            sl = slice(t * LANES, (t + 1) * LANES)
            u = d_buf[l, :, sl] * a * b[:, sl]
            acc = acc + jnp.sum(u * u, axis=0, keepdims=True)
        lane = lax.broadcasted_iota(jnp.int32, (1, LANES), 1)
        lane = lane - jnp.where(l == late, 3, 0)
        row = jnp.where(lane == 0, jnp.sum(acc, axis=1, keepdims=True), 0.0)
        row = jnp.where(lane == 1, jnp.sum(w_sq[pl.ds(l, 1)], axis=1, keepdims=True), row)
        row = jnp.where(lane == 2, jnp.sum(r_new, axis=1, keepdims=True), row)

        @pl.when(l < late)
        def _():
            s_all[l, 2 * z + core] = row
            spread(s_all.at[l, 2 * z + core], ring(s_send, l), ring(s_recv, l), column_peers)

        @pl.when(l == late)
        def _():
            held[...] = row

        @pl.when(l == last)
        def _():
            me = ds * z + d
            t_last[me] = row + held[...]
            spread(t_last.at[me], tl_send.at[0], tl_recv.at[0], others)

    def stage_gather(l):
        drain(s_all.at[l, 0:2 * zs - 1], ring(s_recv, l))
        drain(s_all.at[l, 0:2 * zs - 1], ring(s_send, l))
        t_all[l, chip] = total(s_all.at[l])
        spread(t_all.at[l, chip], ring(t_send, l), ring(t_recv, l), plane_peers)

    def stage_update(l):
        drain(t_all.at[l, 0:chips - 1], ring(t_recv, l))
        drain(t_all.at[l, 0:chips - 1], ring(t_send, l))
        scale, clip, a = factors(total(t_all.at[l]), r_pad[pl.ds(l, 1)], rate_ref[...], rows, zs, rows_total, cols_total)
        b = lax.rsqrt(c_buf[pl.ds(l, 1)]) / clip
        for t in range(cols // LANES):
            sl = slice(t * LANES, (t + 1) * LANES)
            w_buf[l, :, sl] = w_buf[l, :, sl] - scale * (d_buf[l, :, sl] * a * b[:, sl])

    def stage_final():
        drain(t_last.at[0:ds * zs - 1], tl_recv.at[0])
        sums_out[...] = total(t_last)
        drain(t_last.at[0:ds * zs - 1], tl_send.at[0])

    def drain_one(l):
        drain(in1x.at[0:2], ring(one_send, l))

    def drain_two(l):
        drain(in2.at[l], ring(two_send, l))

    def at(i, lag, stage, begin=0, end=layers):
        @pl.when((i >= begin + lag) & (i < end + lag))
        def _():
            stage(i - lag)

    def once(i, when, stage):
        @pl.when(i == when)
        def _():
            stage()

    def prefetch(l):
        load_own(l)
        send_pair(l)

    def body(i, carry):
        at(i, -AHEAD, prefetch)
        at(i, 0, stage_combine, 1)
        once(i, 0, stage_first)
        at(i, 1, stage_forward, 1)
        once(i, 1, forward_first)
        once(i, 1, norm_split)
        at(i, 3, stage_columns, 0, last)
        at(i, 4, stage_share, 0, last)
        at(i, 5, stage_moments)
        at(i, 7, stage_gather, 0, late)
        at(i, 8, stage_update, 0, late)
        at(i, 2, drain_one, 1)
        once(i, 2, lambda: drain(first_part, one_send.at[0]))
        at(i, 3, drain_two)
        once(i, 4, norm_stats)
        once(i, 6, norm_update)
        at(i, 2, stage_stats)
        return carry

    lax.fori_loop(0, late + 8, body, 0)
    stage_final()


def write_kernel(ds, zs, rate_ref, w, d, r, c, n, v, r_pad, sums, wo, ro, co, no, vo, w_new, sem):
    layers, rows, cols = w.shape
    late = layers - DIRECT
    pairs = ((w.at[0:late], wo.at[0:late]), (r, ro), (c, co), (v, vo), (n, no))
    for i, pair in enumerate(pairs):
        pltpu.make_async_copy(*pair, sem.at[i]).start()
    for e in range(DIRECT):
        l = late + e
        lane = 3 * (DIRECT - 1 - e)
        scale, clip, a = factors(sums[:, lane:lane + 3], r_pad[l:l + 1], rate_ref[...], rows, zs, rows * ds, cols * zs)
        b = lax.rsqrt(c[l:l + 1]) / clip
        for t in range(cols // LANES):
            sl = slice(t * LANES, (t + 1) * LANES)
            w_new[e, :, sl] = w[l, :, sl] - scale * (d[l, :, sl] * a * b[:, sl])
    for e in range(DIRECT):
        pltpu.make_async_copy(w_new.at[e], wo.at[late + e], sem.at[5]).start()
    for i, pair in enumerate(pairs):
        pltpu.make_async_copy(*pair, sem.at[i]).wait()
    pltpu.make_async_copy(w_new, wo.at[late:layers], sem.at[5]).wait()


def write_out(ds, zs, rate, w, d, r, c, n, v, r_pad, sums):
    return pl.pallas_call(
        functools.partial(write_kernel, ds, zs),
        out_shape=[jax.ShapeDtypeStruct(a.shape, a.dtype) for a in (w, r, c, n, v)],
        in_specs=[pl.BlockSpec(memory_space=pltpu.MemorySpace.SMEM)] + [pl.BlockSpec(memory_space=pltpu.MemorySpace.VMEM)] * 8,
        out_specs=[pl.BlockSpec(memory_space=pltpu.MemorySpace.HBM)] * 5,
        scratch_shapes=[pltpu.VMEM((DIRECT,) + w.shape[1:], w.dtype), pltpu.SemaphoreType.DMA((6,))],
        compiler_params=pltpu.CompilerParams(vmem_limit_bytes=4 << 20),
        name='write_out',
    )(rate, w, d, r, c, n, v, r_pad, sums)


def solution(mesh):
    ds = mesh.shape['dp']
    zs = mesh.shape['model']

    def local_step(weight, grad_parts, row_stat, col_stat, norm_scale, norm_grads, norm_stat, learn_rate):
        layers, rows, cols = weight.shape
        half = rows // 2
        f32 = jnp.float32
        grads = grad_parts.reshape(layers, ds, rows, cols)
        any_spec = pl.BlockSpec(memory_space=pltpu.MemorySpace.HBM)
        dma = pltpu.SemaphoreType.DMA
        outs = pl.pallas_call(
            step_kernel,
            out_shape=[pltpu.VMEM(a.shape, f32) for a in (weight, weight, row_stat, col_stat, norm_scale, norm_stat)]
            + [pltpu.VMEM((layers, LANES), f32), pltpu.VMEM((1, LANES), f32)],
            in_specs=[any_spec] * 7 + [pl.BlockSpec(memory_space=pltpu.MemorySpace.SMEM)],
            out_specs=[pl.BlockSpec(memory_space=pltpu.MemorySpace.VMEM)] * 8,
            scratch_shapes=[
                pltpu.VMEM((layers, 3, rows, cols), f32),
                pltpu.VMEM((layers, 4, rows, cols), f32),
                pltpu.VMEM((layers, 2, half, cols), f32),
                pltpu.VMEM((layers, 2, half, cols), f32),
                pltpu.VMEM((layers, 2, half, cols), f32),
                pltpu.VMEM((2, 2, EARLY, cols), f32),
                pltpu.VMEM(norm_grads.shape, f32),
                pltpu.VMEM((layers, LANES), f32),
                pltpu.VMEM((layers, zs, 1, LANES), f32),
                pltpu.VMEM((layers, 2, 1, cols // 2), f32),
                pltpu.VMEM((layers, 1, cols // 2), f32),
                pltpu.VMEM((layers, ds // 2, 1, cols // 2), f32),
                pltpu.VMEM((layers, 2, 1, cols // 2), f32),
                pltpu.VMEM((ds, 1, cols), f32),
                pltpu.VMEM((layers, 2 * zs, 1, LANES), f32),
                pltpu.VMEM((layers, ds // 2, 1, LANES), f32),
                pltpu.VMEM((ds * zs, 1, LANES), f32),
                pltpu.VMEM((1, LANES), f32),
                pltpu.VMEM((ds, layers, LANES), f32),
                pltpu.VMEM((ds, layers, LANES), f32),
                pltpu.VMEM((ds, 1, 2 * LANES), f32),
                *[dma((n,)) for n in (3, 3, 5, 3, 3, 3, 4, 4, 4, 2, 2, 2, 4, 2, 4, 3, 6, 2, 4, 2)],
                *[dma((DIRECT,))] * 4,
            ],
            compiler_params=pltpu.CompilerParams(collective_id=0, has_side_effects=True, vmem_limit_bytes=50 * 1000 * 1000),
            name='adafactor_step',
        )(weight, grads, row_stat, col_stat, norm_scale, norm_grads, norm_stat, learn_rate)
        return write_out(ds, zs, learn_rate, *outs)

    mat_spec = P(None, 'dp', 'model')
    row_spec = P(None, 'dp')
    col_spec = P(None, 'model')
    return jax.shard_map(local_step, mesh=mesh, in_specs=(mat_spec, mat_spec, row_spec, col_spec, row_spec, row_spec, row_spec, P()), out_specs=(mat_spec, row_spec, col_spec, row_spec, row_spec), check_vma=False)
```

```python
import functools

import jax
import jax.numpy as jnp
from jax import lax
from jax.experimental import pallas as pl
from jax.experimental.pallas import tpu as pltpu
from jax.sharding import PartitionSpec as P

STEP_COUNT = 4
DECAY_POWER = 0.8
EPS_FLOOR = 1e-30
SCALE_FLOOR = 1e-3
CLIP_LIMIT = 1.0
DECAY = 1.0 - STEP_COUNT ** -DECAY_POWER
MESH = pl.DeviceIdType.MESH
LANES = 128
AHEAD = 2
DIRECT = 2
EARLY = 8


def column(row, rows):
    return jnp.transpose(jnp.broadcast_to(row, (LANES, LANES)))[0:rows]


def factors(sums, r_row, rate, rows, zs, rows_total, cols_total):
    count = rows_total * cols_total
    r_mean = sums[:, 2:3] / (rows_total * zs)
    u_rms = jnp.sqrt(sums[:, 0:1] / count * r_mean)
    clip = jnp.maximum(1.0, u_rms / CLIP_LIMIT)
    scale = rate * jnp.maximum(SCALE_FLOOR, jnp.sqrt(sums[:, 1:2] / count))
    return scale, clip, column(lax.rsqrt(r_row / r_mean), rows)


def step_kernel(w_hbm, g_hbm, r_hbm, c_hbm, n_hbm, ng_hbm, v_hbm, rate_ref,
                w_buf, d_buf, r_buf, c_buf, n_buf, v_buf, r_pad, sums_out,
                own, peer, in1x, in1y, in2, early, ng_buf, w_sq,
                r_all, c_mine, c_pair, c_all, c_full, c_last, s_all, t_all, t_last, held, h_out, h_pair, h_all, k_all,
                load_sem, pair_send, pair_recv, one_send, one_recv, two_send, two_recv,
                r_send, r_recv, cp_send, cp_recv, c_send, c_recv, cf_send, cf_recv,
                s_send, s_recv, t_send, t_recv, w_sem,
                cl_send, cl_recv, tl_send, tl_recv):
    layers, _, rows, cols = own.shape
    half = rows // 2
    last, ds = layers - 1, c_last.shape[0]
    late = layers - DIRECT
    zs = r_all.shape[1]
    chips = ds // 2
    rows_total, cols_total = rows * ds, cols * zs
    z = lax.axis_index('model')
    d = lax.axis_index('dp')
    chip, core = lax.div(d, 2), lax.rem(d, 2)
    dx = d + 2 - 4 * lax.rem(chip, 2)
    dy = d + 4 - 8 * lax.div(d, 4)
    dxy = dx + dy - d
    dc = d + 1 - 2 * core
    blocks = (dx, dxy, dy, d)
    z_peers = [{'model': lax.rem(z + j, zs)} for j in range(1, zs)]
    d_peers = [{'dp': e} for e in (dc, dx, dx + dc - d, dy, dy + dc - d, dxy, dxy + dc - d)]
    column_peers = [{'dp': dc}] + [{'model': p['model'], 'dp': e} for p in z_peers for e in (d, dc)]
    plane_peers = [{'dp': e} for e in (dx, dy, dxy)]
    others = [{'model': p['model'], **q} for q in d_peers[::-1] for p in z_peers] + d_peers[::-1] + z_peers

    def ring(sem, l):
        return sem.at[lax.rem(l, sem.shape[0])]

    def remote(src, dst, send, recv, where):
        return pltpu.make_async_remote_copy(src_ref=src, dst_ref=dst, send_sem=send, recv_sem=recv,
                                            device_id=where, device_id_type=MESH)

    def spread(ref, send, recv, peers):
        for where in peers:
            remote(ref, ref, send, recv, where).start()

    def drain(ref, sem):
        pltpu.make_async_copy(ref, ref, sem).wait()

    def load_own(l):
        for k in range(3):
            pltpu.make_async_copy(g_hbm.at[l, blocks[k]], own.at[l, k], ring(load_sem, l)).start()
        pltpu.make_async_copy(g_hbm.at[l, d], d_buf.at[l], ring(load_sem, l)).start()

    def pair_copy(l, k, row, source, recv):
        part = pl.ds(row, half)
        return remote(source.at[part], peer.at[l, k, part], ring(pair_send, l), recv, {'dp': dc})

    def from_hbm(l, k):
        return g_hbm.at[l, blocks[k] + dc - d]

    def send_pair(l):
        for k in range(4):
            remote(from_hbm(l, k), peer.at[l, k], ring(pair_send, l), ring(pair_recv, l), {'dp': dc}).start()

    def x1(l):
        return remote(own.at[l, 0:2, 0:half], in1x.at[l], ring(one_send, l), ring(one_recv, l), {'dp': dx})

    def y1(l):
        return remote(own.at[l, 1:3, half:rows], in1y.at[l], ring(one_send, l), ring(one_recv, l), {'dp': dy})

    def y2(l):
        return remote(own.at[l, 2, 0:half], in2.at[l, 0], ring(two_send, l), ring(two_recv, l), {'dp': dy})

    def x2(l):
        return remote(own.at[l, 0, half:rows], in2.at[l, 1], ring(two_send, l), ring(two_recv, l), {'dp': dx})

    def total(buf):
        parts = [buf[j] for j in range(buf.shape[0])]
        while len(parts) > 1:
            parts = [a + b for a, b in zip(parts[::2], parts[1::2])]
        return parts[0]

    def fold(values):
        acc = values[:, 0:LANES]
        for t in range(1, cols // LANES):
            acc = acc + values[:, t * LANES:(t + 1) * LANES]
        return acc

    small = ((r_hbm, r_buf), (c_hbm, c_buf), (n_hbm, n_buf), (ng_hbm, ng_buf), (v_hbm, v_buf))
    groups = (((0, 0), (1, 0)), ((1, half), (2, half)))
    for i, group in enumerate(groups):
        for k, row in group:
            part = pl.ds(row, half)
            pltpu.make_async_copy(from_hbm(0, k).at[part], own.at[layers - 1, i, pl.ds((k - i) * half, half)], w_sem.at[i]).start()
    load_own(0)
    small_sems = (r_send.at[0], r_send.at[1], r_send.at[2], r_send.at[3], cl_send.at[0])
    for (src, dst), sem in zip(small, small_sems):
        pltpu.make_async_copy(src, dst, sem).start()

    barrier = pltpu.get_barrier_semaphore()
    known = d_peers + column_peers[1:]
    for where in known:
        pl.semaphore_signal(barrier, inc=1, device_id=where, device_id_type=MESH)
    pl.semaphore_wait(barrier, len(known))
    for i, (near, row) in enumerate(((dx, 0), (dy, half))):
        for e in (near, near + dc - d):
            remote(g_hbm.at[0, e, pl.ds(row, EARLY)], early.at[i, core], tl_send.at[1], tl_recv.at[1], {'dp': e}).start()
    for i, group in enumerate(groups):
        drain(own.at[layers - 1, i], w_sem.at[i])
        for k, row in group:
            part = pl.ds(row, half)
            remote(own.at[layers - 1, i, pl.ds((k - i) * half, half)], peer.at[0, k, part],
                   pair_send.at[0], two_recv.at[i + 1], {'dp': dc}).start()
    for k, row in ((0, half), (2, 0), (3, 0), (3, half)):
        pair_copy(0, k, row, from_hbm(0, k), two_recv.at[3]).start()
    for l in range(1, AHEAD):
        send_pair(l)
        load_own(l)

    def norm_split():
        for (src, dst), sem in zip(small, small_sems):
            pltpu.make_async_copy(src, dst, sem).wait()
        r_pad[...] = jnp.zeros_like(r_pad)
        r_pad[:, 0:rows] = r_buf[...]
        h_out[...] = jnp.zeros_like(h_out)
        k_all[...] = jnp.zeros_like(k_all)
        for k in range(ds):
            h_out[k // 2, k % 2, :, 0:rows] = ng_buf[:, k * rows:(k + 1) * rows]
        remote(h_out.at[:, 1 - core], h_pair, cl_send.at[0], cl_recv.at[0], {'dp': dc}).start()

    def norm_send():
        remote(h_out.at[:, 1 - core], h_pair, cl_send.at[0], cl_recv.at[0], {'dp': dc}).wait()
        for k in range(chips):
            h_pair[k] = h_pair[k] + h_out[k, core]
        h_all[chip] = h_pair[chip]
        for e in (dx, dy, dxy):
            remote(h_pair.at[lax.div(e, 2)], h_all.at[chip], cl_send.at[1], cl_recv.at[1], {'dp': e}).start()

    def layer_sums(values):
        padded = jnp.concatenate([values, jnp.zeros((layers, LANES - rows), jnp.float32)], axis=1)
        return jnp.sum(jnp.transpose(padded), axis=0, keepdims=True)

    def norm_stats():
        drain(h_all.at[0:chips - 1], cl_recv.at[1])
        drain(h_all.at[0:chips - 1], cl_send.at[1])
        h = total(h_all)[:, 0:rows]
        v_new = DECAY * v_buf[...] + (1.0 - DECAY) * (h * h + EPS_FLOOR)
        v_buf[...] = v_new
        zv = h * lax.rsqrt(v_new)
        nv = n_buf[...]
        k_all[d, :, 0:layers] = layer_sums(zv * zv)
        k_all[d, :, LANES:LANES + layers] = layer_sums(nv * nv)
        spread(k_all.at[d], tl_send.at[0], tl_recv.at[0], d_peers)

    def norm_update():
        drain(k_all.at[0:ds - 1], tl_recv.at[0])
        drain(k_all.at[0:ds - 1], tl_send.at[0])
        acc = total(k_all)
        z_sq, n_sq = acc[:, 0:layers], acc[:, LANES:LANES + layers]
        clip = jnp.maximum(1.0, jnp.sqrt(z_sq / rows_total) / CLIP_LIMIT)
        scale = rate_ref[...] * jnp.maximum(SCALE_FLOOR, jnp.sqrt(n_sq / rows_total))
        clip = jnp.transpose(jnp.broadcast_to(clip, (LANES, layers)))[:, 0:rows]
        scale = jnp.transpose(jnp.broadcast_to(scale, (LANES, layers)))[:, 0:rows]
        zv = total(h_all)[:, 0:rows] * lax.rsqrt(v_buf[...])
        n_buf[...] = n_buf[...] - scale * (zv / clip)

    def combine(l, k, part):
        own[l, k, part] = own[l, k, part] + peer[l, k, part]

    first, second = slice(0, half), slice(half, rows)

    def stage_first():
        drain(peer.at[0], load_sem.at[0])
        drain(in1x.at[0], two_recv.at[1])
        combine(0, slice(0, 2), first)
        for k, row in ((0, EARLY), (1, 0)):
            part = pl.ds(row, half - row)
            remote(own.at[0, k, part], in1x.at[0, k, part], one_send.at[0], one_recv.at[0], {'dp': dx}).start()
        drain(in1y.at[0], two_recv.at[2])
        combine(0, slice(1, 3), second)
        for k, row in ((0, 0), (1, EARLY)):
            remote(own.at[0, k + 1, pl.ds(half + row, half - row)], in1y.at[0, k, pl.ds(row, half - row)],
                   one_send.at[0], one_recv.at[0], {'dp': dy}).start()
        drain(peer.at[0, 0:2], two_recv.at[3])
        combine(0, 0, second)
        combine(0, 2, first)
        d_buf[0] = d_buf[0] + peer[0, 3]
        drain(peer.at[0], pair_send.at[0])

    def stage_combine(l):
        drain(peer.at[l], ring(load_sem, l))
        drain(peer.at[l], ring(pair_recv, l))
        combine(l, slice(0, 2), first)
        x1(l).start()
        combine(l, slice(1, 3), second)
        y1(l).start()
        combine(l, 0, second)
        combine(l, 2, first)
        d_buf[l] = d_buf[l] + peer[l, 3]
        drain(peer.at[l], ring(pair_send, l))

    def stage_forward(l):
        pltpu.make_async_copy(w_hbm.at[l], w_buf.at[l], ring(w_sem, l)).start()
        drain(in1x.at[0:2], ring(one_recv, l))
        own[l, 2, 0:half] = own[l, 2, 0:half] + in1x[l, 1]
        own[l, 0, half:rows] = own[l, 0, half:rows] + in1y[l, 0]
        y2(l).start()
        d_buf[l, 0:half] = d_buf[l, 0:half] + in1x[l, 0]
        x2(l).start()
        d_buf[l, half:rows] = d_buf[l, half:rows] + in1y[l, 1]

    first_part = w_buf.at[0:half // 4 - EARLY // 8, 0:16]

    def forward_first():
        drain(first_part, one_recv.at[0])
        own[0, 2, first] = own[0, 2, first] + in1x[0, 1]
        own[0, 0, second] = own[0, 0, second] + in1y[0, 0]
        y2(0).start()
        x2(0).start()
        pltpu.make_async_copy(w_hbm.at[0], w_buf.at[0], w_sem.at[0]).start()
        drain(early, tl_recv.at[1])
        drain(early, tl_send.at[1])
        rest = slice(EARLY, half)
        d_buf[0, 0:EARLY] = d_buf[0, 0:EARLY] + (early[0, 0] + early[0, 1])
        d_buf[0, rest] = d_buf[0, rest] + in1x[0, 0, rest]
        d_buf[0, half:half + EARLY] = d_buf[0, half:half + EARLY] + (early[1, 0] + early[1, 1])
        d_buf[0, half + EARLY:rows] = d_buf[0, half + EARLY:rows] + in1y[0, 1, rest]

    def stage_stats(l):
        drain(w_buf.at[l], ring(w_sem, l))
        w = w_buf[l]
        w_sq[pl.ds(l, 1)] = fold(jnp.sum(w * w, axis=0, keepdims=True))
        drain(in2.at[l], ring(two_recv, l))
        g = d_buf[l] + in2[l].reshape(rows, cols)
        d_buf[l] = g
        q = g * g + EPS_FLOOR
        col = jnp.sum(q, axis=0, keepdims=True)

        @pl.when(l < last)
        def _():
            c_mine[l, 0] = col[:, 0:cols // 2]
            c_mine[l, 1] = col[:, cols // 2:cols]

        @pl.when(l == last)
        def _():
            c_last[d] = col

        p = jnp.concatenate([fold(q), jnp.zeros((LANES - rows, LANES), jnp.float32)], axis=0)
        r_all[l, z] = jnp.sum(jnp.transpose(p), axis=0, keepdims=True)

        @pl.when(l < last)
        def _():
            pair_columns(l).start()

        @pl.when(l == last)
        def _():
            spread(c_last.at[d], cl_send.at[0], cl_recv.at[0], d_peers)

        spread(r_all.at[l, z], ring(r_send, l), ring(r_recv, l), z_peers)

    def pair_columns(l):
        return remote(c_mine.at[l, 1 - core], c_pair.at[l], ring(cp_send, l), ring(cp_recv, l), {'dp': dc})

    def full_columns(l):
        return remote(c_full.at[l, core], c_full.at[l, core], ring(cf_send, l), ring(cf_recv, l), {'dp': dc})

    def drain_rows(l):
        if zs > 1:
            drain(r_all.at[l, 0:zs - 1], ring(r_recv, l))
            drain(r_all.at[l, 0:zs - 1], ring(r_send, l))

    def stage_columns(l):
        pair_columns(l).wait()
        drain_rows(l)
        c_all[l, chip] = c_mine[l, core] + c_pair[l]
        spread(c_all.at[l, chip], ring(c_send, l), ring(c_recv, l), plane_peers)

    def stage_share(l):
        drain(c_all.at[l, 0:chips - 1], ring(c_recv, l))
        drain(c_all.at[l, 0:chips - 1], ring(c_send, l))
        c_full[l, core] = total(c_all.at[l])
        full_columns(l).start()

    def stage_moments(l):
        @pl.when(l < last)
        def _():
            full_columns(l).wait()

        @pl.when(l == last)
        def _():
            drain(c_last.at[0:ds - 1], cl_recv.at[0])
            drain(c_last.at[0:ds - 1], cl_send.at[0])
            drain_rows(l)
            col = total(c_last)
            c_full[l, 0] = col[:, 0:cols // 2]
            c_full[l, 1] = col[:, cols // 2:cols]

        col = jnp.concatenate([c_full[l, 0], c_full[l, 1]], axis=1)
        r_new = DECAY * r_pad[pl.ds(l, 1)] + (1.0 - DECAY) * (total(r_all.at[l]) / cols_total)
        c_new = DECAY * c_buf[pl.ds(l, 1)] + (1.0 - DECAY) * (col / rows_total)
        r_pad[pl.ds(l, 1)] = r_new
        r_buf[pl.ds(l, 1)] = r_new[:, 0:rows]
        c_buf[pl.ds(l, 1)] = c_new
        a = column(lax.rsqrt(r_new), rows)
        b = lax.rsqrt(c_new)
        acc = jnp.zeros((1, LANES), jnp.float32)
        for t in range(cols // LANES):
            sl = slice(t * LANES, (t + 1) * LANES)
            u = d_buf[l, :, sl] * a * b[:, sl]
            acc = acc + jnp.sum(u * u, axis=0, keepdims=True)
        lane = lax.broadcasted_iota(jnp.int32, (1, LANES), 1)
        lane = lane - jnp.where(l == late, 3, 0)
        row = jnp.where(lane == 0, jnp.sum(acc, axis=1, keepdims=True), 0.0)
        row = jnp.where(lane == 1, jnp.sum(w_sq[pl.ds(l, 1)], axis=1, keepdims=True), row)
        row = jnp.where(lane == 2, jnp.sum(r_new, axis=1, keepdims=True), row)

        @pl.when(l < late)
        def _():
            s_all[l, 2 * z + core] = row
            spread(s_all.at[l, 2 * z + core], ring(s_send, l), ring(s_recv, l), column_peers)

        @pl.when(l == late)
        def _():
            held[...] = row

        @pl.when(l == last)
        def _():
            me = ds * z + d
            t_last[me] = row + held[...]
            spread(t_last.at[me], tl_send.at[0], tl_recv.at[0], others)

    def stage_gather(l):
        drain(s_all.at[l, 0:2 * zs - 1], ring(s_recv, l))
        drain(s_all.at[l, 0:2 * zs - 1], ring(s_send, l))
        t_all[l, chip] = total(s_all.at[l])
        spread(t_all.at[l, chip], ring(t_send, l), ring(t_recv, l), plane_peers)

    def stage_update(l):
        drain(t_all.at[l, 0:chips - 1], ring(t_recv, l))
        drain(t_all.at[l, 0:chips - 1], ring(t_send, l))
        scale, clip, a = factors(total(t_all.at[l]), r_pad[pl.ds(l, 1)], rate_ref[...], rows, zs, rows_total, cols_total)
        b = lax.rsqrt(c_buf[pl.ds(l, 1)]) / clip
        for t in range(cols // LANES):
            sl = slice(t * LANES, (t + 1) * LANES)
            w_buf[l, :, sl] = w_buf[l, :, sl] - scale * (d_buf[l, :, sl] * a * b[:, sl])

    def stage_final():
        drain(t_last.at[0:ds * zs - 1], tl_recv.at[0])
        sums_out[...] = total(t_last)
        drain(t_last.at[0:ds * zs - 1], tl_send.at[0])

    def drain_one(l):
        drain(in1x.at[0:2], ring(one_send, l))

    def drain_two(l):
        drain(in2.at[l], ring(two_send, l))

    def at(i, lag, stage, begin=0, end=layers):
        @pl.when((i >= begin + lag) & (i < end + lag))
        def _():
            stage(i - lag)

    def once(i, when, stage):
        @pl.when(i == when)
        def _():
            stage()

    def prefetch(l):
        load_own(l)
        send_pair(l)

    def body(i, carry):
        at(i, -AHEAD, prefetch)
        at(i, 0, stage_combine, 1)
        once(i, 0, stage_first)
        at(i, 1, stage_forward, 1)
        once(i, 1, forward_first)
        once(i, 1, norm_split)
        once(i, 2, norm_send)
        at(i, 3, stage_columns, 0, last)
        at(i, 4, stage_share, 0, last)
        at(i, 5, stage_moments)
        at(i, 7, stage_gather, 0, late)
        at(i, 8, stage_update, 0, late)
        at(i, 2, drain_one, 1)
        once(i, 2, lambda: drain(first_part, one_send.at[0]))
        at(i, 3, drain_two)
        once(i, 4, norm_stats)
        once(i, 6, norm_update)
        at(i, 2, stage_stats)
        return carry

    lax.fori_loop(0, late + 8, body, 0)
    stage_final()


def write_kernel(ds, zs, rate_ref, w, d, r, c, n, v, r_pad, sums, wo, ro, co, no, vo, w_new, sem):
    layers, rows, cols = w.shape
    late = layers - DIRECT
    pairs = ((w.at[0:late], wo.at[0:late]), (r, ro), (c, co), (v, vo), (n, no))
    for i, pair in enumerate(pairs):
        pltpu.make_async_copy(*pair, sem.at[i]).start()
    for e in range(DIRECT):
        l = late + e
        lane = 3 * (DIRECT - 1 - e)
        scale, clip, a = factors(sums[:, lane:lane + 3], r_pad[l:l + 1], rate_ref[...], rows, zs, rows * ds, cols * zs)
        b = lax.rsqrt(c[l:l + 1]) / clip
        for t in range(cols // LANES):
            sl = slice(t * LANES, (t + 1) * LANES)
            w_new[e, :, sl] = w[l, :, sl] - scale * (d[l, :, sl] * a * b[:, sl])
    for e in range(DIRECT):
        pltpu.make_async_copy(w_new.at[e], wo.at[late + e], sem.at[5]).start()
    for i, pair in enumerate(pairs):
        pltpu.make_async_copy(*pair, sem.at[i]).wait()
    pltpu.make_async_copy(w_new, wo.at[late:layers], sem.at[5]).wait()


def write_out(ds, zs, rate, w, d, r, c, n, v, r_pad, sums):
    return pl.pallas_call(
        functools.partial(write_kernel, ds, zs),
        out_shape=[jax.ShapeDtypeStruct(a.shape, a.dtype) for a in (w, r, c, n, v)],
        in_specs=[pl.BlockSpec(memory_space=pltpu.MemorySpace.SMEM)] + [pl.BlockSpec(memory_space=pltpu.MemorySpace.VMEM)] * 8,
        out_specs=[pl.BlockSpec(memory_space=pltpu.MemorySpace.HBM)] * 5,
        scratch_shapes=[pltpu.VMEM((DIRECT,) + w.shape[1:], w.dtype), pltpu.SemaphoreType.DMA((6,))],
        compiler_params=pltpu.CompilerParams(vmem_limit_bytes=4 << 20),
        name='write_out',
    )(rate, w, d, r, c, n, v, r_pad, sums)


def solution(mesh):
    ds = mesh.shape['dp']
    zs = mesh.shape['model']

    def local_step(weight, grad_parts, row_stat, col_stat, norm_scale, norm_grads, norm_stat, learn_rate):
        layers, rows, cols = weight.shape
        half = rows // 2
        f32 = jnp.float32
        grads = grad_parts.reshape(layers, ds, rows, cols)
        any_spec = pl.BlockSpec(memory_space=pltpu.MemorySpace.HBM)
        dma = pltpu.SemaphoreType.DMA
        outs = pl.pallas_call(
            step_kernel,
            out_shape=[pltpu.VMEM(a.shape, f32) for a in (weight, weight, row_stat, col_stat, norm_scale, norm_stat)]
            + [pltpu.VMEM((layers, LANES), f32), pltpu.VMEM((1, LANES), f32)],
            in_specs=[any_spec] * 7 + [pl.BlockSpec(memory_space=pltpu.MemorySpace.SMEM)],
            out_specs=[pl.BlockSpec(memory_space=pltpu.MemorySpace.VMEM)] * 8,
            scratch_shapes=[
                pltpu.VMEM((layers, 3, rows, cols), f32),
                pltpu.VMEM((layers, 4, rows, cols), f32),
                pltpu.VMEM((layers, 2, half, cols), f32),
                pltpu.VMEM((layers, 2, half, cols), f32),
                pltpu.VMEM((layers, 2, half, cols), f32),
                pltpu.VMEM((2, 2, EARLY, cols), f32),
                pltpu.VMEM(norm_grads.shape, f32),
                pltpu.VMEM((layers, LANES), f32),
                pltpu.VMEM((layers, zs, 1, LANES), f32),
                pltpu.VMEM((layers, 2, 1, cols // 2), f32),
                pltpu.VMEM((layers, 1, cols // 2), f32),
                pltpu.VMEM((layers, ds // 2, 1, cols // 2), f32),
                pltpu.VMEM((layers, 2, 1, cols // 2), f32),
                pltpu.VMEM((ds, 1, cols), f32),
                pltpu.VMEM((layers, 2 * zs, 1, LANES), f32),
                pltpu.VMEM((layers, ds // 2, 1, LANES), f32),
                pltpu.VMEM((ds * zs, 1, LANES), f32),
                pltpu.VMEM((1, LANES), f32),
                pltpu.VMEM((ds // 2, 2, layers, LANES), f32),
                pltpu.VMEM((ds // 2, layers, LANES), f32),
                pltpu.VMEM((ds // 2, layers, LANES), f32),
                pltpu.VMEM((ds, 1, 2 * LANES), f32),
                *[dma((n,)) for n in (3, 3, 5, 3, 3, 3, 4, 4, 4, 2, 2, 2, 4, 2, 4, 3, 6, 2, 4, 2)],
                *[dma((DIRECT,))] * 4,
            ],
            compiler_params=pltpu.CompilerParams(collective_id=0, has_side_effects=True, vmem_limit_bytes=50 * 1000 * 1000),
            name='adafactor_step',
        )(weight, grads, row_stat, col_stat, norm_scale, norm_grads, norm_stat, learn_rate)
        return write_out(ds, zs, learn_rate, *outs)

    mat_spec = P(None, 'dp', 'model')
    row_spec = P(None, 'dp')
    col_spec = P(None, 'model')
    return jax.shard_map(local_step, mesh=mesh, in_specs=(mat_spec, mat_spec, row_spec, col_spec, row_spec, row_spec, row_spec, P()), out_specs=(mat_spec, row_spec, col_spec, row_spec, row_spec), check_vma=False)
```

```python
import functools

import jax
import jax.numpy as jnp
from jax import lax
from jax.experimental import pallas as pl
from jax.experimental.pallas import tpu as pltpu
from jax.sharding import PartitionSpec as P

STEP_COUNT = 4
DECAY_POWER = 0.8
EPS_FLOOR = 1e-30
SCALE_FLOOR = 1e-3
CLIP_LIMIT = 1.0
DECAY = 1.0 - STEP_COUNT ** -DECAY_POWER
MESH = pl.DeviceIdType.MESH
LANES = 128
AHEAD = 2
DIRECT = 2
EARLY = 8


def column(row, rows):
    return jnp.transpose(jnp.broadcast_to(row, (LANES, LANES)))[0:rows]


def factors(sums, r_row, rate, rows, zs, rows_total, cols_total):
    count = rows_total * cols_total
    r_mean = sums[:, 2:3] / (rows_total * zs)
    u_rms = jnp.sqrt(sums[:, 0:1] / count * r_mean)
    clip = jnp.maximum(1.0, u_rms / CLIP_LIMIT)
    scale = rate * jnp.maximum(SCALE_FLOOR, jnp.sqrt(sums[:, 1:2] / count))
    return scale, clip, column(lax.rsqrt(r_row / r_mean), rows)


def step_kernel(w_hbm, g_hbm, r_hbm, c_hbm, n_hbm, ng_hbm, v_hbm, rate_ref,
                w_buf, d_buf, r_buf, c_buf, n_buf, v_buf, r_pad, sums_out,
                own, peer, in1x, in1y, in2, early, ng_buf, w_sq,
                r_all, c_mine, c_pair, c_all, c_full, c_last, s_all, t_all, t_last, held, h_out, h_all, k_all,
                load_sem, pair_send, pair_recv, one_send, one_recv, two_send, two_recv,
                r_send, r_recv, cp_send, cp_recv, c_send, c_recv, cf_send, cf_recv,
                s_send, s_recv, t_send, t_recv, w_sem,
                cl_send, cl_recv, tl_send, tl_recv):
    layers, _, rows, cols = own.shape
    half = rows // 2
    last, ds = layers - 1, c_last.shape[0]
    late = layers - DIRECT
    zs = r_all.shape[1]
    chips = ds // 2
    rows_total, cols_total = rows * ds, cols * zs
    z = lax.axis_index('model')
    d = lax.axis_index('dp')
    chip, core = lax.div(d, 2), lax.rem(d, 2)
    dx = d + 2 - 4 * lax.rem(chip, 2)
    dy = d + 4 - 8 * lax.div(d, 4)
    dxy = dx + dy - d
    dc = d + 1 - 2 * core
    blocks = (dx, dxy, dy, d)
    z_peers = [{'model': lax.rem(z + j, zs)} for j in range(1, zs)]
    d_peers = [{'dp': e} for e in (dc, dx, dx + dc - d, dy, dy + dc - d, dxy, dxy + dc - d)]
    column_peers = [{'dp': dc}] + [{'model': p['model'], 'dp': e} for p in z_peers for e in (d, dc)]
    plane_peers = [{'dp': e} for e in (dx, dy, dxy)]
    others = [{'model': p['model'], **q} for q in d_peers[::-1] for p in z_peers] + d_peers[::-1] + z_peers

    def ring(sem, l):
        return sem.at[lax.rem(l, sem.shape[0])]

    def remote(src, dst, send, recv, where):
        return pltpu.make_async_remote_copy(src_ref=src, dst_ref=dst, send_sem=send, recv_sem=recv,
                                            device_id=where, device_id_type=MESH)

    def spread(ref, send, recv, peers):
        for where in peers:
            remote(ref, ref, send, recv, where).start()

    def drain(ref, sem):
        pltpu.make_async_copy(ref, ref, sem).wait()

    def load_own(l):
        for k in range(3):
            pltpu.make_async_copy(g_hbm.at[l, blocks[k]], own.at[l, k], ring(load_sem, l)).start()
        pltpu.make_async_copy(g_hbm.at[l, d], d_buf.at[l], ring(load_sem, l)).start()

    def pair_copy(l, k, row, source, recv):
        part = pl.ds(row, half)
        return remote(source.at[part], peer.at[l, k, part], ring(pair_send, l), recv, {'dp': dc})

    def from_hbm(l, k):
        return g_hbm.at[l, blocks[k] + dc - d]

    def send_pair(l):
        for k in range(4):
            remote(from_hbm(l, k), peer.at[l, k], ring(pair_send, l), ring(pair_recv, l), {'dp': dc}).start()

    def x1(l):
        return remote(own.at[l, 0:2, 0:half], in1x.at[l], ring(one_send, l), ring(one_recv, l), {'dp': dx})

    def y1(l):
        return remote(own.at[l, 1:3, half:rows], in1y.at[l], ring(one_send, l), ring(one_recv, l), {'dp': dy})

    def y2(l):
        return remote(own.at[l, 2, 0:half], in2.at[l, 0], ring(two_send, l), ring(two_recv, l), {'dp': dy})

    def x2(l):
        return remote(own.at[l, 0, half:rows], in2.at[l, 1], ring(two_send, l), ring(two_recv, l), {'dp': dx})

    def total(buf):
        parts = [buf[j] for j in range(buf.shape[0])]
        while len(parts) > 1:
            parts = [a + b for a, b in zip(parts[::2], parts[1::2])]
        return parts[0]

    def fold(values):
        acc = values[:, 0:LANES]
        for t in range(1, cols // LANES):
            acc = acc + values[:, t * LANES:(t + 1) * LANES]
        return acc

    small = ((r_hbm, r_buf), (c_hbm, c_buf), (n_hbm, n_buf), (ng_hbm, ng_buf), (v_hbm, v_buf))
    groups = (((0, 0), (1, 0)), ((1, half), (2, half)))
    for i, group in enumerate(groups):
        for k, row in group:
            part = pl.ds(row, half)
            pltpu.make_async_copy(from_hbm(0, k).at[part], own.at[layers - 1, i, pl.ds((k - i) * half, half)], w_sem.at[i]).start()
    load_own(0)
    small_sems = (r_send.at[0], r_send.at[1], r_send.at[2], r_send.at[3], cl_send.at[0])
    for (src, dst), sem in zip(small, small_sems):
        pltpu.make_async_copy(src, dst, sem).start()

    barrier = pltpu.get_barrier_semaphore()
    known = d_peers + column_peers[1:]
    for where in known:
        pl.semaphore_signal(barrier, inc=1, device_id=where, device_id_type=MESH)
    pl.semaphore_wait(barrier, len(known))
    for i, (near, row) in enumerate(((dx, 0), (dy, half))):
        for e in (near, near + dc - d):
            remote(g_hbm.at[0, e, pl.ds(row, EARLY)], early.at[i, core], tl_send.at[1], tl_recv.at[1], {'dp': e}).start()
    for i, group in enumerate(groups):
        drain(own.at[layers - 1, i], w_sem.at[i])
        for k, row in group:
            part = pl.ds(row, half)
            remote(own.at[layers - 1, i, pl.ds((k - i) * half, half)], peer.at[0, k, part],
                   pair_send.at[0], two_recv.at[i + 1], {'dp': dc}).start()
    for k, row in ((0, half), (2, 0), (3, 0), (3, half)):
        pair_copy(0, k, row, from_hbm(0, k), two_recv.at[3]).start()
    for l in range(1, AHEAD):
        send_pair(l)
        load_own(l)

    def norm_split():
        for i in (0, 1, 2, 4):
            pltpu.make_async_copy(*small[i], small_sems[i]).wait()
        r_pad[...] = jnp.zeros_like(r_pad)
        r_pad[:, 0:rows] = r_buf[...]
        k_all[...] = jnp.zeros_like(k_all)

    h_out[...] = jnp.zeros_like(h_out)
    pltpu.make_async_copy(*small[3], small_sems[3]).wait()
    for k in range(ds):
        h_out[k, :, 0:rows] = ng_buf[:, k * rows:(k + 1) * rows]
    h_all[d] = h_out[d]
    for where in d_peers:
        remote(h_out.at[where['dp']], h_all.at[d], cl_send.at[1], cl_recv.at[1], where).start()

    def layer_sums(values):
        padded = jnp.concatenate([values, jnp.zeros((layers, LANES - rows), jnp.float32)], axis=1)
        return jnp.sum(jnp.transpose(padded), axis=0, keepdims=True)

    def norm_stats():
        drain(h_all.at[0:ds - 1], cl_recv.at[1])
        drain(h_all.at[0:ds - 1], cl_send.at[1])
        h = total(h_all)[:, 0:rows]
        v_new = DECAY * v_buf[...] + (1.0 - DECAY) * (h * h + EPS_FLOOR)
        v_buf[...] = v_new
        zv = h * lax.rsqrt(v_new)
        nv = n_buf[...]
        k_all[d, :, 0:layers] = layer_sums(zv * zv)
        k_all[d, :, LANES:LANES + layers] = layer_sums(nv * nv)
        spread(k_all.at[d], tl_send.at[0], tl_recv.at[0], d_peers)

    def norm_update():
        drain(k_all.at[0:ds - 1], tl_recv.at[0])
        drain(k_all.at[0:ds - 1], tl_send.at[0])
        acc = total(k_all)
        z_sq, n_sq = acc[:, 0:layers], acc[:, LANES:LANES + layers]
        clip = jnp.maximum(1.0, jnp.sqrt(z_sq / rows_total) / CLIP_LIMIT)
        scale = rate_ref[...] * jnp.maximum(SCALE_FLOOR, jnp.sqrt(n_sq / rows_total))
        clip = jnp.transpose(jnp.broadcast_to(clip, (LANES, layers)))[:, 0:rows]
        scale = jnp.transpose(jnp.broadcast_to(scale, (LANES, layers)))[:, 0:rows]
        zv = total(h_all)[:, 0:rows] * lax.rsqrt(v_buf[...])
        n_buf[...] = n_buf[...] - scale * (zv / clip)

    def combine(l, k, part):
        own[l, k, part] = own[l, k, part] + peer[l, k, part]

    first, second = slice(0, half), slice(half, rows)

    def stage_first():
        drain(peer.at[0], load_sem.at[0])
        drain(in1x.at[0], two_recv.at[1])
        combine(0, slice(0, 2), first)
        for k, row in ((0, EARLY), (1, 0)):
            part = pl.ds(row, half - row)
            remote(own.at[0, k, part], in1x.at[0, k, part], one_send.at[0], one_recv.at[0], {'dp': dx}).start()
        drain(in1y.at[0], two_recv.at[2])
        combine(0, slice(1, 3), second)
        for k, row in ((0, 0), (1, EARLY)):
            remote(own.at[0, k + 1, pl.ds(half + row, half - row)], in1y.at[0, k, pl.ds(row, half - row)],
                   one_send.at[0], one_recv.at[0], {'dp': dy}).start()
        drain(peer.at[0, 0:2], two_recv.at[3])
        combine(0, 0, second)
        combine(0, 2, first)
        d_buf[0] = d_buf[0] + peer[0, 3]
        drain(peer.at[0], pair_send.at[0])

    def stage_combine(l):
        drain(peer.at[l], ring(load_sem, l))
        drain(peer.at[l], ring(pair_recv, l))
        combine(l, slice(0, 2), first)
        x1(l).start()
        combine(l, slice(1, 3), second)
        y1(l).start()
        combine(l, 0, second)
        combine(l, 2, first)
        d_buf[l] = d_buf[l] + peer[l, 3]
        drain(peer.at[l], ring(pair_send, l))

    def stage_forward(l):
        pltpu.make_async_copy(w_hbm.at[l], w_buf.at[l], ring(w_sem, l)).start()
        drain(in1x.at[0:2], ring(one_recv, l))
        own[l, 2, 0:half] = own[l, 2, 0:half] + in1x[l, 1]
        own[l, 0, half:rows] = own[l, 0, half:rows] + in1y[l, 0]
        y2(l).start()
        d_buf[l, 0:half] = d_buf[l, 0:half] + in1x[l, 0]
        x2(l).start()
        d_buf[l, half:rows] = d_buf[l, half:rows] + in1y[l, 1]

    first_part = w_buf.at[0:half // 4 - EARLY // 8, 0:16]

    def forward_first():
        drain(first_part, one_recv.at[0])
        own[0, 2, first] = own[0, 2, first] + in1x[0, 1]
        own[0, 0, second] = own[0, 0, second] + in1y[0, 0]
        y2(0).start()
        x2(0).start()
        pltpu.make_async_copy(w_hbm.at[0], w_buf.at[0], w_sem.at[0]).start()
        drain(early, tl_recv.at[1])
        drain(early, tl_send.at[1])
        rest = slice(EARLY, half)
        d_buf[0, 0:EARLY] = d_buf[0, 0:EARLY] + (early[0, 0] + early[0, 1])
        d_buf[0, rest] = d_buf[0, rest] + in1x[0, 0, rest]
        d_buf[0, half:half + EARLY] = d_buf[0, half:half + EARLY] + (early[1, 0] + early[1, 1])
        d_buf[0, half + EARLY:rows] = d_buf[0, half + EARLY:rows] + in1y[0, 1, rest]

    def stage_stats(l):
        drain(w_buf.at[l], ring(w_sem, l))
        w = w_buf[l]
        w_sq[pl.ds(l, 1)] = fold(jnp.sum(w * w, axis=0, keepdims=True))
        drain(in2.at[l], ring(two_recv, l))
        g = d_buf[l] + in2[l].reshape(rows, cols)
        d_buf[l] = g
        q = g * g + EPS_FLOOR
        col = jnp.sum(q, axis=0, keepdims=True)

        @pl.when(l < last)
        def _():
            c_mine[l, 0] = col[:, 0:cols // 2]
            c_mine[l, 1] = col[:, cols // 2:cols]

        @pl.when(l == last)
        def _():
            c_last[d] = col

        p = jnp.concatenate([fold(q), jnp.zeros((LANES - rows, LANES), jnp.float32)], axis=0)
        r_all[l, z] = jnp.sum(jnp.transpose(p), axis=0, keepdims=True)

        @pl.when(l < last)
        def _():
            pair_columns(l).start()

        @pl.when(l == last)
        def _():
            spread(c_last.at[d], cl_send.at[0], cl_recv.at[0], d_peers)

        spread(r_all.at[l, z], ring(r_send, l), ring(r_recv, l), z_peers)

    def pair_columns(l):
        return remote(c_mine.at[l, 1 - core], c_pair.at[l], ring(cp_send, l), ring(cp_recv, l), {'dp': dc})

    def full_columns(l):
        return remote(c_full.at[l, core], c_full.at[l, core], ring(cf_send, l), ring(cf_recv, l), {'dp': dc})

    def drain_rows(l):
        if zs > 1:
            drain(r_all.at[l, 0:zs - 1], ring(r_recv, l))
            drain(r_all.at[l, 0:zs - 1], ring(r_send, l))

    def stage_columns(l):
        pair_columns(l).wait()
        c_all[l, chip] = c_mine[l, core] + c_pair[l]
        spread(c_all.at[l, chip], ring(c_send, l), ring(c_recv, l), plane_peers)

    def stage_share(l):
        drain(c_all.at[l, 0:chips - 1], ring(c_recv, l))
        drain(c_all.at[l, 0:chips - 1], ring(c_send, l))
        c_full[l, core] = total(c_all.at[l])
        full_columns(l).start()
        drain_rows(l)

    def stage_moments(l):
        @pl.when(l < last)
        def _():
            full_columns(l).wait()

        @pl.when(l == last)
        def _():
            drain(c_last.at[0:ds - 1], cl_recv.at[0])
            drain(c_last.at[0:ds - 1], cl_send.at[0])
            drain_rows(l)
            col = total(c_last)
            c_full[l, 0] = col[:, 0:cols // 2]
            c_full[l, 1] = col[:, cols // 2:cols]

        col = jnp.concatenate([c_full[l, 0], c_full[l, 1]], axis=1)
        r_new = DECAY * r_pad[pl.ds(l, 1)] + (1.0 - DECAY) * (total(r_all.at[l]) / cols_total)
        c_new = DECAY * c_buf[pl.ds(l, 1)] + (1.0 - DECAY) * (col / rows_total)
        r_pad[pl.ds(l, 1)] = r_new
        r_buf[pl.ds(l, 1)] = r_new[:, 0:rows]
        c_buf[pl.ds(l, 1)] = c_new
        a = column(lax.rsqrt(r_new), rows)
        b = lax.rsqrt(c_new)
        acc = jnp.zeros((1, LANES), jnp.float32)
        for t in range(cols // LANES):
            sl = slice(t * LANES, (t + 1) * LANES)
            u = d_buf[l, :, sl] * a * b[:, sl]
            acc = acc + jnp.sum(u * u, axis=0, keepdims=True)
        lane = lax.broadcasted_iota(jnp.int32, (1, LANES), 1)
        lane = lane - jnp.where(l == late, 3, 0)
        row = jnp.where(lane == 0, jnp.sum(acc, axis=1, keepdims=True), 0.0)
        row = jnp.where(lane == 1, jnp.sum(w_sq[pl.ds(l, 1)], axis=1, keepdims=True), row)
        row = jnp.where(lane == 2, jnp.sum(r_new, axis=1, keepdims=True), row)

        @pl.when(l < late)
        def _():
            s_all[l, 2 * z + core] = row
            spread(s_all.at[l, 2 * z + core], ring(s_send, l), ring(s_recv, l), column_peers)

        @pl.when(l == late)
        def _():
            held[...] = row

        @pl.when(l == last)
        def _():
            me = ds * z + d
            t_last[me] = row + held[...]
            spread(t_last.at[me], tl_send.at[0], tl_recv.at[0], others)

    def stage_gather(l):
        drain(s_all.at[l, 0:2 * zs - 1], ring(s_recv, l))
        drain(s_all.at[l, 0:2 * zs - 1], ring(s_send, l))
        t_all[l, chip] = total(s_all.at[l])
        spread(t_all.at[l, chip], ring(t_send, l), ring(t_recv, l), plane_peers)

    def stage_update(l):
        drain(t_all.at[l, 0:chips - 1], ring(t_recv, l))
        drain(t_all.at[l, 0:chips - 1], ring(t_send, l))
        scale, clip, a = factors(total(t_all.at[l]), r_pad[pl.ds(l, 1)], rate_ref[...], rows, zs, rows_total, cols_total)
        b = lax.rsqrt(c_buf[pl.ds(l, 1)]) / clip
        for t in range(cols // LANES):
            sl = slice(t * LANES, (t + 1) * LANES)
            w_buf[l, :, sl] = w_buf[l, :, sl] - scale * (d_buf[l, :, sl] * a * b[:, sl])

    def stage_final():
        drain(t_last.at[0:ds * zs - 1], tl_recv.at[0])
        sums_out[...] = total(t_last)
        drain(t_last.at[0:ds * zs - 1], tl_send.at[0])

    def drain_one(l):
        drain(in1x.at[0:2], ring(one_send, l))

    def drain_two(l):
        drain(in2.at[l], ring(two_send, l))

    def at(i, lag, stage, begin=0, end=layers):
        @pl.when((i >= begin + lag) & (i < end + lag))
        def _():
            stage(i - lag)

    def once(i, when, stage):
        @pl.when(i == when)
        def _():
            stage()

    def prefetch(l):
        load_own(l)
        send_pair(l)

    def body(i, carry):
        at(i, -AHEAD, prefetch)
        at(i, 0, stage_combine, 1)
        once(i, 0, stage_first)
        at(i, 1, stage_forward, 1)
        once(i, 1, forward_first)
        once(i, 1, norm_split)
        at(i, 3, stage_columns, 0, last)
        at(i, 4, stage_share, 0, last)
        at(i, 5, stage_moments)
        at(i, 7, stage_gather, 0, late)
        at(i, 8, stage_update, 0, late)
        at(i, 2, drain_one, 1)
        once(i, 2, lambda: drain(first_part, one_send.at[0]))
        at(i, 3, drain_two)
        once(i, 4, norm_stats)
        once(i, 6, norm_update)
        at(i, 2, stage_stats)
        return carry

    lax.fori_loop(0, late + 8, body, 0)
    stage_final()


def write_kernel(ds, zs, rate_ref, w, d, r, c, n, v, r_pad, sums, wo, ro, co, no, vo, w_new, sem):
    layers, rows, cols = w.shape
    late = layers - DIRECT
    pairs = ((w.at[0:late], wo.at[0:late]), (r, ro), (c, co), (v, vo), (n, no))
    for i, pair in enumerate(pairs):
        pltpu.make_async_copy(*pair, sem.at[i]).start()
    for e in range(DIRECT):
        l = late + e
        lane = 3 * (DIRECT - 1 - e)
        scale, clip, a = factors(sums[:, lane:lane + 3], r_pad[l:l + 1], rate_ref[...], rows, zs, rows * ds, cols * zs)
        b = lax.rsqrt(c[l:l + 1]) / clip
        for t in range(cols // LANES):
            sl = slice(t * LANES, (t + 1) * LANES)
            w_new[e, :, sl] = w[l, :, sl] - scale * (d[l, :, sl] * a * b[:, sl])
    for e in range(DIRECT):
        pltpu.make_async_copy(w_new.at[e], wo.at[late + e], sem.at[5]).start()
    for i, pair in enumerate(pairs):
        pltpu.make_async_copy(*pair, sem.at[i]).wait()
    pltpu.make_async_copy(w_new, wo.at[late:layers], sem.at[5]).wait()


def write_out(ds, zs, rate, w, d, r, c, n, v, r_pad, sums):
    return pl.pallas_call(
        functools.partial(write_kernel, ds, zs),
        out_shape=[jax.ShapeDtypeStruct(a.shape, a.dtype) for a in (w, r, c, n, v)],
        in_specs=[pl.BlockSpec(memory_space=pltpu.MemorySpace.SMEM)] + [pl.BlockSpec(memory_space=pltpu.MemorySpace.VMEM)] * 8,
        out_specs=[pl.BlockSpec(memory_space=pltpu.MemorySpace.HBM)] * 5,
        scratch_shapes=[pltpu.VMEM((DIRECT,) + w.shape[1:], w.dtype), pltpu.SemaphoreType.DMA((6,))],
        compiler_params=pltpu.CompilerParams(vmem_limit_bytes=4 << 20),
        name='write_out',
    )(rate, w, d, r, c, n, v, r_pad, sums)


def solution(mesh):
    ds = mesh.shape['dp']
    zs = mesh.shape['model']

    def local_step(weight, grad_parts, row_stat, col_stat, norm_scale, norm_grads, norm_stat, learn_rate):
        layers, rows, cols = weight.shape
        half = rows // 2
        f32 = jnp.float32
        grads = grad_parts.reshape(layers, ds, rows, cols)
        any_spec = pl.BlockSpec(memory_space=pltpu.MemorySpace.HBM)
        dma = pltpu.SemaphoreType.DMA
        outs = pl.pallas_call(
            step_kernel,
            out_shape=[pltpu.VMEM(a.shape, f32) for a in (weight, weight, row_stat, col_stat, norm_scale, norm_stat)]
            + [pltpu.VMEM((layers, LANES), f32), pltpu.VMEM((1, LANES), f32)],
            in_specs=[any_spec] * 7 + [pl.BlockSpec(memory_space=pltpu.MemorySpace.SMEM)],
            out_specs=[pl.BlockSpec(memory_space=pltpu.MemorySpace.VMEM)] * 8,
            scratch_shapes=[
                pltpu.VMEM((layers, 3, rows, cols), f32),
                pltpu.VMEM((layers, 4, rows, cols), f32),
                pltpu.VMEM((layers, 2, half, cols), f32),
                pltpu.VMEM((layers, 2, half, cols), f32),
                pltpu.VMEM((layers, 2, half, cols), f32),
                pltpu.VMEM((2, 2, EARLY, cols), f32),
                pltpu.VMEM(norm_grads.shape, f32),
                pltpu.VMEM((layers, LANES), f32),
                pltpu.VMEM((layers, zs, 1, LANES), f32),
                pltpu.VMEM((layers, 2, 1, cols // 2), f32),
                pltpu.VMEM((layers, 1, cols // 2), f32),
                pltpu.VMEM((layers, ds // 2, 1, cols // 2), f32),
                pltpu.VMEM((layers, 2, 1, cols // 2), f32),
                pltpu.VMEM((ds, 1, cols), f32),
                pltpu.VMEM((layers, 2 * zs, 1, LANES), f32),
                pltpu.VMEM((layers, ds // 2, 1, LANES), f32),
                pltpu.VMEM((ds * zs, 1, LANES), f32),
                pltpu.VMEM((1, LANES), f32),
                pltpu.VMEM((ds, layers, LANES), f32),
                pltpu.VMEM((ds, layers, LANES), f32),
                pltpu.VMEM((ds, 1, 2 * LANES), f32),
                *[dma((n,)) for n in (3, 3, 5, 3, 3, 3, 4, 4, 5, 2, 2, 2, 4, 2, 4, 3, 6, 2, 4, 2)],
                *[dma((DIRECT,))] * 4,
            ],
            compiler_params=pltpu.CompilerParams(collective_id=0, has_side_effects=True, vmem_limit_bytes=50 * 1000 * 1000),
            name='adafactor_step',
        )(weight, grads, row_stat, col_stat, norm_scale, norm_grads, norm_stat, learn_rate)
        return write_out(ds, zs, learn_rate, *outs)

    mat_spec = P(None, 'dp', 'model')
    row_spec = P(None, 'dp')
    col_spec = P(None, 'model')
    return jax.shard_map(local_step, mesh=mesh, in_specs=(mat_spec, mat_spec, row_spec, col_spec, row_spec, row_spec, row_spec, P()), out_specs=(mat_spec, row_spec, col_spec, row_spec, row_spec), check_vma=False)
```

```python
import functools

import jax
import jax.numpy as jnp
from jax import lax
from jax.experimental import pallas as pl
from jax.experimental.pallas import tpu as pltpu
from jax.sharding import PartitionSpec as P

STEP_COUNT = 4
DECAY_POWER = 0.8
EPS_FLOOR = 1e-30
SCALE_FLOOR = 1e-3
CLIP_LIMIT = 1.0
DECAY = 1.0 - STEP_COUNT ** -DECAY_POWER
MESH = pl.DeviceIdType.MESH
LANES = 128
AHEAD = 2
DIRECT = 3
EARLY = 8


def column(row, rows):
    return jnp.transpose(jnp.broadcast_to(row, (LANES, LANES)))[0:rows]


def factors(sums, r_row, rate, rows, zs, rows_total, cols_total):
    count = rows_total * cols_total
    r_mean = sums[:, 2:3] / (rows_total * zs)
    u_rms = jnp.sqrt(sums[:, 0:1] / count * r_mean)
    clip = jnp.maximum(1.0, u_rms / CLIP_LIMIT)
    scale = rate * jnp.maximum(SCALE_FLOOR, jnp.sqrt(sums[:, 1:2] / count))
    return scale, clip, column(lax.rsqrt(r_row / r_mean), rows)


def step_kernel(w_hbm, g_hbm, r_hbm, c_hbm, n_hbm, ng_hbm, v_hbm, rate_ref,
                w_buf, d_buf, r_buf, c_buf, n_buf, v_buf, r_pad, sums_out,
                own, peer, in1x, in1y, in2, early, ng_buf, w_sq,
                r_all, c_mine, c_pair, c_all, c_full, c_last, s_all, t_all, t_last, held, h_out, h_all, k_all,
                load_sem, pair_send, pair_recv, one_send, one_recv, two_send, two_recv,
                r_send, r_recv, cp_send, cp_recv, c_send, c_recv, cf_send, cf_recv,
                s_send, s_recv, t_send, t_recv, w_sem,
                cl_send, cl_recv, tl_send, tl_recv):
    layers, _, rows, cols = own.shape
    half = rows // 2
    last, ds = layers - 1, c_last.shape[0]
    late = layers - DIRECT
    zs = r_all.shape[1]
    chips = ds // 2
    rows_total, cols_total = rows * ds, cols * zs
    z = lax.axis_index('model')
    d = lax.axis_index('dp')
    chip, core = lax.div(d, 2), lax.rem(d, 2)
    dx = d + 2 - 4 * lax.rem(chip, 2)
    dy = d + 4 - 8 * lax.div(d, 4)
    dxy = dx + dy - d
    dc = d + 1 - 2 * core
    blocks = (dx, dxy, dy, d)
    z_peers = [{'model': lax.rem(z + j, zs)} for j in range(1, zs)]
    d_peers = [{'dp': e} for e in (dc, dx, dx + dc - d, dy, dy + dc - d, dxy, dxy + dc - d)]
    column_peers = [{'dp': dc}] + [{'model': p['model'], 'dp': e} for p in z_peers for e in (d, dc)]
    plane_peers = [{'dp': e} for e in (dx, dy, dxy)]
    others = [{'model': p['model'], **q} for q in d_peers[::-1] for p in z_peers] + d_peers[::-1] + z_peers

    def ring(sem, l):
        return sem.at[lax.rem(l, sem.shape[0])]

    def remote(src, dst, send, recv, where):
        return pltpu.make_async_remote_copy(src_ref=src, dst_ref=dst, send_sem=send, recv_sem=recv,
                                            device_id=where, device_id_type=MESH)

    def spread(ref, send, recv, peers):
        for where in peers:
            remote(ref, ref, send, recv, where).start()

    def drain(ref, sem):
        pltpu.make_async_copy(ref, ref, sem).wait()

    def load_own(l):
        for k in range(3):
            pltpu.make_async_copy(g_hbm.at[l, blocks[k]], own.at[l, k], ring(load_sem, l)).start()
        pltpu.make_async_copy(g_hbm.at[l, d], d_buf.at[l], ring(load_sem, l)).start()

    def pair_copy(l, k, row, source, recv):
        part = pl.ds(row, half)
        return remote(source.at[part], peer.at[l, k, part], ring(pair_send, l), recv, {'dp': dc})

    def from_hbm(l, k):
        return g_hbm.at[l, blocks[k] + dc - d]

    def send_pair(l):
        for k in range(4):
            remote(from_hbm(l, k), peer.at[l, k], ring(pair_send, l), ring(pair_recv, l), {'dp': dc}).start()

    def x1(l):
        return remote(own.at[l, 0:2, 0:half], in1x.at[l], ring(one_send, l), ring(one_recv, l), {'dp': dx})

    def y1(l):
        return remote(own.at[l, 1:3, half:rows], in1y.at[l], ring(one_send, l), ring(one_recv, l), {'dp': dy})

    def y2(l):
        return remote(own.at[l, 2, 0:half], in2.at[l, 0], ring(two_send, l), ring(two_recv, l), {'dp': dy})

    def x2(l):
        return remote(own.at[l, 0, half:rows], in2.at[l, 1], ring(two_send, l), ring(two_recv, l), {'dp': dx})

    def total(buf):
        parts = [buf[j] for j in range(buf.shape[0])]
        while len(parts) > 1:
            parts = [a + b for a, b in zip(parts[::2], parts[1::2])]
        return parts[0]

    def fold(values):
        acc = values[:, 0:LANES]
        for t in range(1, cols // LANES):
            acc = acc + values[:, t * LANES:(t + 1) * LANES]
        return acc

    small = ((r_hbm, r_buf), (c_hbm, c_buf), (n_hbm, n_buf), (ng_hbm, ng_buf), (v_hbm, v_buf))
    groups = (((0, 0), (1, 0)), ((1, half), (2, half)))
    for i, group in enumerate(groups):
        for k, row in group:
            part = pl.ds(row, half)
            pltpu.make_async_copy(from_hbm(0, k).at[part], own.at[layers - 1, i, pl.ds((k - i) * half, half)], w_sem.at[i]).start()
    load_own(0)
    small_sems = (r_send.at[0], r_send.at[1], r_send.at[2], r_send.at[3], cl_send.at[0])
    for (src, dst), sem in zip(small, small_sems):
        pltpu.make_async_copy(src, dst, sem).start()

    barrier = pltpu.get_barrier_semaphore()
    known = d_peers + column_peers[1:]
    for where in known:
        pl.semaphore_signal(barrier, inc=1, device_id=where, device_id_type=MESH)
    pl.semaphore_wait(barrier, len(known))
    for i, (near, row) in enumerate(((dx, 0), (dy, half))):
        for e in (near, near + dc - d):
            remote(g_hbm.at[0, e, pl.ds(row, EARLY)], early.at[i, core], tl_send.at[1], tl_recv.at[1], {'dp': e}).start()
    for i, group in enumerate(groups):
        drain(own.at[layers - 1, i], w_sem.at[i])
        for k, row in group:
            part = pl.ds(row, half)
            remote(own.at[layers - 1, i, pl.ds((k - i) * half, half)], peer.at[0, k, part],
                   pair_send.at[0], two_recv.at[i + 1], {'dp': dc}).start()
    for k, row in ((0, half), (2, 0), (3, 0), (3, half)):
        pair_copy(0, k, row, from_hbm(0, k), two_recv.at[3]).start()
    for l in range(1, AHEAD):
        send_pair(l)
        load_own(l)

    def norm_split():
        for i in (0, 1, 2, 4):
            pltpu.make_async_copy(*small[i], small_sems[i]).wait()
        r_pad[...] = jnp.zeros_like(r_pad)
        r_pad[:, 0:rows] = r_buf[...]
        k_all[...] = jnp.zeros_like(k_all)

    h_out[...] = jnp.zeros_like(h_out)
    pltpu.make_async_copy(*small[3], small_sems[3]).wait()
    for k in range(ds):
        h_out[k, :, 0:rows] = ng_buf[:, k * rows:(k + 1) * rows]
    h_all[d] = h_out[d]
    for where in d_peers:
        remote(h_out.at[where['dp']], h_all.at[d], cl_send.at[1], cl_recv.at[1], where).start()

    def layer_sums(values):
        padded = jnp.concatenate([values, jnp.zeros((layers, LANES - rows), jnp.float32)], axis=1)
        return jnp.sum(jnp.transpose(padded), axis=0, keepdims=True)

    def norm_stats():
        drain(h_all.at[0:ds - 1], cl_recv.at[1])
        drain(h_all.at[0:ds - 1], cl_send.at[1])
        h = total(h_all)[:, 0:rows]
        v_new = DECAY * v_buf[...] + (1.0 - DECAY) * (h * h + EPS_FLOOR)
        v_buf[...] = v_new
        zv = h * lax.rsqrt(v_new)
        nv = n_buf[...]
        k_all[d, :, 0:layers] = layer_sums(zv * zv)
        k_all[d, :, LANES:LANES + layers] = layer_sums(nv * nv)
        spread(k_all.at[d], tl_send.at[0], tl_recv.at[0], d_peers)

    def norm_update():
        drain(k_all.at[0:ds - 1], tl_recv.at[0])
        drain(k_all.at[0:ds - 1], tl_send.at[0])
        acc = total(k_all)
        z_sq, n_sq = acc[:, 0:layers], acc[:, LANES:LANES + layers]
        clip = jnp.maximum(1.0, jnp.sqrt(z_sq / rows_total) / CLIP_LIMIT)
        scale = rate_ref[...] * jnp.maximum(SCALE_FLOOR, jnp.sqrt(n_sq / rows_total))
        clip = jnp.transpose(jnp.broadcast_to(clip, (LANES, layers)))[:, 0:rows]
        scale = jnp.transpose(jnp.broadcast_to(scale, (LANES, layers)))[:, 0:rows]
        zv = total(h_all)[:, 0:rows] * lax.rsqrt(v_buf[...])
        n_buf[...] = n_buf[...] - scale * (zv / clip)

    def combine(l, k, part):
        own[l, k, part] = own[l, k, part] + peer[l, k, part]

    first, second = slice(0, half), slice(half, rows)

    def stage_first():
        drain(peer.at[0], load_sem.at[0])
        drain(in1x.at[0], two_recv.at[1])
        combine(0, slice(0, 2), first)
        for k, row in ((0, EARLY), (1, 0)):
            part = pl.ds(row, half - row)
            remote(own.at[0, k, part], in1x.at[0, k, part], one_send.at[0], one_recv.at[0], {'dp': dx}).start()
        drain(in1y.at[0], two_recv.at[2])
        combine(0, slice(1, 3), second)
        for k, row in ((0, 0), (1, EARLY)):
            remote(own.at[0, k + 1, pl.ds(half + row, half - row)], in1y.at[0, k, pl.ds(row, half - row)],
                   one_send.at[0], one_recv.at[0], {'dp': dy}).start()
        drain(peer.at[0, 0:2], two_recv.at[3])
        combine(0, 0, second)
        combine(0, 2, first)
        d_buf[0] = d_buf[0] + peer[0, 3]
        drain(peer.at[0], pair_send.at[0])

    def stage_combine(l):
        drain(peer.at[l], ring(load_sem, l))
        drain(peer.at[l], ring(pair_recv, l))
        combine(l, slice(0, 2), first)
        x1(l).start()
        combine(l, slice(1, 3), second)
        y1(l).start()
        combine(l, 0, second)
        combine(l, 2, first)
        d_buf[l] = d_buf[l] + peer[l, 3]
        drain(peer.at[l], ring(pair_send, l))

    def stage_forward(l):
        pltpu.make_async_copy(w_hbm.at[l], w_buf.at[l], ring(w_sem, l)).start()
        drain(in1x.at[0:2], ring(one_recv, l))
        own[l, 2, 0:half] = own[l, 2, 0:half] + in1x[l, 1]
        own[l, 0, half:rows] = own[l, 0, half:rows] + in1y[l, 0]
        y2(l).start()
        d_buf[l, 0:half] = d_buf[l, 0:half] + in1x[l, 0]
        x2(l).start()
        d_buf[l, half:rows] = d_buf[l, half:rows] + in1y[l, 1]

    first_part = w_buf.at[0:half // 4 - EARLY // 8, 0:16]

    def forward_first():
        drain(first_part, one_recv.at[0])
        own[0, 2, first] = own[0, 2, first] + in1x[0, 1]
        own[0, 0, second] = own[0, 0, second] + in1y[0, 0]
        y2(0).start()
        x2(0).start()
        pltpu.make_async_copy(w_hbm.at[0], w_buf.at[0], w_sem.at[0]).start()
        drain(early, tl_recv.at[1])
        drain(early, tl_send.at[1])
        rest = slice(EARLY, half)
        d_buf[0, 0:EARLY] = d_buf[0, 0:EARLY] + (early[0, 0] + early[0, 1])
        d_buf[0, rest] = d_buf[0, rest] + in1x[0, 0, rest]
        d_buf[0, half:half + EARLY] = d_buf[0, half:half + EARLY] + (early[1, 0] + early[1, 1])
        d_buf[0, half + EARLY:rows] = d_buf[0, half + EARLY:rows] + in1y[0, 1, rest]

    def stage_stats(l):
        drain(w_buf.at[l], ring(w_sem, l))
        w = w_buf[l]
        w_sq[pl.ds(l, 1)] = fold(jnp.sum(w * w, axis=0, keepdims=True))
        drain(in2.at[l], ring(two_recv, l))
        g = d_buf[l] + in2[l].reshape(rows, cols)
        d_buf[l] = g
        q = g * g + EPS_FLOOR
        col = jnp.sum(q, axis=0, keepdims=True)

        @pl.when(l < last)
        def _():
            c_mine[l, 0] = col[:, 0:cols // 2]
            c_mine[l, 1] = col[:, cols // 2:cols]

        @pl.when(l == last)
        def _():
            c_last[d] = col

        p = jnp.concatenate([fold(q), jnp.zeros((LANES - rows, LANES), jnp.float32)], axis=0)
        r_all[l, z] = jnp.sum(jnp.transpose(p), axis=0, keepdims=True)

        @pl.when(l < last)
        def _():
            pair_columns(l).start()

        @pl.when(l == last)
        def _():
            spread(c_last.at[d], cl_send.at[0], cl_recv.at[0], d_peers)

        spread(r_all.at[l, z], ring(r_send, l), ring(r_recv, l), z_peers)

    def pair_columns(l):
        return remote(c_mine.at[l, 1 - core], c_pair.at[l], ring(cp_send, l), ring(cp_recv, l), {'dp': dc})

    def full_columns(l):
        return remote(c_full.at[l, core], c_full.at[l, core], ring(cf_send, l), ring(cf_recv, l), {'dp': dc})

    def drain_rows(l):
        if zs > 1:
            drain(r_all.at[l, 0:zs - 1], ring(r_recv, l))
            drain(r_all.at[l, 0:zs - 1], ring(r_send, l))

    def stage_columns(l):
        pair_columns(l).wait()
        c_all[l, chip] = c_mine[l, core] + c_pair[l]
        spread(c_all.at[l, chip], ring(c_send, l), ring(c_recv, l), plane_peers)

    def stage_share(l):
        drain(c_all.at[l, 0:chips - 1], ring(c_recv, l))
        drain(c_all.at[l, 0:chips - 1], ring(c_send, l))
        c_full[l, core] = total(c_all.at[l])
        full_columns(l).start()
        drain_rows(l)

    def stage_moments(l):
        @pl.when(l < last)
        def _():
            full_columns(l).wait()

        @pl.when(l == last)
        def _():
            drain(c_last.at[0:ds - 1], cl_recv.at[0])
            drain(c_last.at[0:ds - 1], cl_send.at[0])
            drain_rows(l)
            col = total(c_last)
            c_full[l, 0] = col[:, 0:cols // 2]
            c_full[l, 1] = col[:, cols // 2:cols]

        col = jnp.concatenate([c_full[l, 0], c_full[l, 1]], axis=1)
        r_new = DECAY * r_pad[pl.ds(l, 1)] + (1.0 - DECAY) * (total(r_all.at[l]) / cols_total)
        c_new = DECAY * c_buf[pl.ds(l, 1)] + (1.0 - DECAY) * (col / rows_total)
        r_pad[pl.ds(l, 1)] = r_new
        r_buf[pl.ds(l, 1)] = r_new[:, 0:rows]
        c_buf[pl.ds(l, 1)] = c_new
        a = column(lax.rsqrt(r_new), rows)
        b = lax.rsqrt(c_new)
        acc = jnp.zeros((1, LANES), jnp.float32)
        for t in range(cols // LANES):
            sl = slice(t * LANES, (t + 1) * LANES)
            u = d_buf[l, :, sl] * a * b[:, sl]
            acc = acc + jnp.sum(u * u, axis=0, keepdims=True)
        lane = lax.broadcasted_iota(jnp.int32, (1, LANES), 1)
        lane = lane - jnp.where(l >= late, 3 * (last - l), 0)
        row = jnp.where(lane == 0, jnp.sum(acc, axis=1, keepdims=True), 0.0)
        row = jnp.where(lane == 1, jnp.sum(w_sq[pl.ds(l, 1)], axis=1, keepdims=True), row)
        row = jnp.where(lane == 2, jnp.sum(r_new, axis=1, keepdims=True), row)

        @pl.when(l < late)
        def _():
            s_all[l, 2 * z + core] = row
            spread(s_all.at[l, 2 * z + core], ring(s_send, l), ring(s_recv, l), column_peers)

        @pl.when(l == late)
        def _():
            held[...] = row

        @pl.when((l > late) & (l < last))
        def _():
            held[...] = held[...] + row

        @pl.when(l == last)
        def _():
            me = ds * z + d
            t_last[me] = row + held[...]
            spread(t_last.at[me], tl_send.at[0], tl_recv.at[0], others)

    def stage_gather(l):
        drain(s_all.at[l, 0:2 * zs - 1], ring(s_recv, l))
        drain(s_all.at[l, 0:2 * zs - 1], ring(s_send, l))
        t_all[l, chip] = total(s_all.at[l])
        spread(t_all.at[l, chip], ring(t_send, l), ring(t_recv, l), plane_peers)

    def stage_update(l):
        drain(t_all.at[l, 0:chips - 1], ring(t_recv, l))
        drain(t_all.at[l, 0:chips - 1], ring(t_send, l))
        scale, clip, a = factors(total(t_all.at[l]), r_pad[pl.ds(l, 1)], rate_ref[...], rows, zs, rows_total, cols_total)
        b = lax.rsqrt(c_buf[pl.ds(l, 1)]) / clip
        for t in range(cols // LANES):
            sl = slice(t * LANES, (t + 1) * LANES)
            w_buf[l, :, sl] = w_buf[l, :, sl] - scale * (d_buf[l, :, sl] * a * b[:, sl])

    def stage_final():
        drain(t_last.at[0:ds * zs - 1], tl_recv.at[0])
        sums_out[...] = total(t_last)
        drain(t_last.at[0:ds * zs - 1], tl_send.at[0])

    def drain_one(l):
        drain(in1x.at[0:2], ring(one_send, l))

    def drain_two(l):
        drain(in2.at[l], ring(two_send, l))

    def at(i, lag, stage, begin=0, end=layers):
        @pl.when((i >= begin + lag) & (i < end + lag))
        def _():
            stage(i - lag)

    def once(i, when, stage):
        @pl.when(i == when)
        def _():
            stage()

    def prefetch(l):
        load_own(l)
        send_pair(l)

    def body(i, carry):
        at(i, -AHEAD, prefetch)
        at(i, 0, stage_combine, 1)
        once(i, 0, stage_first)
        at(i, 1, stage_forward, 1)
        once(i, 1, forward_first)
        once(i, 1, norm_split)
        at(i, 3, stage_columns, 0, last)
        at(i, 4, stage_share, 0, last)
        at(i, 5, stage_moments)
        at(i, 7, stage_gather, 0, late)
        at(i, 8, stage_update, 0, late)
        at(i, 2, drain_one, 1)
        once(i, 2, lambda: drain(first_part, one_send.at[0]))
        at(i, 3, drain_two)
        once(i, 4, norm_stats)
        once(i, 6, norm_update)
        at(i, 2, stage_stats)
        return carry

    lax.fori_loop(0, late + 8, body, 0)
    stage_final()


def write_kernel(ds, zs, rate_ref, w, d, r, c, n, v, r_pad, sums, wo, ro, co, no, vo, w_new, sem):
    layers, rows, cols = w.shape
    late = layers - DIRECT
    pairs = ((w.at[0:late], wo.at[0:late]), (r, ro), (c, co), (v, vo), (n, no))
    for i, pair in enumerate(pairs):
        pltpu.make_async_copy(*pair, sem.at[i]).start()
    for e in range(DIRECT):
        l = late + e
        lane = 3 * (DIRECT - 1 - e)
        scale, clip, a = factors(sums[:, lane:lane + 3], r_pad[l:l + 1], rate_ref[...], rows, zs, rows * ds, cols * zs)
        b = lax.rsqrt(c[l:l + 1]) / clip
        for t in range(cols // LANES):
            sl = slice(t * LANES, (t + 1) * LANES)
            w_new[e, :, sl] = w[l, :, sl] - scale * (d[l, :, sl] * a * b[:, sl])
    for e in range(DIRECT):
        pltpu.make_async_copy(w_new.at[e], wo.at[late + e], sem.at[5]).start()
    for i, pair in enumerate(pairs):
        pltpu.make_async_copy(*pair, sem.at[i]).wait()
    pltpu.make_async_copy(w_new, wo.at[late:layers], sem.at[5]).wait()


def write_out(ds, zs, rate, w, d, r, c, n, v, r_pad, sums):
    return pl.pallas_call(
        functools.partial(write_kernel, ds, zs),
        out_shape=[jax.ShapeDtypeStruct(a.shape, a.dtype) for a in (w, r, c, n, v)],
        in_specs=[pl.BlockSpec(memory_space=pltpu.MemorySpace.SMEM)] + [pl.BlockSpec(memory_space=pltpu.MemorySpace.VMEM)] * 8,
        out_specs=[pl.BlockSpec(memory_space=pltpu.MemorySpace.HBM)] * 5,
        scratch_shapes=[pltpu.VMEM((DIRECT,) + w.shape[1:], w.dtype), pltpu.SemaphoreType.DMA((6,))],
        compiler_params=pltpu.CompilerParams(vmem_limit_bytes=4 << 20),
        name='write_out',
    )(rate, w, d, r, c, n, v, r_pad, sums)


def solution(mesh):
    ds = mesh.shape['dp']
    zs = mesh.shape['model']

    def local_step(weight, grad_parts, row_stat, col_stat, norm_scale, norm_grads, norm_stat, learn_rate):
        layers, rows, cols = weight.shape
        half = rows // 2
        f32 = jnp.float32
        grads = grad_parts.reshape(layers, ds, rows, cols)
        any_spec = pl.BlockSpec(memory_space=pltpu.MemorySpace.HBM)
        dma = pltpu.SemaphoreType.DMA
        outs = pl.pallas_call(
            step_kernel,
            out_shape=[pltpu.VMEM(a.shape, f32) for a in (weight, weight, row_stat, col_stat, norm_scale, norm_stat)]
            + [pltpu.VMEM((layers, LANES), f32), pltpu.VMEM((1, LANES), f32)],
            in_specs=[any_spec] * 7 + [pl.BlockSpec(memory_space=pltpu.MemorySpace.SMEM)],
            out_specs=[pl.BlockSpec(memory_space=pltpu.MemorySpace.VMEM)] * 8,
            scratch_shapes=[
                pltpu.VMEM((layers, 3, rows, cols), f32),
                pltpu.VMEM((layers, 4, rows, cols), f32),
                pltpu.VMEM((layers, 2, half, cols), f32),
                pltpu.VMEM((layers, 2, half, cols), f32),
                pltpu.VMEM((layers, 2, half, cols), f32),
                pltpu.VMEM((2, 2, EARLY, cols), f32),
                pltpu.VMEM(norm_grads.shape, f32),
                pltpu.VMEM((layers, LANES), f32),
                pltpu.VMEM((layers, zs, 1, LANES), f32),
                pltpu.VMEM((layers, 2, 1, cols // 2), f32),
                pltpu.VMEM((layers, 1, cols // 2), f32),
                pltpu.VMEM((layers, ds // 2, 1, cols // 2), f32),
                pltpu.VMEM((layers, 2, 1, cols // 2), f32),
                pltpu.VMEM((ds, 1, cols), f32),
                pltpu.VMEM((layers, 2 * zs, 1, LANES), f32),
                pltpu.VMEM((layers, ds // 2, 1, LANES), f32),
                pltpu.VMEM((ds * zs, 1, LANES), f32),
                pltpu.VMEM((1, LANES), f32),
                pltpu.VMEM((ds, layers, LANES), f32),
                pltpu.VMEM((ds, layers, LANES), f32),
                pltpu.VMEM((ds, 1, 2 * LANES), f32),
                *[dma((n,)) for n in (3, 3, 5, 3, 3, 3, 4, 4, 5, 2, 2, 2, 4, 2, 4, 3, 6, 2, 4, 2)],
                *[dma((2,))] * 4,
            ],
            compiler_params=pltpu.CompilerParams(collective_id=0, has_side_effects=True, vmem_limit_bytes=50 * 1000 * 1000),
            name='adafactor_step',
        )(weight, grads, row_stat, col_stat, norm_scale, norm_grads, norm_stat, learn_rate)
        return write_out(ds, zs, learn_rate, *outs)

    mat_spec = P(None, 'dp', 'model')
    row_spec = P(None, 'dp')
    col_spec = P(None, 'model')
    return jax.shard_map(local_step, mesh=mesh, in_specs=(mat_spec, mat_spec, row_spec, col_spec, row_spec, row_spec, row_spec, P()), out_specs=(mat_spec, row_spec, col_spec, row_spec, row_spec), check_vma=False)
```

```python
import functools

import jax
import jax.numpy as jnp
from jax import lax
from jax.experimental import pallas as pl
from jax.experimental.pallas import tpu as pltpu
from jax.sharding import PartitionSpec as P

STEP_COUNT = 4
DECAY_POWER = 0.8
EPS_FLOOR = 1e-30
SCALE_FLOOR = 1e-3
CLIP_LIMIT = 1.0
DECAY = 1.0 - STEP_COUNT ** -DECAY_POWER
MESH = pl.DeviceIdType.MESH
LANES = 128
AHEAD = 2
DIRECT = 3
EARLY = 8


def column(row, rows):
    return jnp.transpose(jnp.broadcast_to(row, (LANES, LANES)))[0:rows]


def factors(sums, r_row, rate, rows, zs, rows_total, cols_total):
    count = rows_total * cols_total
    r_mean = sums[:, 2:3] / (rows_total * zs)
    u_rms = jnp.sqrt(sums[:, 0:1] / count * r_mean)
    clip = jnp.maximum(1.0, u_rms / CLIP_LIMIT)
    scale = rate * jnp.maximum(SCALE_FLOOR, jnp.sqrt(sums[:, 1:2] / count))
    return scale, clip, column(lax.rsqrt(r_row / r_mean), rows)


def step_kernel(w_hbm, g_hbm, r_hbm, c_hbm, n_hbm, ng_hbm, v_hbm, rate_ref,
                w_buf, d_buf, r_buf, c_buf, n_buf, v_buf, r_pad, sums_out,
                own, peer, in1x, in1y, in2, early, ng_buf, w_sq,
                r_all, c_mine, c_pair, c_all, c_full, c_last, s_all, t_all, t_last, held, h_out, h_all, k_all,
                load_sem, pair_send, pair_recv, one_send, one_recv, two_send, two_recv,
                r_send, r_recv, cp_send, cp_recv, c_send, c_recv, cf_send, cf_recv,
                s_send, s_recv, t_send, t_recv, w_sem,
                cl_send, cl_recv, tl_send, tl_recv):
    layers, _, rows, cols = own.shape
    half = rows // 2
    last, ds = layers - 1, c_last.shape[1]
    near_end = layers - c_last.shape[0]
    late = layers - DIRECT
    zs = r_all.shape[1]
    chips = ds // 2
    rows_total, cols_total = rows * ds, cols * zs
    z = lax.axis_index('model')
    d = lax.axis_index('dp')
    chip, core = lax.div(d, 2), lax.rem(d, 2)
    dx = d + 2 - 4 * lax.rem(chip, 2)
    dy = d + 4 - 8 * lax.div(d, 4)
    dxy = dx + dy - d
    dc = d + 1 - 2 * core
    blocks = (dx, dxy, dy, d)
    z_peers = [{'model': lax.rem(z + j, zs)} for j in range(1, zs)]
    d_peers = [{'dp': e} for e in (dc, dx, dx + dc - d, dy, dy + dc - d, dxy, dxy + dc - d)]
    column_peers = [{'dp': dc}] + [{'model': p['model'], 'dp': e} for p in z_peers for e in (d, dc)]
    plane_peers = [{'dp': e} for e in (dx, dy, dxy)]
    others = [{'model': p['model'], **q} for q in d_peers[::-1] for p in z_peers] + d_peers[::-1] + z_peers

    def ring(sem, l):
        return sem.at[lax.rem(l, sem.shape[0])]

    def remote(src, dst, send, recv, where):
        return pltpu.make_async_remote_copy(src_ref=src, dst_ref=dst, send_sem=send, recv_sem=recv,
                                            device_id=where, device_id_type=MESH)

    def spread(ref, send, recv, peers):
        for where in peers:
            remote(ref, ref, send, recv, where).start()

    def drain(ref, sem):
        pltpu.make_async_copy(ref, ref, sem).wait()

    def load_own(l):
        for k in range(3):
            pltpu.make_async_copy(g_hbm.at[l, blocks[k]], own.at[l, k], ring(load_sem, l)).start()
        pltpu.make_async_copy(g_hbm.at[l, d], d_buf.at[l], ring(load_sem, l)).start()

    def pair_copy(l, k, row, source, recv):
        part = pl.ds(row, half)
        return remote(source.at[part], peer.at[l, k, part], ring(pair_send, l), recv, {'dp': dc})

    def from_hbm(l, k):
        return g_hbm.at[l, blocks[k] + dc - d]

    def send_pair(l):
        for k in range(4):
            remote(from_hbm(l, k), peer.at[l, k], ring(pair_send, l), ring(pair_recv, l), {'dp': dc}).start()

    def x1(l):
        return remote(own.at[l, 0:2, 0:half], in1x.at[l], ring(one_send, l), ring(one_recv, l), {'dp': dx})

    def y1(l):
        return remote(own.at[l, 1:3, half:rows], in1y.at[l], ring(one_send, l), ring(one_recv, l), {'dp': dy})

    def y2(l):
        return remote(own.at[l, 2, 0:half], in2.at[l, 0], ring(two_send, l), ring(two_recv, l), {'dp': dy})

    def x2(l):
        return remote(own.at[l, 0, half:rows], in2.at[l, 1], ring(two_send, l), ring(two_recv, l), {'dp': dx})

    def total(buf):
        parts = [buf[j] for j in range(buf.shape[0])]
        while len(parts) > 1:
            parts = [a + b for a, b in zip(parts[::2], parts[1::2])]
        return parts[0]

    def fold(values):
        acc = values[:, 0:LANES]
        for t in range(1, cols // LANES):
            acc = acc + values[:, t * LANES:(t + 1) * LANES]
        return acc

    small = ((r_hbm, r_buf), (c_hbm, c_buf), (n_hbm, n_buf), (ng_hbm, ng_buf), (v_hbm, v_buf))
    groups = (((0, 0), (1, 0)), ((1, half), (2, half)))
    for i, group in enumerate(groups):
        for k, row in group:
            part = pl.ds(row, half)
            pltpu.make_async_copy(from_hbm(0, k).at[part], own.at[layers - 1, i, pl.ds((k - i) * half, half)], w_sem.at[i]).start()
    load_own(0)
    small_sems = (r_send.at[0], r_send.at[1], r_send.at[2], r_send.at[3], cl_send.at[0])
    for (src, dst), sem in zip(small, small_sems):
        pltpu.make_async_copy(src, dst, sem).start()

    barrier = pltpu.get_barrier_semaphore()
    known = d_peers + column_peers[1:]
    for where in known:
        pl.semaphore_signal(barrier, inc=1, device_id=where, device_id_type=MESH)
    pl.semaphore_wait(barrier, len(known))
    for i, (near, row) in enumerate(((dx, 0), (dy, half))):
        for e in (near, near + dc - d):
            remote(g_hbm.at[0, e, pl.ds(row, EARLY)], early.at[i, core], tl_send.at[1], tl_recv.at[1], {'dp': e}).start()
    for i, group in enumerate(groups):
        drain(own.at[layers - 1, i], w_sem.at[i])
        for k, row in group:
            part = pl.ds(row, half)
            remote(own.at[layers - 1, i, pl.ds((k - i) * half, half)], peer.at[0, k, part],
                   pair_send.at[0], two_recv.at[i + 1], {'dp': dc}).start()
    for k, row in ((0, half), (2, 0), (3, 0), (3, half)):
        pair_copy(0, k, row, from_hbm(0, k), two_recv.at[3]).start()
    for l in range(1, AHEAD):
        send_pair(l)
        load_own(l)

    def norm_split():
        for i in (0, 1, 2, 4):
            pltpu.make_async_copy(*small[i], small_sems[i]).wait()
        r_pad[...] = jnp.zeros_like(r_pad)
        r_pad[:, 0:rows] = r_buf[...]
        k_all[...] = jnp.zeros_like(k_all)

    h_out[...] = jnp.zeros_like(h_out)
    pltpu.make_async_copy(*small[3], small_sems[3]).wait()
    for k in range(ds):
        h_out[k, :, 0:rows] = ng_buf[:, k * rows:(k + 1) * rows]
    h_all[d] = h_out[d]
    for where in d_peers:
        remote(h_out.at[where['dp']], h_all.at[d], cl_send.at[1], cl_recv.at[1], where).start()

    def layer_sums(values):
        padded = jnp.concatenate([values, jnp.zeros((layers, LANES - rows), jnp.float32)], axis=1)
        return jnp.sum(jnp.transpose(padded), axis=0, keepdims=True)

    def norm_stats():
        drain(h_all.at[0:ds - 1], cl_recv.at[1])
        drain(h_all.at[0:ds - 1], cl_send.at[1])
        h = total(h_all)[:, 0:rows]
        v_new = DECAY * v_buf[...] + (1.0 - DECAY) * (h * h + EPS_FLOOR)
        v_buf[...] = v_new
        zv = h * lax.rsqrt(v_new)
        nv = n_buf[...]
        k_all[d, :, 0:layers] = layer_sums(zv * zv)
        k_all[d, :, LANES:LANES + layers] = layer_sums(nv * nv)
        spread(k_all.at[d], tl_send.at[0], tl_recv.at[0], d_peers)

    def norm_update():
        drain(k_all.at[0:ds - 1], tl_recv.at[0])
        drain(k_all.at[0:ds - 1], tl_send.at[0])
        acc = total(k_all)
        z_sq, n_sq = acc[:, 0:layers], acc[:, LANES:LANES + layers]
        clip = jnp.maximum(1.0, jnp.sqrt(z_sq / rows_total) / CLIP_LIMIT)
        scale = rate_ref[...] * jnp.maximum(SCALE_FLOOR, jnp.sqrt(n_sq / rows_total))
        clip = jnp.transpose(jnp.broadcast_to(clip, (LANES, layers)))[:, 0:rows]
        scale = jnp.transpose(jnp.broadcast_to(scale, (LANES, layers)))[:, 0:rows]
        zv = total(h_all)[:, 0:rows] * lax.rsqrt(v_buf[...])
        n_buf[...] = n_buf[...] - scale * (zv / clip)

    def combine(l, k, part):
        own[l, k, part] = own[l, k, part] + peer[l, k, part]

    first, second = slice(0, half), slice(half, rows)

    def stage_first():
        drain(peer.at[0], load_sem.at[0])
        drain(in1x.at[0], two_recv.at[1])
        combine(0, slice(0, 2), first)
        for k, row in ((0, EARLY), (1, 0)):
            part = pl.ds(row, half - row)
            remote(own.at[0, k, part], in1x.at[0, k, part], one_send.at[0], one_recv.at[0], {'dp': dx}).start()
        drain(in1y.at[0], two_recv.at[2])
        combine(0, slice(1, 3), second)
        for k, row in ((0, 0), (1, EARLY)):
            remote(own.at[0, k + 1, pl.ds(half + row, half - row)], in1y.at[0, k, pl.ds(row, half - row)],
                   one_send.at[0], one_recv.at[0], {'dp': dy}).start()
        drain(peer.at[0, 0:2], two_recv.at[3])
        combine(0, 0, second)
        combine(0, 2, first)
        d_buf[0] = d_buf[0] + peer[0, 3]
        drain(peer.at[0], pair_send.at[0])

    def stage_combine(l):
        drain(peer.at[l], ring(load_sem, l))
        drain(peer.at[l], ring(pair_recv, l))
        combine(l, slice(0, 2), first)
        x1(l).start()
        combine(l, slice(1, 3), second)
        y1(l).start()
        combine(l, 0, second)
        combine(l, 2, first)
        d_buf[l] = d_buf[l] + peer[l, 3]
        drain(peer.at[l], ring(pair_send, l))

    def stage_forward(l):
        pltpu.make_async_copy(w_hbm.at[l], w_buf.at[l], ring(w_sem, l)).start()
        drain(in1x.at[0:2], ring(one_recv, l))
        own[l, 2, 0:half] = own[l, 2, 0:half] + in1x[l, 1]
        own[l, 0, half:rows] = own[l, 0, half:rows] + in1y[l, 0]
        y2(l).start()
        d_buf[l, 0:half] = d_buf[l, 0:half] + in1x[l, 0]
        x2(l).start()
        d_buf[l, half:rows] = d_buf[l, half:rows] + in1y[l, 1]

    first_part = w_buf.at[0:half // 4 - EARLY // 8, 0:16]

    def forward_first():
        drain(first_part, one_recv.at[0])
        own[0, 2, first] = own[0, 2, first] + in1x[0, 1]
        own[0, 0, second] = own[0, 0, second] + in1y[0, 0]
        y2(0).start()
        x2(0).start()
        pltpu.make_async_copy(w_hbm.at[0], w_buf.at[0], w_sem.at[0]).start()
        drain(early, tl_recv.at[1])
        drain(early, tl_send.at[1])
        rest = slice(EARLY, half)
        d_buf[0, 0:EARLY] = d_buf[0, 0:EARLY] + (early[0, 0] + early[0, 1])
        d_buf[0, rest] = d_buf[0, rest] + in1x[0, 0, rest]
        d_buf[0, half:half + EARLY] = d_buf[0, half:half + EARLY] + (early[1, 0] + early[1, 1])
        d_buf[0, half + EARLY:rows] = d_buf[0, half + EARLY:rows] + in1y[0, 1, rest]

    def stage_stats(l):
        drain(w_buf.at[l], ring(w_sem, l))
        w = w_buf[l]
        w_sq[pl.ds(l, 1)] = fold(jnp.sum(w * w, axis=0, keepdims=True))
        drain(in2.at[l], ring(two_recv, l))
        g = d_buf[l] + in2[l].reshape(rows, cols)
        d_buf[l] = g
        q = g * g + EPS_FLOOR
        col = jnp.sum(q, axis=0, keepdims=True)

        @pl.when(l < near_end)
        def _():
            c_mine[l, 0] = col[:, 0:cols // 2]
            c_mine[l, 1] = col[:, cols // 2:cols]

        @pl.when(l >= near_end)
        def _():
            c_last[l - near_end, d] = col

        p = jnp.concatenate([fold(q), jnp.zeros((LANES - rows, LANES), jnp.float32)], axis=0)
        r_all[l, z] = jnp.sum(jnp.transpose(p), axis=0, keepdims=True)

        @pl.when(l < near_end)
        def _():
            pair_columns(l).start()

        @pl.when(l >= near_end)
        def _():
            e = l - near_end
            spread(c_last.at[e, d], cl_send.at[e], cl_recv.at[e], d_peers)

        spread(r_all.at[l, z], ring(r_send, l), ring(r_recv, l), z_peers)

    def pair_columns(l):
        return remote(c_mine.at[l, 1 - core], c_pair.at[l], ring(cp_send, l), ring(cp_recv, l), {'dp': dc})

    def full_columns(l):
        return remote(c_full.at[l, core], c_full.at[l, core], ring(cf_send, l), ring(cf_recv, l), {'dp': dc})

    def drain_rows(l):
        if zs > 1:
            drain(r_all.at[l, 0:zs - 1], ring(r_recv, l))
            drain(r_all.at[l, 0:zs - 1], ring(r_send, l))

    def stage_columns(l):
        pair_columns(l).wait()
        c_all[l, chip] = c_mine[l, core] + c_pair[l]
        spread(c_all.at[l, chip], ring(c_send, l), ring(c_recv, l), plane_peers)

    def stage_share(l):
        drain(c_all.at[l, 0:chips - 1], ring(c_recv, l))
        drain(c_all.at[l, 0:chips - 1], ring(c_send, l))
        c_full[l, core] = total(c_all.at[l])
        full_columns(l).start()
        drain_rows(l)

    def stage_moments(l):
        @pl.when(l < near_end)
        def _():
            full_columns(l).wait()

        @pl.when(l >= near_end)
        def _():
            e = l - near_end
            drain(c_last.at[e, 0:ds - 1], cl_recv.at[e])
            drain(c_last.at[e, 0:ds - 1], cl_send.at[e])
            drain_rows(l)
            col = total(c_last.at[e])
            c_full[l, 0] = col[:, 0:cols // 2]
            c_full[l, 1] = col[:, cols // 2:cols]

        col = jnp.concatenate([c_full[l, 0], c_full[l, 1]], axis=1)
        r_new = DECAY * r_pad[pl.ds(l, 1)] + (1.0 - DECAY) * (total(r_all.at[l]) / cols_total)
        c_new = DECAY * c_buf[pl.ds(l, 1)] + (1.0 - DECAY) * (col / rows_total)
        r_pad[pl.ds(l, 1)] = r_new
        r_buf[pl.ds(l, 1)] = r_new[:, 0:rows]
        c_buf[pl.ds(l, 1)] = c_new
        a = column(lax.rsqrt(r_new), rows)
        b = lax.rsqrt(c_new)
        acc = jnp.zeros((1, LANES), jnp.float32)
        for t in range(cols // LANES):
            sl = slice(t * LANES, (t + 1) * LANES)
            u = d_buf[l, :, sl] * a * b[:, sl]
            acc = acc + jnp.sum(u * u, axis=0, keepdims=True)
        lane = lax.broadcasted_iota(jnp.int32, (1, LANES), 1)
        lane = lane - jnp.where(l >= late, 3 * (last - l), 0)
        row = jnp.where(lane == 0, jnp.sum(acc, axis=1, keepdims=True), 0.0)
        row = jnp.where(lane == 1, jnp.sum(w_sq[pl.ds(l, 1)], axis=1, keepdims=True), row)
        row = jnp.where(lane == 2, jnp.sum(r_new, axis=1, keepdims=True), row)

        @pl.when(l < late)
        def _():
            s_all[l, 2 * z + core] = row
            spread(s_all.at[l, 2 * z + core], ring(s_send, l), ring(s_recv, l), column_peers)

        @pl.when(l == late)
        def _():
            held[...] = row

        @pl.when((l > late) & (l < last))
        def _():
            held[...] = held[...] + row

        @pl.when(l == last)
        def _():
            me = ds * z + d
            t_last[me] = row + held[...]
            spread(t_last.at[me], tl_send.at[0], tl_recv.at[0], others)

    def stage_gather(l):
        drain(s_all.at[l, 0:2 * zs - 1], ring(s_recv, l))
        drain(s_all.at[l, 0:2 * zs - 1], ring(s_send, l))
        t_all[l, chip] = total(s_all.at[l])
        spread(t_all.at[l, chip], ring(t_send, l), ring(t_recv, l), plane_peers)

    def stage_update(l):
        drain(t_all.at[l, 0:chips - 1], ring(t_recv, l))
        drain(t_all.at[l, 0:chips - 1], ring(t_send, l))
        scale, clip, a = factors(total(t_all.at[l]), r_pad[pl.ds(l, 1)], rate_ref[...], rows, zs, rows_total, cols_total)
        b = lax.rsqrt(c_buf[pl.ds(l, 1)]) / clip
        for t in range(cols // LANES):
            sl = slice(t * LANES, (t + 1) * LANES)
            w_buf[l, :, sl] = w_buf[l, :, sl] - scale * (d_buf[l, :, sl] * a * b[:, sl])

    def stage_final():
        drain(t_last.at[0:ds * zs - 1], tl_recv.at[0])
        sums_out[...] = total(t_last)
        drain(t_last.at[0:ds * zs - 1], tl_send.at[0])

    def drain_one(l):
        drain(in1x.at[0:2], ring(one_send, l))

    def drain_two(l):
        drain(in2.at[l], ring(two_send, l))

    def at(i, lag, stage, begin=0, end=layers):
        @pl.when((i >= begin + lag) & (i < end + lag))
        def _():
            stage(i - lag)

    def once(i, when, stage):
        @pl.when(i == when)
        def _():
            stage()

    def prefetch(l):
        load_own(l)
        send_pair(l)

    def body(i, carry):
        at(i, -AHEAD, prefetch)
        at(i, 0, stage_combine, 1)
        once(i, 0, stage_first)
        at(i, 1, stage_forward, 1)
        once(i, 1, forward_first)
        once(i, 1, norm_split)
        at(i, 3, stage_columns, 0, near_end)
        at(i, 4, stage_share, 0, near_end)
        at(i, 5, stage_moments)
        at(i, 7, stage_gather, 0, late)
        at(i, 8, stage_update, 0, late)
        at(i, 2, drain_one, 1)
        once(i, 2, lambda: drain(first_part, one_send.at[0]))
        at(i, 3, drain_two)
        once(i, 4, norm_stats)
        once(i, 6, norm_update)
        at(i, 2, stage_stats)
        return carry

    lax.fori_loop(0, late + 8, body, 0)
    stage_final()


def write_kernel(ds, zs, rate_ref, w, d, r, c, n, v, r_pad, sums, wo, ro, co, no, vo, w_new, sem):
    layers, rows, cols = w.shape
    late = layers - DIRECT
    pairs = ((w.at[0:late], wo.at[0:late]), (r, ro), (c, co), (v, vo), (n, no))
    for i, pair in enumerate(pairs):
        pltpu.make_async_copy(*pair, sem.at[i]).start()
    for e in range(DIRECT):
        l = late + e
        lane = 3 * (DIRECT - 1 - e)
        scale, clip, a = factors(sums[:, lane:lane + 3], r_pad[l:l + 1], rate_ref[...], rows, zs, rows * ds, cols * zs)
        b = lax.rsqrt(c[l:l + 1]) / clip
        for t in range(cols // LANES):
            sl = slice(t * LANES, (t + 1) * LANES)
            w_new[e, :, sl] = w[l, :, sl] - scale * (d[l, :, sl] * a * b[:, sl])
    for e in range(DIRECT):
        pltpu.make_async_copy(w_new.at[e], wo.at[late + e], sem.at[5]).start()
    for i, pair in enumerate(pairs):
        pltpu.make_async_copy(*pair, sem.at[i]).wait()
    pltpu.make_async_copy(w_new, wo.at[late:layers], sem.at[5]).wait()


def write_out(ds, zs, rate, w, d, r, c, n, v, r_pad, sums):
    return pl.pallas_call(
        functools.partial(write_kernel, ds, zs),
        out_shape=[jax.ShapeDtypeStruct(a.shape, a.dtype) for a in (w, r, c, n, v)],
        in_specs=[pl.BlockSpec(memory_space=pltpu.MemorySpace.SMEM)] + [pl.BlockSpec(memory_space=pltpu.MemorySpace.VMEM)] * 8,
        out_specs=[pl.BlockSpec(memory_space=pltpu.MemorySpace.HBM)] * 5,
        scratch_shapes=[pltpu.VMEM((DIRECT,) + w.shape[1:], w.dtype), pltpu.SemaphoreType.DMA((6,))],
        compiler_params=pltpu.CompilerParams(vmem_limit_bytes=4 << 20),
        name='write_out',
    )(rate, w, d, r, c, n, v, r_pad, sums)


def solution(mesh):
    ds = mesh.shape['dp']
    zs = mesh.shape['model']

    def local_step(weight, grad_parts, row_stat, col_stat, norm_scale, norm_grads, norm_stat, learn_rate):
        layers, rows, cols = weight.shape
        half = rows // 2
        f32 = jnp.float32
        grads = grad_parts.reshape(layers, ds, rows, cols)
        any_spec = pl.BlockSpec(memory_space=pltpu.MemorySpace.HBM)
        dma = pltpu.SemaphoreType.DMA
        outs = pl.pallas_call(
            step_kernel,
            out_shape=[pltpu.VMEM(a.shape, f32) for a in (weight, weight, row_stat, col_stat, norm_scale, norm_stat)]
            + [pltpu.VMEM((layers, LANES), f32), pltpu.VMEM((1, LANES), f32)],
            in_specs=[any_spec] * 7 + [pl.BlockSpec(memory_space=pltpu.MemorySpace.SMEM)],
            out_specs=[pl.BlockSpec(memory_space=pltpu.MemorySpace.VMEM)] * 8,
            scratch_shapes=[
                pltpu.VMEM((layers, 3, rows, cols), f32),
                pltpu.VMEM((layers, 4, rows, cols), f32),
                pltpu.VMEM((layers, 2, half, cols), f32),
                pltpu.VMEM((layers, 2, half, cols), f32),
                pltpu.VMEM((layers, 2, half, cols), f32),
                pltpu.VMEM((2, 2, EARLY, cols), f32),
                pltpu.VMEM(norm_grads.shape, f32),
                pltpu.VMEM((layers, LANES), f32),
                pltpu.VMEM((layers, zs, 1, LANES), f32),
                pltpu.VMEM((layers, 2, 1, cols // 2), f32),
                pltpu.VMEM((layers, 1, cols // 2), f32),
                pltpu.VMEM((layers, ds // 2, 1, cols // 2), f32),
                pltpu.VMEM((layers, 2, 1, cols // 2), f32),
                pltpu.VMEM((2, ds, 1, cols), f32),
                pltpu.VMEM((layers, 2 * zs, 1, LANES), f32),
                pltpu.VMEM((layers, ds // 2, 1, LANES), f32),
                pltpu.VMEM((ds * zs, 1, LANES), f32),
                pltpu.VMEM((1, LANES), f32),
                pltpu.VMEM((ds, layers, LANES), f32),
                pltpu.VMEM((ds, layers, LANES), f32),
                pltpu.VMEM((ds, 1, 2 * LANES), f32),
                *[dma((n,)) for n in (3, 3, 5, 3, 3, 3, 4, 4, 5, 2, 2, 2, 4, 2, 4, 3, 6, 2, 4, 2)],
                *[dma((2,))] * 4,
            ],
            compiler_params=pltpu.CompilerParams(collective_id=0, has_side_effects=True, vmem_limit_bytes=50 * 1000 * 1000),
            name='adafactor_step',
        )(weight, grads, row_stat, col_stat, norm_scale, norm_grads, norm_stat, learn_rate)
        return write_out(ds, zs, learn_rate, *outs)

    mat_spec = P(None, 'dp', 'model')
    row_spec = P(None, 'dp')
    col_spec = P(None, 'model')
    return jax.shard_map(local_step, mesh=mesh, in_specs=(mat_spec, mat_spec, row_spec, col_spec, row_spec, row_spec, row_spec, P()), out_specs=(mat_spec, row_spec, col_spec, row_spec, row_spec), check_vma=False)
```

```python
import functools

import jax
import jax.numpy as jnp
from jax import lax
from jax.experimental import pallas as pl
from jax.experimental.pallas import tpu as pltpu
from jax.sharding import PartitionSpec as P

STEP_COUNT = 4
DECAY_POWER = 0.8
EPS_FLOOR = 1e-30
SCALE_FLOOR = 1e-3
CLIP_LIMIT = 1.0
DECAY = 1.0 - STEP_COUNT ** -DECAY_POWER
MESH = pl.DeviceIdType.MESH
LANES = 128
AHEAD = 2
DIRECT = 3
EARLY = 8


def column(row, rows):
    return jnp.transpose(jnp.broadcast_to(row, (LANES, LANES)))[0:rows]


def factors(sums, r_row, rate, rows, zs, rows_total, cols_total):
    count = rows_total * cols_total
    r_mean = sums[:, 2:3] / (rows_total * zs)
    u_rms = jnp.sqrt(sums[:, 0:1] / count * r_mean)
    clip = jnp.maximum(1.0, u_rms / CLIP_LIMIT)
    scale = rate * jnp.maximum(SCALE_FLOOR, jnp.sqrt(sums[:, 1:2] / count))
    return scale, clip, column(lax.rsqrt(r_row / r_mean), rows)


def step_kernel(w_hbm, g_hbm, r_hbm, c_hbm, n_hbm, ng_hbm, v_hbm, rate_ref,
                w_buf, d_buf, r_buf, c_buf, n_buf, v_buf, r_pad, sums_out,
                own, peer, in1x, in1y, in2, early, ng_buf, w_sq,
                r_all, c_mine, c_pair, c_all, c_full, c_last, s_all, t_all, t_last, held, h_out, h_all, k_all,
                load_sem, pair_send, pair_recv, one_send, one_recv, two_send, two_recv,
                r_send, r_recv, cp_send, cp_recv, c_send, c_recv, cf_send, cf_recv,
                s_send, s_recv, t_send, t_recv, w_sem,
                cl_send, cl_recv, tl_send, tl_recv):
    layers, _, rows, cols = own.shape
    half = rows // 2
    last, ds = layers - 1, c_last.shape[1]
    near_end = layers - c_last.shape[0]
    late = layers - DIRECT
    zs = r_all.shape[1]
    chips = ds // 2
    rows_total, cols_total = rows * ds, cols * zs
    z = lax.axis_index('model')
    d = lax.axis_index('dp')
    chip, core = lax.div(d, 2), lax.rem(d, 2)
    dx = d + 2 - 4 * lax.rem(chip, 2)
    dy = d + 4 - 8 * lax.div(d, 4)
    dxy = dx + dy - d
    dc = d + 1 - 2 * core
    blocks = (dx, dxy, dy, d)
    z_peers = [{'model': lax.rem(z + j, zs)} for j in range(1, zs)]
    d_peers = [{'dp': e} for e in (dc, dx, dx + dc - d, dy, dy + dc - d, dxy, dxy + dc - d)]
    column_peers = [{'dp': dc}] + [{'model': p['model'], 'dp': e} for p in z_peers for e in (d, dc)]
    plane_peers = [{'dp': e} for e in (dx, dy, dxy)]
    me = ds * z + d

    def everyone_else():
        for j in range(ds * zs - 1):
            e = j + jnp.where(me <= j, 1, 0)
            yield {'model': lax.div(e, ds), 'dp': lax.rem(e, ds)}

    def ring(sem, l):
        return sem.at[lax.rem(l, sem.shape[0])]

    def remote(src, dst, send, recv, where):
        return pltpu.make_async_remote_copy(src_ref=src, dst_ref=dst, send_sem=send, recv_sem=recv,
                                            device_id=where, device_id_type=MESH)

    def spread(ref, send, recv, peers):
        for where in peers:
            remote(ref, ref, send, recv, where).start()

    def drain(ref, sem):
        pltpu.make_async_copy(ref, ref, sem).wait()

    def load_own(l):
        for k in range(3):
            pltpu.make_async_copy(g_hbm.at[l, blocks[k]], own.at[l, k], ring(load_sem, l)).start()
        pltpu.make_async_copy(g_hbm.at[l, d], d_buf.at[l], ring(load_sem, l)).start()

    def pair_copy(l, k, row, source, recv):
        part = pl.ds(row, half)
        return remote(source.at[part], peer.at[l, k, part], ring(pair_send, l), recv, {'dp': dc})

    def from_hbm(l, k):
        return g_hbm.at[l, blocks[k] + dc - d]

    def send_pair(l):
        for k in range(4):
            remote(from_hbm(l, k), peer.at[l, k], ring(pair_send, l), ring(pair_recv, l), {'dp': dc}).start()

    def x1(l):
        return remote(own.at[l, 0:2, 0:half], in1x.at[l], ring(one_send, l), ring(one_recv, l), {'dp': dx})

    def y1(l):
        return remote(own.at[l, 1:3, half:rows], in1y.at[l], ring(one_send, l), ring(one_recv, l), {'dp': dy})

    def y2(l):
        return remote(own.at[l, 2, 0:half], in2.at[l, 0], ring(two_send, l), ring(two_recv, l), {'dp': dy})

    def x2(l):
        return remote(own.at[l, 0, half:rows], in2.at[l, 1], ring(two_send, l), ring(two_recv, l), {'dp': dx})

    def total(buf):
        parts = [buf[j] for j in range(buf.shape[0])]
        while len(parts) > 1:
            parts = [a + b for a, b in zip(parts[::2], parts[1::2])]
        return parts[0]

    def fold(values):
        acc = values[:, 0:LANES]
        for t in range(1, cols // LANES):
            acc = acc + values[:, t * LANES:(t + 1) * LANES]
        return acc

    small = ((r_hbm, r_buf), (c_hbm, c_buf), (n_hbm, n_buf), (ng_hbm, ng_buf), (v_hbm, v_buf))
    groups = (((0, 0), (1, 0)), ((1, half), (2, half)))
    for i, group in enumerate(groups):
        for k, row in group:
            part = pl.ds(row, half)
            pltpu.make_async_copy(from_hbm(0, k).at[part], own.at[layers - 1, i, pl.ds((k - i) * half, half)], w_sem.at[i]).start()
    load_own(0)
    small_sems = (r_send.at[0], r_send.at[1], r_send.at[2], r_send.at[3], cl_send.at[0])
    for (src, dst), sem in zip(small, small_sems):
        pltpu.make_async_copy(src, dst, sem).start()

    barrier = pltpu.get_barrier_semaphore()
    known = d_peers + column_peers[1:]
    for where in known:
        pl.semaphore_signal(barrier, inc=1, device_id=where, device_id_type=MESH)
    pl.semaphore_wait(barrier, len(known))
    for i, (near, row) in enumerate(((dx, 0), (dy, half))):
        for e in (near, near + dc - d):
            remote(g_hbm.at[0, e, pl.ds(row, EARLY)], early.at[i, core], tl_send.at[1], tl_recv.at[1], {'dp': e}).start()
    for i, group in enumerate(groups):
        drain(own.at[layers - 1, i], w_sem.at[i])
        for k, row in group:
            part = pl.ds(row, half)
            remote(own.at[layers - 1, i, pl.ds((k - i) * half, half)], peer.at[0, k, part],
                   pair_send.at[0], two_recv.at[i + 1], {'dp': dc}).start()
    for k, row in ((0, half), (2, 0), (3, 0), (3, half)):
        pair_copy(0, k, row, from_hbm(0, k), two_recv.at[3]).start()
    for l in range(1, AHEAD):
        send_pair(l)
        load_own(l)

    def norm_split():
        for i in (0, 1, 2, 4):
            pltpu.make_async_copy(*small[i], small_sems[i]).wait()
        r_pad[...] = jnp.zeros_like(r_pad)
        r_pad[:, 0:rows] = r_buf[...]
        k_all[...] = jnp.zeros_like(k_all)

    h_out[...] = jnp.zeros_like(h_out)
    pltpu.make_async_copy(*small[3], small_sems[3]).wait()
    for k in range(ds):
        h_out[k, :, 0:rows] = ng_buf[:, k * rows:(k + 1) * rows]
    h_all[d] = h_out[d]
    for where in d_peers:
        remote(h_out.at[where['dp']], h_all.at[d], cl_send.at[1], cl_recv.at[1], where).start()

    def layer_sums(values):
        padded = jnp.concatenate([values, jnp.zeros((layers, LANES - rows), jnp.float32)], axis=1)
        return jnp.sum(jnp.transpose(padded), axis=0, keepdims=True)

    def norm_stats():
        drain(h_all.at[0:ds - 1], cl_recv.at[1])
        drain(h_all.at[0:ds - 1], cl_send.at[1])
        h = total(h_all)[:, 0:rows]
        v_new = DECAY * v_buf[...] + (1.0 - DECAY) * (h * h + EPS_FLOOR)
        v_buf[...] = v_new
        zv = h * lax.rsqrt(v_new)
        nv = n_buf[...]
        k_all[d, :, 0:layers] = layer_sums(zv * zv)
        k_all[d, :, LANES:LANES + layers] = layer_sums(nv * nv)
        spread(k_all.at[d], tl_send.at[0], tl_recv.at[0], d_peers)

    def norm_update():
        drain(k_all.at[0:ds - 1], tl_recv.at[0])
        drain(k_all.at[0:ds - 1], tl_send.at[0])
        acc = total(k_all)
        z_sq, n_sq = acc[:, 0:layers], acc[:, LANES:LANES + layers]
        clip = jnp.maximum(1.0, jnp.sqrt(z_sq / rows_total) / CLIP_LIMIT)
        scale = rate_ref[...] * jnp.maximum(SCALE_FLOOR, jnp.sqrt(n_sq / rows_total))
        clip = jnp.transpose(jnp.broadcast_to(clip, (LANES, layers)))[:, 0:rows]
        scale = jnp.transpose(jnp.broadcast_to(scale, (LANES, layers)))[:, 0:rows]
        zv = total(h_all)[:, 0:rows] * lax.rsqrt(v_buf[...])
        n_buf[...] = n_buf[...] - scale * (zv / clip)

    def combine(l, k, part):
        own[l, k, part] = own[l, k, part] + peer[l, k, part]

    first, second = slice(0, half), slice(half, rows)

    def stage_first():
        drain(peer.at[0], load_sem.at[0])
        drain(in1x.at[0], two_recv.at[1])
        combine(0, slice(0, 2), first)
        for k, row in ((0, EARLY), (1, 0)):
            part = pl.ds(row, half - row)
            remote(own.at[0, k, part], in1x.at[0, k, part], one_send.at[0], one_recv.at[0], {'dp': dx}).start()
        drain(in1y.at[0], two_recv.at[2])
        combine(0, slice(1, 3), second)
        for k, row in ((0, 0), (1, EARLY)):
            remote(own.at[0, k + 1, pl.ds(half + row, half - row)], in1y.at[0, k, pl.ds(row, half - row)],
                   one_send.at[0], one_recv.at[0], {'dp': dy}).start()
        drain(peer.at[0, 0:2], two_recv.at[3])
        combine(0, 0, second)
        combine(0, 2, first)
        d_buf[0] = d_buf[0] + peer[0, 3]
        drain(peer.at[0], pair_send.at[0])

    def stage_combine(l):
        drain(peer.at[l], ring(load_sem, l))
        drain(peer.at[l], ring(pair_recv, l))
        combine(l, slice(0, 2), first)
        x1(l).start()
        combine(l, slice(1, 3), second)
        y1(l).start()
        combine(l, 0, second)
        combine(l, 2, first)
        d_buf[l] = d_buf[l] + peer[l, 3]
        drain(peer.at[l], ring(pair_send, l))

    def stage_forward(l):
        pltpu.make_async_copy(w_hbm.at[l], w_buf.at[l], ring(w_sem, l)).start()
        drain(in1x.at[0:2], ring(one_recv, l))
        own[l, 2, 0:half] = own[l, 2, 0:half] + in1x[l, 1]
        own[l, 0, half:rows] = own[l, 0, half:rows] + in1y[l, 0]
        y2(l).start()
        d_buf[l, 0:half] = d_buf[l, 0:half] + in1x[l, 0]
        x2(l).start()
        d_buf[l, half:rows] = d_buf[l, half:rows] + in1y[l, 1]

    first_part = w_buf.at[0:half // 4 - EARLY // 8, 0:16]

    def forward_first():
        drain(first_part, one_recv.at[0])
        own[0, 2, first] = own[0, 2, first] + in1x[0, 1]
        own[0, 0, second] = own[0, 0, second] + in1y[0, 0]
        y2(0).start()
        x2(0).start()
        pltpu.make_async_copy(w_hbm.at[0], w_buf.at[0], w_sem.at[0]).start()
        drain(early, tl_recv.at[1])
        drain(early, tl_send.at[1])
        rest = slice(EARLY, half)
        d_buf[0, 0:EARLY] = d_buf[0, 0:EARLY] + (early[0, 0] + early[0, 1])
        d_buf[0, rest] = d_buf[0, rest] + in1x[0, 0, rest]
        d_buf[0, half:half + EARLY] = d_buf[0, half:half + EARLY] + (early[1, 0] + early[1, 1])
        d_buf[0, half + EARLY:rows] = d_buf[0, half + EARLY:rows] + in1y[0, 1, rest]

    def stage_stats(l):
        drain(w_buf.at[l], ring(w_sem, l))
        w = w_buf[l]
        w_sq[pl.ds(l, 1)] = fold(jnp.sum(w * w, axis=0, keepdims=True))
        drain(in2.at[l], ring(two_recv, l))
        g = d_buf[l] + in2[l].reshape(rows, cols)
        d_buf[l] = g
        q = g * g + EPS_FLOOR
        col = jnp.sum(q, axis=0, keepdims=True)

        @pl.when(l < near_end)
        def _():
            c_mine[l, 0] = col[:, 0:cols // 2]
            c_mine[l, 1] = col[:, cols // 2:cols]

        @pl.when(l >= near_end)
        def _():
            c_last[l - near_end, d] = col

        p = jnp.concatenate([fold(q), jnp.zeros((LANES - rows, LANES), jnp.float32)], axis=0)
        r_all[l, z] = jnp.sum(jnp.transpose(p), axis=0, keepdims=True)

        @pl.when(l < near_end)
        def _():
            pair_columns(l).start()

        @pl.when(l >= near_end)
        def _():
            e = l - near_end
            spread(c_last.at[e, d], cl_send.at[e], cl_recv.at[e], d_peers)

        spread(r_all.at[l, z], ring(r_send, l), ring(r_recv, l), z_peers)

    def pair_columns(l):
        return remote(c_mine.at[l, 1 - core], c_pair.at[l], ring(cp_send, l), ring(cp_recv, l), {'dp': dc})

    def full_columns(l):
        return remote(c_full.at[l, core], c_full.at[l, core], ring(cf_send, l), ring(cf_recv, l), {'dp': dc})

    def drain_rows(l):
        if zs > 1:
            drain(r_all.at[l, 0:zs - 1], ring(r_recv, l))
            drain(r_all.at[l, 0:zs - 1], ring(r_send, l))

    def stage_columns(l):
        pair_columns(l).wait()
        c_all[l, chip] = c_mine[l, core] + c_pair[l]
        spread(c_all.at[l, chip], ring(c_send, l), ring(c_recv, l), plane_peers)

    def stage_share(l):
        drain(c_all.at[l, 0:chips - 1], ring(c_recv, l))
        drain(c_all.at[l, 0:chips - 1], ring(c_send, l))
        c_full[l, core] = total(c_all.at[l])
        full_columns(l).start()
        drain_rows(l)

    def stage_moments(l):
        @pl.when(l < near_end)
        def _():
            full_columns(l).wait()

        @pl.when(l >= near_end)
        def _():
            e = l - near_end
            drain(c_last.at[e, 0:ds - 1], cl_recv.at[e])
            drain(c_last.at[e, 0:ds - 1], cl_send.at[e])
            drain_rows(l)
            col = total(c_last.at[e])
            c_full[l, 0] = col[:, 0:cols // 2]
            c_full[l, 1] = col[:, cols // 2:cols]

        col = jnp.concatenate([c_full[l, 0], c_full[l, 1]], axis=1)
        r_new = DECAY * r_pad[pl.ds(l, 1)] + (1.0 - DECAY) * (total(r_all.at[l]) / cols_total)
        c_new = DECAY * c_buf[pl.ds(l, 1)] + (1.0 - DECAY) * (col / rows_total)
        r_pad[pl.ds(l, 1)] = r_new
        r_buf[pl.ds(l, 1)] = r_new[:, 0:rows]
        c_buf[pl.ds(l, 1)] = c_new
        a = column(lax.rsqrt(r_new), rows)
        b = lax.rsqrt(c_new)
        acc = jnp.zeros((1, LANES), jnp.float32)
        for t in range(cols // LANES):
            sl = slice(t * LANES, (t + 1) * LANES)
            u = d_buf[l, :, sl] * a * b[:, sl]
            acc = acc + jnp.sum(u * u, axis=0, keepdims=True)
        lane = lax.broadcasted_iota(jnp.int32, (1, LANES), 1)
        lane = lane - jnp.where(l >= late, 3 * (last - l), 0)
        row = jnp.where(lane == 0, jnp.sum(acc, axis=1, keepdims=True), 0.0)
        row = jnp.where(lane == 1, jnp.sum(w_sq[pl.ds(l, 1)], axis=1, keepdims=True), row)
        row = jnp.where(lane == 2, jnp.sum(r_new, axis=1, keepdims=True), row)

        @pl.when(l < late)
        def _():
            s_all[l, 2 * z + core] = row
            spread(s_all.at[l, 2 * z + core], ring(s_send, l), ring(s_recv, l), column_peers)

        @pl.when(l == late)
        def _():
            held[...] = row

        @pl.when((l > late) & (l < last))
        def _():
            held[...] = held[...] + row

        @pl.when(l == last)
        def _():
            t_last[me] = row + held[...]
            spread(t_last.at[me], tl_send.at[0], tl_recv.at[0], everyone_else())

    def stage_gather(l):
        drain(s_all.at[l, 0:2 * zs - 1], ring(s_recv, l))
        drain(s_all.at[l, 0:2 * zs - 1], ring(s_send, l))
        t_all[l, chip] = total(s_all.at[l])
        spread(t_all.at[l, chip], ring(t_send, l), ring(t_recv, l), plane_peers)

    def stage_update(l):
        drain(t_all.at[l, 0:chips - 1], ring(t_recv, l))
        drain(t_all.at[l, 0:chips - 1], ring(t_send, l))
        scale, clip, a = factors(total(t_all.at[l]), r_pad[pl.ds(l, 1)], rate_ref[...], rows, zs, rows_total, cols_total)
        b = lax.rsqrt(c_buf[pl.ds(l, 1)]) / clip
        for t in range(cols // LANES):
            sl = slice(t * LANES, (t + 1) * LANES)
            w_buf[l, :, sl] = w_buf[l, :, sl] - scale * (d_buf[l, :, sl] * a * b[:, sl])

    def stage_final():
        drain(t_last.at[0:ds * zs - 1], tl_recv.at[0])
        sums_out[...] = total(t_last)
        drain(t_last.at[0:ds * zs - 1], tl_send.at[0])

    def drain_one(l):
        drain(in1x.at[0:2], ring(one_send, l))

    def drain_two(l):
        drain(in2.at[l], ring(two_send, l))

    def at(i, lag, stage, begin=0, end=layers):
        @pl.when((i >= begin + lag) & (i < end + lag))
        def _():
            stage(i - lag)

    def once(i, when, stage):
        @pl.when(i == when)
        def _():
            stage()

    def prefetch(l):
        load_own(l)
        send_pair(l)

    def body(i, carry):
        at(i, -AHEAD, prefetch)
        at(i, 0, stage_combine, 1)
        once(i, 0, stage_first)
        at(i, 1, stage_forward, 1)
        once(i, 1, forward_first)
        once(i, 1, norm_split)
        at(i, 3, stage_columns, 0, near_end)
        at(i, 4, stage_share, 0, near_end)
        at(i, 5, stage_moments)
        at(i, 7, stage_gather, 0, late)
        at(i, 8, stage_update, 0, late)
        at(i, 2, drain_one, 1)
        once(i, 2, lambda: drain(first_part, one_send.at[0]))
        at(i, 3, drain_two)
        once(i, 4, norm_stats)
        once(i, 6, norm_update)
        at(i, 2, stage_stats)
        return carry

    lax.fori_loop(0, late + 8, body, 0)
    stage_final()


def write_kernel(ds, zs, rate_ref, w, d, r, c, n, v, r_pad, sums, wo, ro, co, no, vo, w_new, sem):
    layers, rows, cols = w.shape
    late = layers - DIRECT
    pairs = ((w.at[0:late], wo.at[0:late]), (r, ro), (c, co), (v, vo), (n, no))
    for i, pair in enumerate(pairs):
        pltpu.make_async_copy(*pair, sem.at[i]).start()
    for e in range(DIRECT):
        l = late + e
        lane = 3 * (DIRECT - 1 - e)
        scale, clip, a = factors(sums[:, lane:lane + 3], r_pad[l:l + 1], rate_ref[...], rows, zs, rows * ds, cols * zs)
        b = lax.rsqrt(c[l:l + 1]) / clip
        for t in range(cols // LANES):
            sl = slice(t * LANES, (t + 1) * LANES)
            w_new[e, :, sl] = w[l, :, sl] - scale * (d[l, :, sl] * a * b[:, sl])
    for e in range(DIRECT):
        pltpu.make_async_copy(w_new.at[e], wo.at[late + e], sem.at[5]).start()
    for i, pair in enumerate(pairs):
        pltpu.make_async_copy(*pair, sem.at[i]).wait()
    pltpu.make_async_copy(w_new, wo.at[late:layers], sem.at[5]).wait()


def write_out(ds, zs, rate, w, d, r, c, n, v, r_pad, sums):
    return pl.pallas_call(
        functools.partial(write_kernel, ds, zs),
        out_shape=[jax.ShapeDtypeStruct(a.shape, a.dtype) for a in (w, r, c, n, v)],
        in_specs=[pl.BlockSpec(memory_space=pltpu.MemorySpace.SMEM)] + [pl.BlockSpec(memory_space=pltpu.MemorySpace.VMEM)] * 8,
        out_specs=[pl.BlockSpec(memory_space=pltpu.MemorySpace.HBM)] * 5,
        scratch_shapes=[pltpu.VMEM((DIRECT,) + w.shape[1:], w.dtype), pltpu.SemaphoreType.DMA((6,))],
        compiler_params=pltpu.CompilerParams(vmem_limit_bytes=4 << 20),
        name='write_out',
    )(rate, w, d, r, c, n, v, r_pad, sums)


def solution(mesh):
    ds = mesh.shape['dp']
    zs = mesh.shape['model']

    def local_step(weight, grad_parts, row_stat, col_stat, norm_scale, norm_grads, norm_stat, learn_rate):
        layers, rows, cols = weight.shape
        half = rows // 2
        f32 = jnp.float32
        grads = grad_parts.reshape(layers, ds, rows, cols)
        any_spec = pl.BlockSpec(memory_space=pltpu.MemorySpace.HBM)
        dma = pltpu.SemaphoreType.DMA
        outs = pl.pallas_call(
            step_kernel,
            out_shape=[pltpu.VMEM(a.shape, f32) for a in (weight, weight, row_stat, col_stat, norm_scale, norm_stat)]
            + [pltpu.VMEM((layers, LANES), f32), pltpu.VMEM((1, LANES), f32)],
            in_specs=[any_spec] * 7 + [pl.BlockSpec(memory_space=pltpu.MemorySpace.SMEM)],
            out_specs=[pl.BlockSpec(memory_space=pltpu.MemorySpace.VMEM)] * 8,
            scratch_shapes=[
                pltpu.VMEM((layers, 3, rows, cols), f32),
                pltpu.VMEM((layers, 4, rows, cols), f32),
                pltpu.VMEM((layers, 2, half, cols), f32),
                pltpu.VMEM((layers, 2, half, cols), f32),
                pltpu.VMEM((layers, 2, half, cols), f32),
                pltpu.VMEM((2, 2, EARLY, cols), f32),
                pltpu.VMEM(norm_grads.shape, f32),
                pltpu.VMEM((layers, LANES), f32),
                pltpu.VMEM((layers, zs, 1, LANES), f32),
                pltpu.VMEM((layers, 2, 1, cols // 2), f32),
                pltpu.VMEM((layers, 1, cols // 2), f32),
                pltpu.VMEM((layers, ds // 2, 1, cols // 2), f32),
                pltpu.VMEM((layers, 2, 1, cols // 2), f32),
                pltpu.VMEM((2, ds, 1, cols), f32),
                pltpu.VMEM((layers, 2 * zs, 1, LANES), f32),
                pltpu.VMEM((layers, ds // 2, 1, LANES), f32),
                pltpu.VMEM((ds * zs, 1, LANES), f32),
                pltpu.VMEM((1, LANES), f32),
                pltpu.VMEM((ds, layers, LANES), f32),
                pltpu.VMEM((ds, layers, LANES), f32),
                pltpu.VMEM((ds, 1, 2 * LANES), f32),
                *[dma((n,)) for n in (3, 3, 5, 3, 3, 3, 4, 4, 5, 2, 2, 2, 4, 2, 4, 3, 6, 2, 4, 2)],
                *[dma((2,))] * 4,
            ],
            compiler_params=pltpu.CompilerParams(collective_id=0, has_side_effects=True, vmem_limit_bytes=50 * 1000 * 1000),
            name='adafactor_step',
        )(weight, grads, row_stat, col_stat, norm_scale, norm_grads, norm_stat, learn_rate)
        return write_out(ds, zs, learn_rate, *outs)

    mat_spec = P(None, 'dp', 'model')
    row_spec = P(None, 'dp')
    col_spec = P(None, 'model')
    return jax.shard_map(local_step, mesh=mesh, in_specs=(mat_spec, mat_spec, row_spec, col_spec, row_spec, row_spec, row_spec, P()), out_specs=(mat_spec, row_spec, col_spec, row_spec, row_spec), check_vma=False)
```
